32 devices in a mesh: groups: 2 (over y), heads: 4 (over x, core), tm: 4 (over z).
Axes of the slice: x: 2, y: 2, z: 4, core: 2. Of those that a mesh axis runs over, the one named last changes fastest.
Arguments:
- queries: bfloat16 [256, 8192], P('groups', 'heads'), parts along dimension 0, may hold values from -6 to 6
- cache_keys: bfloat16 [8192, 8192], P(('groups', 'tm'), 'heads'), parts along dimension 0, may hold values from -650 to 650
- cache_values: bfloat16 [8192, 8192], P(('groups', 'tm'), 'heads'), parts along dimension 0, may hold values from -6 to 6
- residual: bfloat16 [256, 8192], P('groups', 'tm'), parts along dimension 0, may hold values from -20 to 20
- out_weight: bfloat16 [8192, 8192], P('heads', 'tm'), may hold values from -0.0625 to 0.0625
- norm_gain: float32 [8192], P('tm'), may hold values from 0.1 to 1.9
- cond_weight: bfloat16 [8192, 1536], P('tm', 'heads'), may hold values from -0.0625 to 0.0625
- in_weight: bfloat16 [1152, 1536], replicated, may hold values from -0.1875 to 0.1875
- head_out: bfloat16 [1536, 1152], replicated, may hold values from -0.15625 to 0.15625
- start_state: float32 [256, 1152], P(('groups', 'heads')), parts along dimension 0, may hold values from -6 to 6
- noise_draws: bfloat16 [256, 8, 1152], P(('groups', 'heads'), 'tm'), parts along dimension 0, may hold values from -6 to 6
- positions: int32 [256], P('groups'), parts along dimension 0, may hold values from 0 to 4095
- cache_length: int32 [2], P('groups'), parts along dimension 0, may hold values from 2048 to 4096
- plan: int32 [9], replicated, may hold values from 0 to 1000, as said below
Outputs:
- states: float32 [256, 8, 1152], P(('groups', 'heads'), 'tm'), parts along dimension 0
The draws below stay inside these ranges and needn't reach their ends.
There are 2 independent parts, one for each index of `groups`. The reference program is written for one: setup_inputs(seed, part) draws one part's arguments, and reference() takes and returns one part's arrays. A program takes and returns all parts, laid end to end along the dimension named above; an argument that names none is the same for every part. Nothing has to cross between parts.
Inputs may be any that keep to these rules, and one draw needn't show every extreme that they name: `plan`: strictly decreasing; the first entry is 1000 and the last is 0.
All inputs are finite; a program needn't handle non-finite values.
Results may differ from the reference program's by a relative error of at most 0.0028.
Values may be sent and summed in bfloat16 or wider, within the bound.
No kernel may reach another device: no remote copies, remote signals or barrier semaphores. Data moves between devices by JAX's collectives and lax.ppermute only.
A program may use at most 128 MiB of HBM per device.

```python
import math
import jax
import jax.numpy as jnp
from jax import lax

D = 8192
HEADS = 64
HD = 128
WIDTH = 1536
CHAN = 1152
CACHE_DEV = 1024
SWEEPS = 3
ROWS = 128
CACHE = 4096
TIMES = 8
N_TM = 4


def draw_plan(key, part):
    inner = jax.random.permutation(key, 999)[:TIMES - 1] + 1
    inner = -jnp.sort(-inner)
    return jnp.concatenate([jnp.array([1000], dtype=jnp.int32), inner.astype(jnp.int32), jnp.array([0], dtype=jnp.int32)])


def draw_cache_keys(key, part):
    key_one = jax.random.fold_in(jax.random.fold_in(key, 11), 0)
    base = jnp.clip(jax.random.normal(key_one, (CACHE, D), jnp.float32), -4.0, 4.0)
    return base.astype(jnp.bfloat16)


def draw_residual(key, part):
    key_one, key_two, key_three = jax.random.split(jax.random.fold_in(key, 23), 3)
    normal_part = jnp.clip(jax.random.normal(key_one, (ROWS, D), jnp.float32), -4.0, 4.0)
    row_scale = jnp.power(10.0, jax.random.uniform(key_two, (ROWS, 1), jnp.float32, -0.5, 0.5))
    column = jnp.arange(D, dtype=jnp.float32) / D
    col_scale = jnp.power(10.0, 0.4 * column - 0.2 + 0.2 * jax.random.uniform(key_three, (D,), jnp.float32, -1.0, 1.0))
    return (normal_part * row_scale * col_scale[None, :] / 3.0).astype(jnp.bfloat16)


def touch_ends(values, own_key, low, high):
    longest = values.shape.index(max(values.shape))
    spots = []
    for shift in (0, 1):
        where = [jax.random.randint(jax.random.fold_in(own_key, axis), (), 0, length) for axis, length in enumerate(values.shape)]
        where[longest] = (where[longest] + shift) % values.shape[longest]
        spots.append(tuple(where))
    return values.at[spots[0]].set(low).at[spots[1]].set(high)


def shard_levels(key, extent, shards, low, high):
    loudness = 1.0
    for position, shards_of in shards:
        steps = jax.random.uniform(jax.random.fold_in(jax.random.fold_in(key, 6), position), (shards_of,), jnp.float32, low / len(shards), high / len(shards))
        loudness = loudness * jnp.repeat(jnp.exp(steps), extent[position] // shards_of).reshape((-1,) + (1,) * (len(extent) - 1 - position))
    return loudness


def noise(rng, dims, deviation, most, cuts=(), kind=jnp.bfloat16):
    values = jax.random.normal(rng, dims, jnp.float32) * deviation
    if len(cuts) > 0:
        values = shard_levels(rng, dims, cuts, -0.22, 0.18) * values
    return jnp.clip(values, min=-most, max=most).astype(kind)


def setup_inputs(seed: int = 0, part: int = 0) -> dict:
    key_of = jax.random.split(jax.random.key(seed), 15)
    part_splits = jax.random.split(jax.random.fold_in(key_of[14], part), 15)
    return {
        "queries": noise(part_splits[0], (ROWS, D), 1.0, 6.0, ((1, 4),)),
        "cache_keys": draw_cache_keys(jax.random.fold_in(jax.random.fold_in(key_of[14], part), 71), part),
        "cache_values": noise(part_splits[2], (CACHE, D), 1.0, 6.0, ((0, 4), (1, 4))),
        "residual": draw_residual(jax.random.fold_in(jax.random.fold_in(key_of[14], part), 71), part),
        "out_weight": noise(key_of[4], (D, D), D ** -0.5, 0.0625, ((0, 4), (1, 4))),
        "norm_gain": jnp.clip(1.0 + 0.18 * jax.random.normal(key_of[5], (D,), jnp.float32), 0.1, 1.9),
        "cond_weight": noise(key_of[6], (D, WIDTH), D ** -0.5, 0.0625, ((0, 4), (1, 4))),
        "in_weight": noise(key_of[7], (CHAN, WIDTH), CHAN ** -0.5, 0.1875),
        "head_out": noise(key_of[8], (WIDTH, CHAN), WIDTH ** -0.5, 0.15625),
        "start_state": noise(part_splits[9], (ROWS, CHAN), 1.0, 6.0, ((0, 4),), jnp.float32),
        "noise_draws": noise(part_splits[10], (ROWS, TIMES, CHAN), 1.0, 6.0, ((0, 4), (1, 4))),
        "positions": touch_ends(jax.random.randint(part_splits[11], (ROWS,), 0, CACHE), jax.random.fold_in(part_splits[11], 1), 0, CACHE - 1).astype(jnp.int32),
        "cache_length": jax.random.randint(part_splits[12], (1,), CACHE // 2, CACHE + 1).astype(jnp.int32),
        "plan": draw_plan(jax.random.fold_in(key_of[14], 71), part),
    }


def rotate(values, angle_pos):
    head_feature_width = values.shape[-1]
    half_dim = head_feature_width // 2
    frequencies = jnp.exp(-math.log(10000.0) * 2.0 * jnp.arange(half_dim, dtype=jnp.float32) / head_feature_width)
    angles = angle_pos[:, None] * frequencies[None, :]
    cosine = jnp.cos(angles)[:, None, :]
    sine_part = jnp.sin(angles)[:, None, :]
    paired = values.astype(jnp.float32).reshape(values.shape[0], values.shape[1], half_dim, 2)
    real_part = paired[..., 0]
    imag_part = paired[..., 1]
    turned = jnp.stack([real_part * cosine - imag_part * sine_part, real_part * sine_part + imag_part * cosine], axis=-1)
    return turned.reshape(values.shape).astype(jnp.bfloat16)

def time_terms(levels, hidden_width):
    half_width = hidden_width // 2
    frequencies = jnp.exp(-math.log(10000.0) * jnp.arange(half_width, dtype=jnp.float32) / half_width)
    angles = levels[:-1, None] * frequencies[None, :]
    embedding = jnp.concatenate([jnp.sin(angles), jnp.cos(angles)], axis=1)
    step_size = (levels[:-1] - levels[1:]) / 1000.0
    return (embedding, step_size, jnp.sqrt(step_size))

def block_attend(rotary_applied, block_key_rows, block_value_rows, valid_keys):
    head_feature_width = rotary_applied.shape[-1]
    attention_logits = jnp.einsum('orp,brp->orb', rotary_applied.astype(jnp.float32), block_key_rows.astype(jnp.float32), precision=lax.Precision.HIGHEST) * (1.0 / math.sqrt(head_feature_width))
    masked = jnp.where(valid_keys[None, None, :], attention_logits, jnp.float32(-1e+30))
    block_max = lax.optimization_barrier(jnp.max(masked, axis=2))
    weights = jnp.where(valid_keys[None, None, :], jnp.exp(masked - block_max[:, :, None]), jnp.float32(0.0))
    block_total = lax.optimization_barrier(jnp.sum(weights, axis=2))
    rounded_values = weights.astype(jnp.bfloat16).astype(jnp.float32)
    block_output_part = jnp.einsum('pzu,uzx->pzx', rounded_values, block_value_rows.astype(jnp.float32), precision=lax.Precision.HIGHEST)
    return (block_max, block_total, block_output_part)

def reference(queries, cache_keys, cache_values, residual, out_weight, norm_gain, cond_weight, in_weight, head_out, start_state, noise_draws, positions, cache_length, plan):
    row_total = queries.shape[0]
    rotary_applied = rotate(queries.reshape(row_total, HEADS, HD), positions.astype(jnp.float32))

    def one_block(block_index):
        first_key = (block_index * CACHE_DEV).astype(jnp.int32)
        block_key_rows = lax.dynamic_slice_in_dim(cache_keys, first_key, CACHE_DEV, 0).reshape(CACHE_DEV, HEADS, HD)
        block_value_rows = lax.dynamic_slice_in_dim(cache_values, first_key, CACHE_DEV, 0).reshape(CACHE_DEV, HEADS, HD)
        key_pos = first_key + jnp.arange(CACHE_DEV, dtype=jnp.int32)
        valid_keys = key_pos < cache_length[0]
        return block_attend(rotary_applied, block_key_rows, block_value_rows, valid_keys)
    block_maxes, block_totals, block_outs = lax.map(one_block, jnp.arange(N_TM, dtype=jnp.int32))
    highest = lax.optimization_barrier(jnp.max(block_maxes, axis=0))
    factors = jnp.exp(block_maxes - highest[None])
    numer = lax.optimization_barrier(jnp.sum(block_outs * factors[..., None], axis=0))
    denom = lax.optimization_barrier(jnp.sum(block_totals * factors, axis=0))
    attended = (numer / denom[:, :, None]).reshape(row_total, D).astype(jnp.bfloat16)
    hidden = residual.astype(jnp.float32) + jnp.dot(attended, out_weight, preferred_element_type=jnp.float32)
    inverse = lax.rsqrt(lax.optimization_barrier(jnp.mean(hidden * hidden, axis=1)) + 1e-06)
    scaled = (hidden * norm_gain[None, :]).astype(jnp.bfloat16)
    condition = inverse[:, None] * jnp.dot(scaled, cond_weight, preferred_element_type=jnp.float32)
    embedding, step_size, noise_scale = time_terms(plan.astype(jnp.float32), WIDTH)
    time_total = noise_draws.shape[1]
    noise_term = noise_scale[None, :, None] * noise_draws.astype(jnp.float32)
    states = jnp.broadcast_to(start_state[:, None, :], noise_draws.shape).astype(jnp.float32)
    for sweep_index in range(SWEEPS):
        flat_states = states.astype(jnp.bfloat16).reshape(row_total * time_total, CHAN)
        preact = jnp.dot(flat_states, in_weight, preferred_element_type=jnp.float32).reshape(row_total, time_total, WIDTH)
        preact = preact + condition[:, None, :] + embedding[None]
        action = jax.nn.silu(preact).astype(jnp.bfloat16)
        drift_term = jnp.dot(action.reshape(row_total * time_total, WIDTH), head_out, preferred_element_type=jnp.float32).reshape(row_total, time_total, CHAN)
        increment = step_size[None, :, None] * drift_term + noise_term
        running = jnp.cumsum(increment, axis=1)
        states = start_state[:, None, :] + (running - increment)
    return states
```

```python
import functools
import math

import jax
import jax.numpy as jnp
from jax import lax
from jax.experimental import pallas as pl
from jax.experimental.pallas import tpu as pltpu
from jax.sharding import PartitionSpec as P

HD = 128
SWEEPS = 3
LANES = 128


def swap(values, axis, distance):
    size = lax.axis_size(axis)
    return lax.ppermute(values, axis, [(i, i ^ distance) for i in range(size)])


def pick(values, index):
    return lax.dynamic_index_in_dim(values, index, 0, False)


def whole(shape):
    return pl.BlockSpec(shape, lambda *_: (0,) * len(shape))


def cost(flops, transcendentals, *arrays):
    moved = sum(math.prod(a.shape) * jnp.dtype(a.dtype).itemsize for a in arrays)
    return pl.CostEstimate(flops=flops, bytes_accessed=moved, transcendentals=transcendentals)


def rotation_tables(positions):
    pair = jnp.arange(HD, dtype=jnp.int32) // 2
    frequencies = jnp.exp(-math.log(10000.0) * 2.0 * pair.astype(jnp.float32) / HD)
    angles = positions.astype(jnp.float32)[:, None] * frequencies[None, :]
    sign = jnp.where(jnp.arange(HD) % 2 == 0, -1.0, 1.0).astype(jnp.float32)
    return jnp.cos(angles), jnp.sin(angles) * sign[None, :]


def attend_kernel(groups, share, step_heads, info, q_ref, k_ref, v_ref, cos_ref, sin_ref, *refs):
    outs, stats, table = refs[:groups], refs[groups : 2 * groups], refs[2 * groups]
    step = pl.program_id(0)
    group_steps = share // step_heads
    rows, keys = q_ref.shape[0], k_ref.shape[0]
    valid = lax.broadcasted_iota(jnp.int32, (1, keys), 1) < info[1]
    even = lax.broadcasted_iota(jnp.int32, (rows, HD), 1) % 2 == 0
    lane = lax.broadcasted_iota(jnp.int32, (rows, LANES), 1)
    scale = 1.0 / math.sqrt(HD)
    results = []
    for i in range(step_heads):
        at = slice(i * HD, (i + 1) * HD)
        wide = q_ref[:, at].astype(jnp.float32)
        partner = jnp.where(even, pltpu.roll(wide, HD - 1, 1), pltpu.roll(wide, 1, 1))
        rotated = (wide * cos_ref[...] + partner * sin_ref[...]).astype(jnp.bfloat16)
        scores = lax.dot_general(
            rotated, k_ref[:, at], (((1,), (1,)), ((), ())), preferred_element_type=jnp.float32
        )
        masked = jnp.where(valid, scores * scale, jnp.float32(-1e30))
        block_max = jnp.max(masked, axis=1, keepdims=True)
        weights = jnp.where(valid, jnp.exp(masked - block_max), 0.0)
        block_total = jnp.sum(weights, axis=1, keepdims=True)
        block_out = jnp.dot(
            weights.astype(jnp.bfloat16), v_ref[:, at], preferred_element_type=jnp.float32
        )
        results.append((block_max, block_total, block_out.astype(jnp.bfloat16)))
    for group in range(groups):
        for part in range(group_steps):

            @pl.when(step == group * group_steps + part)
            def _(group=group, part=part):
                held = table[...] if part else jnp.zeros((rows, LANES), jnp.float32)
                for i, (block_max, block_total, block_out) in enumerate(results):
                    head = part * step_heads + i
                    outs[group][:, head * HD : (head + 1) * HD] = block_out
                    held = jnp.where(lane == head, block_max, held)
                    held = jnp.where(lane == share + head, block_total, held)
                if part == group_steps - 1:
                    stats[group][...] = held.T[: 2 * share]
                else:
                    table[...] = held


def attend(queries, keys, values, cosine, sine, first, valid_count, groups, share):
    rows = queries.shape[0]
    key_count = keys.shape[0]
    step_heads = 2 if share % 2 == 0 else 1
    per = share // step_heads
    width = step_heads * HD
    info = jnp.stack([first, valid_count]).astype(jnp.int32)

    def column(step, info):
        a = jnp.int32(0)
        for g, value in enumerate(groups):
            a = jnp.where(step // per == g, value, a)
        return (0, (info[0] ^ a) * per + step % per)

    n = len(groups)
    result = pl.pallas_call(
        functools.partial(attend_kernel, n, share, step_heads),
        grid_spec=pltpu.PrefetchScalarGridSpec(
            num_scalar_prefetch=1,
            grid=(n * per,),
            in_specs=[
                pl.BlockSpec((rows, width), column),
                pl.BlockSpec((key_count, width), column),
                pl.BlockSpec((key_count, width), column),
                whole((rows, HD)),
                whole((rows, HD)),
            ],
            out_specs=[whole((rows, share * HD))] * n + [whole((2 * share, rows))] * n,
            scratch_shapes=[pltpu.VMEM((rows, LANES), jnp.float32)],
        ),
        out_shape=[jax.ShapeDtypeStruct((rows, share * HD), jnp.bfloat16)] * n
        + [jax.ShapeDtypeStruct((2 * share, rows), jnp.float32)] * n,
        cost_estimate=pl.CostEstimate(
            flops=4 * n * share * rows * key_count * HD,
            bytes_accessed=4 * n * share * key_count * HD,
            transcendentals=n * share * rows * key_count,
        ),
        name="attend",
    )(info, queries, keys, values, cosine, sine)
    return list(zip(result[:n], result[n:]))


def merge_kernel(count, share, *refs):
    outs, stats, out_ref = refs[:count], refs[count : 2 * count], refs[2 * count]
    rows = out_ref.shape[0]
    maxima = [s[:share] for s in stats]
    totals = [s[share:] for s in stats]
    top = functools.reduce(jnp.maximum, maxima)
    factors = [jnp.exp(m - top) for m in maxima]
    total = sum(f * s for f, s in zip(factors, totals))
    scales = [f / total for f in factors]
    pad = -(count * share) % LANES
    table = jnp.concatenate(scales + [jnp.zeros((pad, rows), jnp.float32)], axis=0).T
    for head in range(share):
        at = slice(head * HD, (head + 1) * HD)
        value = sum(
            o[:, at].astype(jnp.float32) * table[:, i * share + head : i * share + head + 1]
            for i, o in enumerate(outs)
        )
        out_ref[:, at] = value.astype(jnp.bfloat16)


def merge(outs, stats, share):
    rows, width = outs[0].shape
    return pl.pallas_call(
        functools.partial(merge_kernel, len(outs), share),
        out_shape=jax.ShapeDtypeStruct((rows, width), jnp.bfloat16),
        cost_estimate=cost(4 * len(outs) * rows * width, 0, *outs, *stats),
        name="merge",
    )(*outs, *stats)


def project_kernel(chained, info, a_ref, w_ref, *refs):
    value = jnp.dot(a_ref[...], w_ref[...], preferred_element_type=jnp.float32)
    if chained:
        value = value + refs[0][...]
    refs[-1][...] = value


def project(part, weight, block, total):
    rows, depth = part.shape
    columns = weight.shape[1]
    tile = min(columns, 512)
    chained = total is not None
    spec = pl.BlockSpec((rows, tile), lambda i, info: (0, i))
    return pl.pallas_call(
        functools.partial(project_kernel, chained),
        grid_spec=pltpu.PrefetchScalarGridSpec(
            num_scalar_prefetch=1,
            grid=(columns // tile,),
            in_specs=[
                whole((rows, depth)),
                pl.BlockSpec((depth, tile), lambda i, info: (info[0], i)),
            ]
            + [spec] * chained,
            out_specs=spec,
        ),
        out_shape=jax.ShapeDtypeStruct((rows, columns), jnp.float32),
        cost_estimate=pl.CostEstimate(
            flops=2 * rows * depth * columns, bytes_accessed=2 * depth * columns, transcendentals=0
        ),
        name="project",
    )(block.astype(jnp.int32)[None], part, weight, *([total] if chained else []))


def condition_kernel(shards, own_rows, info, mine_ref, residual_ref, gain_ref, *refs):
    weights, out_ref = refs[:shards], refs[shards]
    hidden = residual_ref[...].astype(jnp.float32) + mine_ref[...]
    squares = jnp.sum(hidden * hidden, axis=1, keepdims=True)
    scaled = (hidden * gain_ref[...]).astype(jnp.bfloat16)
    width = weights[0].shape[1]
    for s, weight in enumerate(weights):
        part = jnp.dot(scaled, weight[...], preferred_element_type=jnp.float32)
        start = (info[0] ^ s) * width
        if width % LANES == 0:
            out_ref[:, pl.ds(pl.multiple_of(start, LANES), width)] = part
        else:
            out_ref[:, s * width : (s + 1) * width] = part
    out_ref[:, shards * width :] = jnp.broadcast_to(squares, (squares.shape[0], LANES))


def condition_part(mine, residual, gain, weights, own_rows, h):
    rows, depth = mine.shape
    width = weights[0].shape[1] * len(weights)
    return pl.pallas_call(
        functools.partial(condition_kernel, len(weights), own_rows),
        grid_spec=pltpu.PrefetchScalarGridSpec(
            num_scalar_prefetch=1,
            grid=(1,),
            in_specs=[
                whole((rows, depth)),
                pl.BlockSpec((rows, depth), lambda i, info: (info[0], 0)),
                whole((1, depth)),
            ]
            + [whole(w.shape) for w in weights],
            out_specs=whole((rows, width + LANES)),
        ),
        out_shape=jax.ShapeDtypeStruct((rows, width + LANES), jnp.float32),
        cost_estimate=cost(2 * rows * depth * width, 0, *weights),
        name="condition",
    )(h.astype(jnp.int32)[None], mine, residual, gain[None, :], *weights)


def sweep_kernel(
    sizes, steps, condition_ref, embed_ref, start_ref, noise_ref, in_ref, head_ref, out_ref
):
    times, rows = sizes
    start = start_ref[...]
    chan = start.shape[1]
    noise = [
        steps[times + i] * noise_ref[i * rows : (i + 1) * rows].astype(jnp.float32)
        for i in range(times - 1)
    ]

    def drift_of(first, preact):
        last = first + len(preact)
        inside = jnp.concatenate(
            [
                p + condition_ref[...] + embed_ref[i : i + 1]
                for i, p in zip(range(first, last), preact)
            ],
            axis=0,
        )
        action = (inside * jax.nn.sigmoid(inside)).astype(jnp.bfloat16)
        drift = jnp.dot(action, head_ref[...], preferred_element_type=jnp.float32)
        return [
            steps[i] * drift[(i - first) * rows : (i - first + 1) * rows] + noise[i]
            for i in range(first, last)
        ]

    opening = jnp.dot(start.astype(jnp.bfloat16), in_ref[...], preferred_element_type=jnp.float32)
    increments = drift_of(0, [opening] * (times - 1))
    for sweep in range(1, SWEEPS + 1):
        change = [jnp.zeros((rows, chan), jnp.float32)]
        for i in range(times - 1):
            change.append(change[-1] + increments[i])
        if sweep == SWEEPS or sweep >= times - 1:
            break
        states = jnp.concatenate(
            [start + change[i] for i in range(sweep, times - 1)], axis=0
        ).astype(jnp.bfloat16)
        product = jnp.dot(states, in_ref[...], preferred_element_type=jnp.float32)
        increments = increments[:sweep] + drift_of(
            sweep, [product[i * rows : (i + 1) * rows] for i in range(times - 1 - sweep)]
        )
    for i in range(times):
        out_ref[i * rows : (i + 1) * rows] = change[i].astype(jnp.bfloat16)


def sweep_all(condition, embedding, steps, start, noise, in_weight, head_out):
    rows, chan = start.shape
    times = noise.shape[0] // rows
    vmem = pl.BlockSpec(memory_space=pltpu.VMEM)
    return pl.pallas_call(
        functools.partial(sweep_kernel, (times, rows)),
        in_specs=[pl.BlockSpec(memory_space=pltpu.SMEM)] + [vmem] * 6,
        out_specs=vmem,
        out_shape=jax.ShapeDtypeStruct((times * rows, chan), jnp.bfloat16),
        cost_estimate=cost(
            12 * times * rows * chan * in_weight.shape[1], 0, in_weight, head_out
        ),
        name="sweeps",
    )(steps, condition, embedding, start, noise, in_weight, head_out)


def finish_kernel(sizes, info, start_ref, *refs):
    time_each, rows = sizes
    parts, out_ref = refs[:-1], refs[-1]
    for s, part in enumerate(parts):
        first = (info[0] ^ s) * rows
        start = start_ref[info[0] ^ s]
        for i in range(time_each):
            out_ref[pl.ds(first, rows), i, :] = start + part[i * rows : (i + 1) * rows].astype(
                jnp.float32
            )


def finish(start_state, parts, t, time_each):
    rows, chan = start_state.shape
    own_rows = rows // len(parts)
    vmem = pl.BlockSpec(memory_space=pltpu.VMEM)
    return pl.pallas_call(
        functools.partial(finish_kernel, (time_each, own_rows)),
        in_specs=[pl.BlockSpec(memory_space=pltpu.SMEM)] + [vmem] * (1 + len(parts)),
        out_specs=vmem,
        out_shape=jax.ShapeDtypeStruct((rows, time_each, chan), jnp.float32),
        name="finish",
    )(t.astype(jnp.int32)[None], start_state.reshape(len(parts), own_rows, chan), *parts)


def shards(
    queries,
    cache_keys,
    cache_values,
    residual,
    out_weight,
    norm_gain,
    cond_weight,
    in_weight,
    head_out,
    start_state,
    noise_draws,
    positions,
    cache_length,
    plan,
):
    rows, width = queries.shape
    n_heads = lax.axis_size("heads")
    n_tm = lax.axis_size("tm")
    h = lax.axis_index("heads")
    t = lax.axis_index("tm")
    local_heads = width // HD
    key_count = cache_keys.shape[0]
    model = out_weight.shape[1] * n_tm
    row_each, time_each, chan = noise_draws.shape
    own_rows = row_each // n_tm
    times = time_each * n_tm
    hidden_width = in_weight.shape[1]

    head_cuts = math.gcd(local_heads, n_tm)
    row_cuts = n_tm // head_cuts
    share = local_heads // head_cuts
    own_cut, own_row_cut = t // row_cuts, t % row_cuts

    def cut(values, index, axis):
        if row_cuts == 1:
            return values
        size = values.shape[axis] // row_cuts
        return lax.dynamic_slice_in_dim(values, index * size, size, axis)

    cosine, sine = rotation_tables(positions)
    valid_count = cache_length[0] - t * key_count
    order = list(range(head_cuts))[::-1]
    half = max(1, head_cuts // 2)
    outs, stats = [None] * n_tm, [None] * n_tm
    for groups in (order[:half], order[half:]):
        if not groups:
            continue
        blocks = attend(
            queries, cache_keys, cache_values, cosine, sine, own_cut, valid_count, groups, share
        )
        for a, (out, stat) in zip(groups, blocks):
            for b in range(row_cuts):
                s = a * row_cuts + b
                outs[s] = cut(out, own_row_cut ^ b, 0)
                stats[s] = cut(stat, own_row_cut ^ b, 1)
                if s:
                    outs[s], stats[s] = swap(outs[s], "tm", s), swap(stats[s], "tm", s)
    attended = merge(outs, stats, share)
    parts = [attended] + [swap(attended, "tm", s) for s in range(1, n_tm)]
    projected = None
    for a in range(head_cuts):
        part = parts[a * row_cuts : (a + 1) * row_cuts]
        if row_cuts > 1:
            part = jnp.take(jnp.stack(part), jnp.arange(row_cuts) ^ own_row_cut, axis=0)
            part = part.reshape(rows, share * HD)
        else:
            part = part[0]
        projected = project(part, out_weight, own_cut ^ a, projected)

    chips = n_heads // 2
    blocks = projected.reshape(chips, 2, row_each, -1).transpose(1, 0, 2, 3)
    core, chip = h % 2, h // 2
    pair = pick(blocks, core) + swap(
        pick(blocks, 1 - core).astype(jnp.bfloat16), "heads", 1
    ).astype(jnp.float32)
    mine = pick(pair, chip)
    for s in range(1, chips):
        mine = mine + swap(pick(pair, chip ^ s).astype(jnp.bfloat16), "heads", 2 * s).astype(
            jnp.float32
        )

    far = [cond_weight] + [swap(cond_weight, "heads", 2 * s) for s in range(1, chips)]
    near = [swap(w, "heads", 1) for w in far]
    cond_shards = [w for pair in zip(far, near) for w in pair]
    cond = condition_part(mine, residual, norm_gain, cond_shards, own_rows, h)
    cond_blocks = cond.reshape(n_tm, own_rows, -1)
    cond_sum = pick(cond_blocks, t) + sum(
        swap(pick(cond_blocks, t ^ s), "tm", s) for s in range(1, n_tm)
    )
    inverse = lax.rsqrt(cond_sum[:, hidden_width] / model + 1e-06)
    condition = cond_sum[:, :hidden_width]
    if cond_weight.shape[1] % LANES:
        condition = condition.reshape(own_rows, n_heads, -1)
        condition = jnp.take(condition, jnp.arange(n_heads) ^ h, axis=1)
        condition = condition.reshape(own_rows, hidden_width)
    condition = condition * inverse[:, None]

    noise_blocks = noise_draws.reshape(n_tm, own_rows, time_each, chan)
    noise = jnp.stack(
        [pick(noise_blocks, t)]
        + [swap(pick(noise_blocks, t ^ s), "tm", s) for s in range(1, n_tm)]
    )
    noise = jnp.take(noise, jnp.arange(n_tm) ^ t, axis=0)
    noise = noise.transpose(0, 2, 1, 3).reshape(times * own_rows, chan)
    levels = plan.astype(jnp.float32)
    half_width = hidden_width // 2
    frequencies = jnp.exp(
        -math.log(10000.0) * jnp.arange(half_width, dtype=jnp.float32) / half_width
    )
    angles = levels[:-1, None] * frequencies[None, :]
    embedding = jnp.concatenate([jnp.sin(angles), jnp.cos(angles)], axis=1)
    step_size = (levels[:-1] - levels[1:]) / 1000.0
    steps = jnp.concatenate([step_size, jnp.sqrt(step_size)])
    start = lax.dynamic_slice_in_dim(start_state, t * own_rows, own_rows, 0)
    change = sweep_all(condition, embedding, steps, start, noise, in_weight, head_out)
    change_blocks = change.reshape(n_tm, time_each * own_rows, chan)
    back = [pick(change_blocks, t)] + [
        swap(pick(change_blocks, t ^ s), "tm", s) for s in range(1, n_tm)
    ]
    return finish(start_state, back, t, time_each)


def solution(mesh):
    placed = (
        P("groups", "heads"),
        P(("groups", "tm"), "heads"),
        P(("groups", "tm"), "heads"),
        P("groups", "tm"),
        P("heads", "tm"),
        P("tm"),
        P("tm", "heads"),
        P(),
        P(),
        P(("groups", "heads"), None),
        P(("groups", "heads"), "tm", None),
        P("groups"),
        P("groups"),
        P(),
    )
    return jax.shard_map(
        shards,
        mesh=mesh,
        in_specs=placed,
        out_specs=P(("groups", "heads"), "tm", None),
        check_vma=False,
    )
```

```python
import functools
import math

import jax
import jax.numpy as jnp
import numpy as np
from jax import lax
from jax.experimental import pallas as pl
from jax.experimental.pallas import tpu as pltpu
from jax.sharding import PartitionSpec as P

HD = 128
SWEEPS = 3
LANES = 128


def swap(values, axis, distance):
    size = lax.axis_size(axis)
    return lax.ppermute(values, axis, [(i, i ^ distance) for i in range(size)])


def pick(values, index):
    return lax.dynamic_index_in_dim(values, index, 0, False)


def cost(flops, transcendentals, *arrays):
    moved = sum(math.prod(a.shape) * jnp.dtype(a.dtype).itemsize for a in arrays)
    return pl.CostEstimate(flops=flops, bytes_accessed=moved, transcendentals=transcendentals)


def mib(count):
    return pltpu.CompilerParams(vmem_limit_bytes=count * 1024 * 1024)


VMEM = pl.BlockSpec(memory_space=pltpu.VMEM)
SMEM = pl.BlockSpec(memory_space=pltpu.SMEM)
HBM = pl.BlockSpec(memory_space=pltpu.HBM)
PIECES = 3


def pieces_of(value):
    high = value.astype(jnp.bfloat16)
    rest = value - high.astype(jnp.float32)
    middle = rest.astype(jnp.bfloat16)
    return high, middle, (rest - middle.astype(jnp.float32)).astype(jnp.bfloat16)


def sum_pieces(pieces):
    high, middle, low = (p.astype(jnp.float32) for p in pieces)
    return high + (middle + low)


def packed(rows, width, share):
    return PIECES * rows <= width and 2 * share <= 8 and rows % LANES == 0


def attend_kernel(
    groups, share, per_copy, row_cuts, length_ref, freq_ref, pos_ref, q_ref, k_hbm, v_hbm, *refs
):
    count = len(groups)
    outs, stats = refs[:count], refs[count:-6]
    k_buf, v_buf, k_sem, v_sem, cos_ref, sin_ref = refs[-6:]
    rows = q_ref.shape[0]
    keys = k_hbm.shape[0]
    t = lax.axis_index("tm")
    own = t // row_cuts
    width = per_copy * HD
    copies = []
    for g, a in enumerate(groups):
        for part in range(share // per_copy):
            slot = len(copies)
            column = pl.multiple_of(((own ^ a) * share + part * per_copy) * HD, HD)
            pair = [
                pltpu.make_async_copy(hbm.at[:, pl.ds(column, width)], buf.at[slot], sem.at[slot])
                for hbm, buf, sem in ((k_hbm, k_buf, k_sem), (v_hbm, v_buf, v_sem))
            ]
            for copy in pair:
                copy.start()
            copies.append((g, part, column, pair))

    even = lax.broadcasted_iota(jnp.int32, (rows, HD), 1) % 2 == 0
    place = jnp.broadcast_to(pos_ref[...].astype(jnp.float32), (HD, rows)).T
    angles = place * freq_ref[...]
    cos_ref[...] = jnp.cos(angles)
    sine = jnp.sin(angles)
    sin_ref[...] = jnp.where(even, -sine, sine)
    lane = lax.broadcasted_iota(jnp.int32, (rows, LANES), 1)
    valid = lax.broadcasted_iota(jnp.int32, (1, keys), 1) < length_ref[0] - t * keys
    scale = 1.0 / math.sqrt(HD)
    held = jnp.zeros((rows, LANES), jnp.float32)
    for slot, (g, part, column, pair) in enumerate(copies):
        for copy in pair:
            copy.wait()
        for i in range(per_copy):
            head = part * per_copy + i
            at = slice(i * HD, (i + 1) * HD)
            to = slice(head * HD, (head + 1) * HD)
            from_column = pl.multiple_of(column + i * HD, HD)
            wide = q_ref[:, pl.ds(from_column, HD)].astype(jnp.float32)
            partner = jnp.where(even, pltpu.roll(wide, HD - 1, 1), pltpu.roll(wide, 1, 1))
            rotated = (wide * cos_ref[...] + partner * sin_ref[...]).astype(jnp.bfloat16)
            scores = lax.dot_general(
                rotated,
                k_buf[slot, :, at],
                (((1,), (1,)), ((), ())),
                preferred_element_type=jnp.float32,
            )
            scores = jnp.where(valid, scores, jnp.float32(-1e30))
            block_max = jnp.maximum(jnp.max(scores, axis=1, keepdims=True), -1e29)
            weights = jnp.exp((scores - block_max) * scale)
            block_total = jnp.sum(weights, axis=1, keepdims=True)
            block_out = jnp.dot(
                weights.astype(jnp.bfloat16),
                v_buf[slot, :, at],
                preferred_element_type=jnp.float32,
            )
            outs[g][:rows, to] = block_out.astype(jnp.bfloat16)
            held = jnp.where(lane == head, block_max * scale, held)
            held = jnp.where(lane == share + head, block_total, held)
        if part == share // per_copy - 1:
            flat = held.T
            if stats:
                stats[g][...] = flat[: 2 * share]
            else:
                extra = outs[g].shape[0] - rows
                for p, piece in enumerate(pieces_of(flat[:extra])):
                    outs[g][rows:, p * rows : (p + 1) * rows] = piece


def attend(queries, keys, values, positions, cache_length, groups, share, row_cuts):
    rows = queries.shape[0]
    key_count = keys.shape[0]
    per_copy = 2 if share % 2 == 0 else 1
    n = len(groups)
    slots = n * share // per_copy
    wide = share * HD
    joined = row_cuts == 1 and packed(rows, wide, share)
    frequencies = np.exp(-math.log(10000.0) * 2.0 * (np.arange(HD) // 2) / HD)
    buffer = pltpu.VMEM((slots, key_count, per_copy * HD), jnp.bfloat16)
    out_shape = [jax.ShapeDtypeStruct((rows + 8 * joined, wide), jnp.bfloat16)] * n
    if not joined:
        out_shape = out_shape + [jax.ShapeDtypeStruct((2 * share, rows), jnp.float32)] * n
    result = pl.pallas_call(
        functools.partial(attend_kernel, groups, share, per_copy, row_cuts),
        in_specs=[SMEM, VMEM, VMEM, VMEM, HBM, HBM],
        out_specs=[VMEM] * len(out_shape),
        out_shape=out_shape,
        scratch_shapes=[
            buffer,
            buffer,
            pltpu.SemaphoreType.DMA((slots,)),
            pltpu.SemaphoreType.DMA((slots,)),
            pltpu.VMEM((rows, HD), jnp.float32),
            pltpu.VMEM((rows, HD), jnp.float32),
        ],
        cost_estimate=pl.CostEstimate(
            flops=4 * n * share * rows * key_count * HD,
            bytes_accessed=4 * n * share * key_count * HD,
            transcendentals=n * share * rows * key_count,
        ),
        compiler_params=mib(60),
        name="attend",
    )(cache_length, frequencies.astype(np.float32)[None], positions[None], queries, keys, values)
    return list(zip(result[:n], result[n:] if not joined else [None] * n))


def merge_kernel(count, share, *refs):
    out_ref = refs[-1]
    rows = out_ref.shape[0]
    outs, stats = refs[:count], refs[count:-1]
    if stats:
        tables = [s[...] for s in stats]
    else:
        tables = [
            sum_pieces([o[rows:, p * rows : (p + 1) * rows] for p in range(PIECES)]) for o in outs
        ]
    maxima = [s[:share] for s in tables]
    totals = [s[share : 2 * share] for s in tables]
    top = functools.reduce(jnp.maximum, maxima)
    factors = [jnp.exp(m - top) for m in maxima]
    total = sum(f * s for f, s in zip(factors, totals))
    scales = [f / total for f in factors]
    pad = -(count * share) % LANES
    table = jnp.concatenate(scales + [jnp.zeros((pad, rows), jnp.float32)], axis=0).T
    for head in range(share):
        at = slice(head * HD, (head + 1) * HD)
        value = sum(
            o[:rows, at].astype(jnp.float32) * table[:, i * share + head : i * share + head + 1]
            for i, o in enumerate(outs)
        )
        out_ref[:, at] = value.astype(jnp.bfloat16)


def merge(outs, stats, share, rows):
    width = outs[0].shape[1]
    stats = [s for s in stats if s is not None]
    return pl.pallas_call(
        functools.partial(merge_kernel, len(outs), share),
        in_specs=[VMEM] * (len(outs) + len(stats)),
        out_specs=VMEM,
        out_shape=jax.ShapeDtypeStruct((rows, width), jnp.bfloat16),
        cost_estimate=cost(4 * len(outs) * rows * width, 0, *outs, *stats),
        compiler_params=mib(4),
        name="merge",
    )(*outs, *stats)


def project_kernel(head_cuts, row_cuts, cuts, chained, last, *refs):
    parts, refs = refs[: len(cuts)], refs[len(cuts) :]
    w_ref, refs = refs[0], refs[1:]
    own = lax.axis_index("tm") // row_cuts
    depth = parts[0].shape[1]
    value = refs[0][...] if chained else None
    for a, part in zip(cuts, parts):
        first = pl.multiple_of((own ^ a) * depth, depth)
        product = jnp.dot(part[...], w_ref[pl.ds(first, depth), :], preferred_element_type=jnp.float32)
        value = product if value is None else value + product
    if not last:
        refs[-1][...] = value
        return
    keep_ref, send_ref, whole_ref = refs[chained:]
    chips, rows = keep_ref.shape[:2]
    core = lax.axis_index("heads") % 2
    for chip in range(chips):
        for c in range(2):
            first = (2 * chip + c) * rows
            whole_ref[c, chip] = value[first : first + rows]
    keep_ref[...] = whole_ref[core]
    send_ref[...] = whole_ref[1 - core].astype(jnp.bfloat16)


def project(parts, cuts, weight, total, row_cuts, chips):
    rows, depth = parts[0].shape
    columns = weight.shape[1]
    chained = total is not None
    last = chips > 0
    if last:
        block = (chips, rows // (2 * chips), columns)
        out_shape = [
            jax.ShapeDtypeStruct(block, jnp.float32),
            jax.ShapeDtypeStruct(block, jnp.bfloat16),
        ]
        scratch = [pltpu.VMEM((2, *block), jnp.float32)]
    else:
        out_shape, scratch = jax.ShapeDtypeStruct((rows, columns), jnp.float32), []
    return pl.pallas_call(
        functools.partial(project_kernel, None, row_cuts, cuts, chained, last),
        in_specs=[VMEM] * (len(parts) + 1 + chained),
        out_specs=[VMEM, VMEM] if last else VMEM,
        out_shape=out_shape,
        scratch_shapes=scratch,
        cost_estimate=pl.CostEstimate(
            flops=2 * len(parts) * rows * depth * columns,
            bytes_accessed=2 * len(parts) * depth * columns,
            transcendentals=0,
        ),
        compiler_params=mib(20),
        name="project",
    )(*parts, weight, *([total] if chained else []))


def pair_kernel(keep_ref, got_ref, mine_ref, *send_refs):
    chip = lax.axis_index("heads") // 2
    mine_ref[...] = keep_ref[chip] + got_ref[chip].astype(jnp.float32)
    for s, send_ref in enumerate(send_refs, 1):
        send_ref[...] = (keep_ref[chip ^ s] + got_ref[chip ^ s].astype(jnp.float32)).astype(
            jnp.bfloat16
        )


def pair_sum(keep, got):
    chips, rows, columns = keep.shape
    result = pl.pallas_call(
        pair_kernel,
        in_specs=[VMEM] * 2,
        out_specs=[VMEM] * chips,
        out_shape=[jax.ShapeDtypeStruct((rows, columns), jnp.float32)]
        + [jax.ShapeDtypeStruct((rows, columns), jnp.bfloat16)] * (chips - 1),
        cost_estimate=cost(chips * rows * columns, 0, keep, got),
        compiler_params=mib(8),
        name="pair",
    )(keep, got)
    return result[0], result[1:]


def condition_kernel(chips, shards, own_rows, mine_ref, residual_ref, gain_ref, *refs):
    got, refs = refs[: chips - 1], refs[chips - 1 :]
    weights, refs = refs[:shards], refs[shards:]
    rows = mine_ref.shape[0]
    h = lax.axis_index("heads")
    hidden = residual_ref[h].astype(jnp.float32) + mine_ref[...]
    for ref in got:
        hidden = hidden + ref[...].astype(jnp.float32)
    squares = jnp.sum(hidden * hidden, axis=1, keepdims=True)
    scaled = (hidden * gain_ref[...]).astype(jnp.bfloat16)
    width = weights[0].shape[1]
    products = [jnp.dot(scaled, w[...], preferred_element_type=jnp.float32) for w in weights]
    tail = jnp.zeros((rows, LANES), jnp.float32)
    lane = lax.broadcasted_iota(jnp.int32, (rows, LANES), 1)
    for p, piece in enumerate(pieces_of(squares)):
        tail = jnp.where(lane == p, piece.astype(jnp.float32), tail)
    if own_rows % 8 == 0 and width % LANES == 0:
        outs, held = refs[:-1], refs[-1]
        t = lax.axis_index("tm")
        for s, product in enumerate(products):
            held[:, pl.ds(pl.multiple_of((h ^ s) * width, LANES), width)] = product
        held[:, shards * width :] = tail
        for s, out_ref in enumerate(outs):
            first = pl.multiple_of((t ^ s) * own_rows, own_rows)
            out_ref[...] = held[pl.ds(first, own_rows), :].astype(jnp.bfloat16)
    else:
        for s, product in enumerate(products):
            refs[0][:, s * width : (s + 1) * width] = product.astype(jnp.bfloat16)
        refs[0][:, shards * width :] = tail.astype(jnp.bfloat16)


def condition_parts(mine, got, residual, gain, weights, n_tm, h, t):
    rows, depth = mine.shape
    shards = len(weights)
    width = weights[0].shape[1]
    full = shards * width + LANES
    own_rows = rows // n_tm
    aligned = own_rows % 8 == 0 and width % LANES == 0
    block = jax.ShapeDtypeStruct((own_rows, full), jnp.bfloat16)
    out_shape = [block] * n_tm if aligned else [jax.ShapeDtypeStruct((rows, full), jnp.bfloat16)]
    result = pl.pallas_call(
        functools.partial(condition_kernel, len(got) + 1, shards, own_rows),
        in_specs=[VMEM] * (3 + len(got) + shards),
        out_specs=[VMEM] * len(out_shape),
        out_shape=out_shape,
        scratch_shapes=[pltpu.VMEM((rows, full), jnp.float32)] * aligned,
        cost_estimate=cost(2 * rows * depth * full, 0, *weights),
        compiler_params=mib(12),
        name="condition",
    )(mine, residual.reshape(-1, rows, depth), gain[None, :], *got, *weights)
    if aligned:
        return result
    columns = result[0][:, :-LANES].reshape(rows, shards, width)
    columns = jnp.take(columns, jnp.arange(shards) ^ h, axis=1).reshape(rows, shards * width)
    result = jnp.concatenate([columns, result[0][:, -LANES:]], axis=1)
    result = result.reshape(n_tm, own_rows, full)
    return [pick(result, t ^ s) for s in range(n_tm)]


def sweep_kernel(sizes, steps, start_ref, embed_ref, in_ref, head_ref, *refs):
    n_tm, time_each, rows, model = sizes
    noise_refs, refs = refs[:n_tm], refs[n_tm:]
    parts, refs = refs[:n_tm], refs[n_tm:]
    outs, held = refs[:n_tm], refs[n_tm]
    t = lax.axis_index("tm")
    times = n_tm * time_each
    start = start_ref[t]
    chan = start.shape[1]
    for s, ref in enumerate(noise_refs):
        held[t ^ s] = ref[...].astype(jnp.float32)

    def block(i):
        at = (i % time_each) * rows
        return i // time_each, slice(at, at + rows)

    noise = [steps[times + i] * held[block(i)] for i in range(times - 1)]
    width = in_ref.shape[1]
    opening = jnp.dot(start.astype(jnp.bfloat16), in_ref[...], preferred_element_type=jnp.float32)
    total = sum(p[...].astype(jnp.float32) for p in parts)
    squares = total[:, width : width + 1]
    for p in range(1, PIECES):
        squares = squares + total[:, width + p : width + p + 1]
    condition = total[:, :width] * lax.rsqrt(squares / model + 1e-06)

    def increments_at(first, products):
        last = first + len(products)
        inside = jnp.concatenate(
            [p + (condition + embed_ref[i : i + 1]) for i, p in enumerate(products, first)], axis=0
        )
        action = (inside * jax.nn.sigmoid(inside)).astype(jnp.bfloat16)
        drift = jnp.dot(action, head_ref[...], preferred_element_type=jnp.float32)
        return [
            steps[i] * drift[(i - first) * rows : (i - first + 1) * rows] + noise[i]
            for i in range(first, last)
        ]

    increments = increments_at(0, [opening] * (times - 1))
    for sweep in range(1, SWEEPS + 1):
        change = [jnp.zeros((rows, chan), jnp.float32)]
        for i in range(times - 1):
            change.append(change[-1] + increments[i])
        if sweep == SWEEPS or sweep >= times - 1:
            break
        states = jnp.concatenate([start + change[i] for i in range(sweep, times - 1)], axis=0)
        product = jnp.dot(
            states.astype(jnp.bfloat16), in_ref[...], preferred_element_type=jnp.float32
        )
        increments = increments[:sweep] + increments_at(
            sweep, [product[i * rows : (i + 1) * rows] for i in range(times - 1 - sweep)]
        )
    for i in range(times):
        held[block(i)] = change[i]
    for s, out_ref in enumerate(outs):
        out_ref[...] = held[t ^ s].astype(jnp.bfloat16)


def sweep_all(parts, noise, embedding, steps, start, in_weight, head_out, time_each, model):
    n_tm, rows, chan = start.shape
    block = (time_each * rows, chan)
    return pl.pallas_call(
        functools.partial(sweep_kernel, (n_tm, time_each, rows, model)),
        in_specs=[SMEM] + [VMEM] * (4 + 2 * n_tm),
        out_specs=[VMEM] * n_tm,
        out_shape=[jax.ShapeDtypeStruct(block, jnp.bfloat16)] * n_tm,
        scratch_shapes=[pltpu.VMEM((n_tm, *block), jnp.float32)],
        cost_estimate=cost(
            10 * n_tm * time_each * rows * chan * in_weight.shape[1], 0, in_weight, head_out
        ),
        compiler_params=mib(16),
        name="sweeps",
    )(steps, start, embedding, in_weight, head_out, *noise, *parts)


def finish_kernel(sizes, start_ref, *refs):
    time_each, rows = sizes
    parts, out_ref = refs[:-1], refs[-1]
    t = lax.axis_index("tm")
    for s, part in enumerate(parts):
        start = start_ref[t ^ s]
        for i in range(time_each):
            out_ref[pl.ds((t ^ s) * rows, rows), i, :] = start + part[
                i * rows : (i + 1) * rows
            ].astype(jnp.float32)


def finish(start, parts, time_each):
    n_tm, rows, chan = start.shape
    return pl.pallas_call(
        functools.partial(finish_kernel, (time_each, rows)),
        in_specs=[VMEM] * (1 + len(parts)),
        out_specs=VMEM,
        out_shape=jax.ShapeDtypeStruct((n_tm * rows, time_each, chan), jnp.float32),
        cost_estimate=cost(n_tm * rows * time_each * chan, 0, start, *parts),
        compiler_params=mib(4),
        name="finish",
    )(start, *parts)


def shards(
    queries,
    cache_keys,
    cache_values,
    residual,
    out_weight,
    norm_gain,
    cond_weight,
    in_weight,
    head_out,
    start_state,
    noise_draws,
    positions,
    cache_length,
    plan,
):
    rows, width = queries.shape
    n_heads = lax.axis_size("heads")
    n_tm = lax.axis_size("tm")
    h = lax.axis_index("heads")
    t = lax.axis_index("tm")
    local_heads = width // HD
    model = out_weight.shape[1] * n_tm
    row_each, time_each, chan = noise_draws.shape
    own_rows = row_each // n_tm
    hidden_width = in_weight.shape[1]

    head_cuts = math.gcd(local_heads, n_tm)
    row_cuts = n_tm // head_cuts
    share = local_heads // head_cuts
    own_cut, own_row_cut = t // row_cuts, t % row_cuts

    def cut(values, index, axis):
        if row_cuts == 1:
            return values
        size = values.shape[axis] // row_cuts
        return lax.dynamic_slice_in_dim(values, index * size, size, axis)

    order = list(range(head_cuts))[::-1]
    half = max(1, head_cuts // 2)
    outs, stats = [None] * n_tm, [None] * n_tm
    for groups in (order[:half], order[half:]):
        if not groups:
            continue
        blocks = attend(
            queries, cache_keys, cache_values, positions, cache_length, groups, share, row_cuts
        )
        for a, (out, stat) in zip(groups, blocks):
            for b in range(row_cuts):
                s = a * row_cuts + b
                outs[s] = cut(out, own_row_cut ^ b, 0)
                stats[s] = None if stat is None else cut(stat, own_row_cut ^ b, 1)
                if s:
                    outs[s] = swap(outs[s], "tm", s)
                    stats[s] = None if stat is None else swap(stats[s], "tm", s)
    attended = merge(outs, stats, share, rows // row_cuts)
    chips = n_heads // 2

    far = [cond_weight] + [swap(cond_weight, "heads", 2 * s) for s in range(1, chips)]
    far, attended = lax.optimization_barrier((far, attended))
    near = [swap(w, "heads", 1) for w in far]
    cond_shards = [w for pair in zip(far, near) for w in pair]

    parts = [attended] + [swap(attended, "tm", s) for s in range(1, n_tm)]
    projected = None
    for a in range(head_cuts):
        part = parts[a * row_cuts : (a + 1) * row_cuts]
        if row_cuts > 1:
            part = jnp.take(jnp.stack(part), jnp.arange(row_cuts) ^ own_row_cut, axis=0)
            part = part.reshape(rows, share * HD)
        else:
            part = part[0]
        projected = project(
            [part], [a], out_weight, projected, row_cuts, chips if a == head_cuts - 1 else 0
        )

    keep, send = projected
    mine, far_rows = pair_sum(keep, swap(send, "heads", 1))
    got = [swap(r, "heads", 2 * s) for s, r in enumerate(far_rows, 1)]

    cond = condition_parts(mine, got, residual, norm_gain, cond_shards, n_tm, h, t)
    cond = [cond[0]] + [swap(cond[s], "tm", s) for s in range(1, n_tm)]

    noise_rows = noise_draws.transpose(1, 0, 2).reshape(time_each, n_tm, own_rows, chan)
    noise = [
        lax.dynamic_index_in_dim(noise_rows, t ^ s, 1, False).reshape(time_each * own_rows, chan)
        for s in range(n_tm)
    ]
    noise = [noise[0]] + [swap(noise[s], "tm", s) for s in range(1, n_tm)]
    levels = plan.astype(jnp.float32)
    half_width = hidden_width // 2
    frequencies = jnp.exp(
        -math.log(10000.0) * jnp.arange(half_width, dtype=jnp.float32) / half_width
    )
    angles = levels[:-1, None] * frequencies[None, :]
    embedding = jnp.concatenate([jnp.sin(angles), jnp.cos(angles)], axis=1)
    step_size = (levels[:-1] - levels[1:]) / 1000.0
    steps = jnp.concatenate([step_size, jnp.sqrt(step_size)])
    start = start_state.reshape(n_tm, own_rows, chan)
    change = sweep_all(
        cond, noise, embedding, steps, start, in_weight, head_out, time_each, model
    )
    back = [change[0]] + [swap(change[s], "tm", s) for s in range(1, n_tm)]
    return finish(start, back, time_each)


def solution(mesh):
    placed = (
        P("groups", "heads"),
        P(("groups", "tm"), "heads"),
        P(("groups", "tm"), "heads"),
        P("groups", "tm"),
        P("heads", "tm"),
        P("tm"),
        P("tm", "heads"),
        P(),
        P(),
        P(("groups", "heads"), None),
        P(("groups", "heads"), "tm", None),
        P("groups"),
        P("groups"),
        P(),
    )
    return jax.shard_map(
        shards,
        mesh=mesh,
        in_specs=placed,
        out_specs=P(("groups", "heads"), "tm", None),
        check_vma=False,
    )
```

```python
import functools
import math

import jax
import jax.numpy as jnp
import numpy as np
from jax import lax
from jax.experimental import pallas as pl
from jax.experimental.pallas import tpu as pltpu
from jax.sharding import PartitionSpec as P


HD = 128
SWEEPS = 3
LANES = 128


def swap(values, axis, distance):
    size = lax.axis_size(axis)
    return lax.ppermute(values, axis, [(i, i ^ distance) for i in range(size)])


def exchange(blocks):
    got = [blocks[0]]
    for s, block in enumerate(blocks[1:], 1):
        got.append(swap(block, "tm", s))
    return got


def pick(values, index):
    return lax.dynamic_index_in_dim(values, index, 0, False)


def cost(flops, transcendentals, *arrays):
    moved = sum(math.prod(a.shape) * jnp.dtype(a.dtype).itemsize for a in arrays)
    return pl.CostEstimate(flops=flops, bytes_accessed=moved, transcendentals=transcendentals)


def mib(count):
    return pltpu.CompilerParams(vmem_limit_bytes=count * 1024 * 1024)


VMEM = pl.BlockSpec(memory_space=pltpu.VMEM)
SMEM = pl.BlockSpec(memory_space=pltpu.SMEM)
HBM = pl.BlockSpec(memory_space=pltpu.HBM)
PIECES = 3


def pieces_of(value):
    high = value.astype(jnp.bfloat16)
    rest = value - high.astype(jnp.float32)
    middle = rest.astype(jnp.bfloat16)
    return high, middle, (rest - middle.astype(jnp.float32)).astype(jnp.bfloat16)


def sum_pieces(pieces):
    high, middle, low = (p.astype(jnp.float32) for p in pieces)
    return high + (middle + low)


def packed(rows, width, share):
    return PIECES * rows <= width and 2 * share <= 8 and rows % LANES == 0


def calls_of(order):
    return [groups for groups in (order[:1], order[1:-1], order[-1:] if order[1:] else []) if groups]


def attend_kernel(
    groups, share, per_copy, row_cuts, length_ref, freq_hbm, pos_hbm, q_hbm, k_hbm, v_hbm, *refs
):
    count = len(groups)
    outs, stats = refs[:count], refs[count:-10]
    k_buf, v_buf, q_buf, freq_ref, pos_ref, k_sem, v_sem, q_sem, cos_ref, sin_ref = refs[-10:]
    rows = q_hbm.shape[0]
    keys = k_hbm.shape[0]
    t = lax.axis_index("tm")
    own = t // row_cuts
    width = per_copy * HD
    small = [
        pltpu.make_async_copy(freq_hbm, freq_ref, q_sem.at[count]),
        pltpu.make_async_copy(pos_hbm, pos_ref, q_sem.at[count + 1]),
    ]
    for copy in small:
        copy.start()
    copies, wanted = [], []
    for g, a in enumerate(groups):
        first = pl.multiple_of((own ^ a) * share * HD, HD)
        wanted.append(
            pltpu.make_async_copy(
                q_hbm.at[:, pl.ds(first, share * HD)], q_buf.at[g], q_sem.at[g]
            )
        )
        wanted[g].start()
        for part in range(share // per_copy):
            slot = len(copies)
            column = pl.multiple_of(((own ^ a) * share + part * per_copy) * HD, HD)
            pair = [
                pltpu.make_async_copy(hbm.at[:, pl.ds(column, width)], buf.at[slot], sem.at[slot])
                for hbm, buf, sem in ((k_hbm, k_buf, k_sem), (v_hbm, v_buf, v_sem))
            ]
            for copy in pair:
                copy.start()
            copies.append((g, part, pair))
    for copy in small:
        copy.wait()

    even = lax.broadcasted_iota(jnp.int32, (rows, HD), 1) % 2 == 0
    place = jnp.broadcast_to(pos_ref[...].astype(jnp.float32), (HD, rows)).T
    angles = place * freq_ref[...]
    cos_ref[...] = jnp.cos(angles)
    sine = jnp.sin(angles)
    sin_ref[...] = jnp.where(even, -sine, sine)
    lane = lax.broadcasted_iota(jnp.int32, (rows, LANES), 1)
    valid = lax.broadcasted_iota(jnp.int32, (1, keys), 1) < length_ref[0] - t * keys
    scale = 1.0 / math.sqrt(HD)
    held = jnp.zeros((rows, LANES), jnp.float32)
    for slot, (g, part, pair) in enumerate(copies):
        for copy in ([wanted[g]] if part == 0 else []) + pair:
            copy.wait()
        for i in range(per_copy):
            head = part * per_copy + i
            at = slice(i * HD, (i + 1) * HD)
            to = slice(head * HD, (head + 1) * HD)
            wide = q_buf[g, :, to].astype(jnp.float32)
            partner = jnp.where(even, pltpu.roll(wide, HD - 1, 1), pltpu.roll(wide, 1, 1))
            rotated = (wide * cos_ref[...] + partner * sin_ref[...]).astype(jnp.bfloat16)
            scores = lax.dot_general(
                rotated,
                k_buf[slot, :, at],
                (((1,), (1,)), ((), ())),
                preferred_element_type=jnp.float32,
            )
            scores = jnp.where(valid, scores, jnp.float32(-1e30))
            block_max = jnp.maximum(jnp.max(scores, axis=1, keepdims=True), -1e29)
            weights = jnp.exp((scores - block_max) * scale)
            block_total = jnp.sum(weights, axis=1, keepdims=True)
            block_out = jnp.dot(
                weights.astype(jnp.bfloat16),
                v_buf[slot, :, at],
                preferred_element_type=jnp.float32,
            )
            outs[g][:rows, to] = block_out.astype(jnp.bfloat16)
            held = jnp.where(lane == head, block_max * scale, held)
            held = jnp.where(lane == share + head, block_total, held)
        if part == share // per_copy - 1:
            flat = held.T
            if stats:
                stats[g][...] = flat[: 2 * share]
            else:
                extra = outs[g].shape[0] - rows
                for p, piece in enumerate(pieces_of(flat[:extra])):
                    outs[g][rows:, p * rows : (p + 1) * rows] = piece


def attend(queries, keys, values, positions, cache_length, groups, share, row_cuts):
    rows = queries.shape[0]
    key_count = keys.shape[0]
    per_copy = 2 if share % 2 == 0 else 1
    n = len(groups)
    slots = n * share // per_copy
    wide = share * HD
    joined = row_cuts == 1 and packed(rows, wide, share)
    frequencies = np.exp(-math.log(10000.0) * 2.0 * (np.arange(HD) // 2) / HD)
    buffer = pltpu.VMEM((slots, key_count, per_copy * HD), jnp.bfloat16)
    out_shape = [jax.ShapeDtypeStruct((rows + 8 * joined, wide), jnp.bfloat16)] * n
    if not joined:
        out_shape = out_shape + [jax.ShapeDtypeStruct((2 * share, rows), jnp.float32)] * n
    result = pl.pallas_call(
        functools.partial(attend_kernel, groups, share, per_copy, row_cuts),
        in_specs=[SMEM, HBM, HBM, HBM, HBM, HBM],
        out_specs=[VMEM] * len(out_shape),
        out_shape=out_shape,
        scratch_shapes=[
            buffer,
            buffer,
            pltpu.VMEM((n, rows, wide), jnp.bfloat16),
            pltpu.VMEM((1, HD), jnp.float32),
            pltpu.VMEM((1, rows), jnp.int32),
            pltpu.SemaphoreType.DMA((slots,)),
            pltpu.SemaphoreType.DMA((slots,)),
            pltpu.SemaphoreType.DMA((n + 2,)),
            pltpu.VMEM((rows, HD), jnp.float32),
            pltpu.VMEM((rows, HD), jnp.float32),
        ],
        cost_estimate=pl.CostEstimate(
            flops=4 * n * share * rows * key_count * HD,
            bytes_accessed=4 * n * share * key_count * HD,
            transcendentals=n * share * rows * key_count,
        ),
        compiler_params=mib(57 if groups[-1] == 0 else 60),
        name="attend",
    )(cache_length, frequencies.astype(np.float32)[None], positions[None], queries, keys, values)
    return list(zip(result[:n], result[n:] if not joined else [None] * n))


def merge_kernel(count, share, *refs):
    out_ref = refs[-1]
    rows = out_ref.shape[0]
    outs, stats = refs[:count], refs[count:-1]
    if stats:
        tables = [s[...] for s in stats]
    else:
        tables = [
            sum_pieces([o[rows:, p * rows : (p + 1) * rows] for p in range(PIECES)]) for o in outs
        ]
    maxima = [s[:share] for s in tables]
    totals = [s[share : 2 * share] for s in tables]
    top = functools.reduce(jnp.maximum, maxima)
    factors = [jnp.exp(m - top) for m in maxima]
    total = sum(f * s for f, s in zip(factors, totals))
    scales = [f / total for f in factors]
    pad = -(count * share) % LANES
    table = jnp.concatenate(scales + [jnp.zeros((pad, rows), jnp.float32)], axis=0).T
    for head in range(share):
        at = slice(head * HD, (head + 1) * HD)
        value = sum(
            o[:rows, at].astype(jnp.float32) * table[:, i * share + head : i * share + head + 1]
            for i, o in enumerate(outs)
        )
        out_ref[:, at] = value.astype(jnp.bfloat16)


def merge(outs, stats, share, rows):
    width = outs[0].shape[1]
    stats = [s for s in stats if s is not None]
    return pl.pallas_call(
        functools.partial(merge_kernel, len(outs), share),
        in_specs=[VMEM] * (len(outs) + len(stats)),
        out_specs=VMEM,
        out_shape=jax.ShapeDtypeStruct((rows, width), jnp.bfloat16),
        cost_estimate=cost(4 * len(outs) * rows * width, 0, *outs, *stats),
        compiler_params=mib(4),
        name="merge",
    )(*outs, *stats)


def project_kernel(cuts, later, row_cuts, *refs):
    parts, refs = refs[: len(cuts)], refs[len(cuts) :]
    w_hbm, total_ref, kept_ref, w_buf, sem = refs
    own = lax.axis_index("tm") // row_cuts
    depth = w_buf.shape[1]
    copies = []
    for i, a in enumerate((*cuts, *later)):
        first = pl.multiple_of((own ^ a) * depth, depth)
        to = w_buf.at[i] if i < len(cuts) else kept_ref.at[i - len(cuts)]
        copies.append(pltpu.make_async_copy(w_hbm.at[pl.ds(first, depth)], to, sem.at[i]))
        copies[i].start()
    for i, part in enumerate(parts):
        copies[i].wait()
        product = jnp.dot(part[...], w_buf[i], preferred_element_type=jnp.float32)
        total_ref[...] = product + total_ref[...] if i else product
    for copy in copies[len(cuts) :]:
        copy.wait()


def project(parts, cuts, later, weight, row_cuts):
    rows, depth = parts[0].shape
    columns = weight.shape[1]
    return pl.pallas_call(
        functools.partial(project_kernel, cuts, later, row_cuts),
        in_specs=[VMEM] * len(parts) + [HBM],
        out_specs=[VMEM, VMEM],
        out_shape=[
            jax.ShapeDtypeStruct((rows, columns), jnp.float32),
            jax.ShapeDtypeStruct((len(later), depth, columns), weight.dtype),
        ],
        scratch_shapes=[
            pltpu.VMEM((len(cuts), depth, columns), weight.dtype),
            pltpu.SemaphoreType.DMA((len(cuts) + len(later),)),
        ],
        cost_estimate=cost(2 * len(parts) * rows * depth * columns, 0, weight),
        compiler_params=mib(16),
        name="project",
    )(*parts, weight)


def project_rest_kernel(count, total_ref, kept_ref, *refs):
    parts, (keep_ref, send_ref, whole_ref) = refs[:count], refs[count:]
    value = total_ref[...]
    for i, part in enumerate(parts):
        value = value + jnp.dot(part[...], kept_ref[i], preferred_element_type=jnp.float32)
    chips, rows = keep_ref.shape[:2]
    core = lax.axis_index("heads") % 2
    for chip in range(chips):
        for c in range(2):
            first = (2 * chip + c) * rows
            whole_ref[c, chip] = value[first : first + rows]
    keep_ref[...] = whole_ref[core]
    send_ref[...] = whole_ref[1 - core].astype(jnp.bfloat16)


def project_rest(total, kept, parts, chips):
    rows, columns = total.shape
    block = (chips, rows // (2 * chips), columns)
    return pl.pallas_call(
        functools.partial(project_rest_kernel, len(parts)),
        in_specs=[VMEM] * (2 + len(parts)),
        out_specs=[VMEM, VMEM],
        out_shape=[
            jax.ShapeDtypeStruct(block, jnp.float32),
            jax.ShapeDtypeStruct(block, jnp.bfloat16),
        ],
        scratch_shapes=[pltpu.VMEM((2, *block), jnp.float32)],
        cost_estimate=cost(2 * rows * columns * kept.shape[0] * kept.shape[1], 0, kept),
        compiler_params=mib(16),
        name="project_rest",
    )(total, kept, *parts)


def pair_kernel(keep_ref, got_ref, mine_ref, *send_refs):
    chip = lax.axis_index("heads") // 2
    mine_ref[...] = keep_ref[chip] + got_ref[chip].astype(jnp.float32)
    for s, send_ref in enumerate(send_refs, 1):
        send_ref[...] = (keep_ref[chip ^ s] + got_ref[chip ^ s].astype(jnp.float32)).astype(
            jnp.bfloat16
        )


def pair_sum(keep, got):
    chips, rows, columns = keep.shape
    result = pl.pallas_call(
        pair_kernel,
        in_specs=[VMEM] * 2,
        out_specs=[VMEM] * chips,
        out_shape=[jax.ShapeDtypeStruct((rows, columns), jnp.float32)]
        + [jax.ShapeDtypeStruct((rows, columns), jnp.bfloat16)] * (chips - 1),
        cost_estimate=cost(chips * rows * columns, 0, keep, got),
        compiler_params=mib(8),
        name="pair",
    )(keep, got)
    return result[0], result[1:]


def condition_kernel(chips, shards, own_rows, mine_ref, residual_ref, gain_ref, *refs):
    got, refs = refs[: chips - 1], refs[chips - 1 :]
    weights, refs = refs[:shards], refs[shards:]
    rows = mine_ref.shape[0]
    h = lax.axis_index("heads")
    hidden = residual_ref[h].astype(jnp.float32) + mine_ref[...]
    for ref in got:
        hidden = hidden + ref[...].astype(jnp.float32)
    squares = jnp.sum(hidden * hidden, axis=1, keepdims=True)
    scaled = (hidden * gain_ref[...]).astype(jnp.bfloat16)
    width = weights[0].shape[1]
    products = [jnp.dot(scaled, w[...], preferred_element_type=jnp.float32) for w in weights]
    tail = jnp.zeros((rows, LANES), jnp.float32)
    lane = lax.broadcasted_iota(jnp.int32, (rows, LANES), 1)
    for p, piece in enumerate(pieces_of(squares)):
        tail = jnp.where(lane == p, piece.astype(jnp.float32), tail)
    if own_rows % 8 == 0 and width % LANES == 0:
        outs, held = refs[:-1], refs[-1]
        t = lax.axis_index("tm")
        for s, product in enumerate(products):
            held[:, pl.ds(pl.multiple_of((h ^ s) * width, LANES), width)] = product
        held[:, shards * width :] = tail
        for s, out_ref in enumerate(outs):
            first = pl.multiple_of((t ^ s) * own_rows, own_rows)
            out_ref[...] = held[pl.ds(first, own_rows), :].astype(jnp.bfloat16)
    else:
        for s, product in enumerate(products):
            refs[0][:, s * width : (s + 1) * width] = product.astype(jnp.bfloat16)
        refs[0][:, shards * width :] = tail.astype(jnp.bfloat16)


def condition_parts(mine, got, residual, gain, weights, n_tm, h, t):
    rows, depth = mine.shape
    shards = len(weights)
    width = weights[0].shape[1]
    full = shards * width + LANES
    own_rows = rows // n_tm
    aligned = own_rows % 8 == 0 and width % LANES == 0
    block = jax.ShapeDtypeStruct((own_rows, full), jnp.bfloat16)
    out_shape = [block] * n_tm if aligned else [jax.ShapeDtypeStruct((rows, full), jnp.bfloat16)]
    result = pl.pallas_call(
        functools.partial(condition_kernel, len(got) + 1, shards, own_rows),
        in_specs=[VMEM] * (3 + len(got) + shards),
        out_specs=[VMEM] * len(out_shape),
        out_shape=out_shape,
        scratch_shapes=[pltpu.VMEM((rows, full), jnp.float32)] * aligned,
        cost_estimate=cost(2 * rows * depth * full, 0, *weights),
        compiler_params=mib(12),
        name="condition",
    )(mine, residual.reshape(-1, rows, depth), gain[None, :], *got, *weights)
    if aligned:
        return result
    columns = result[0][:, :-LANES].reshape(rows, shards, width)
    columns = jnp.take(columns, jnp.arange(shards) ^ h, axis=1).reshape(rows, shards * width)
    result = jnp.concatenate([columns, result[0][:, -LANES:]], axis=1)
    result = result.reshape(n_tm, own_rows, full)
    return [pick(result, t ^ s) for s in range(n_tm)]


def sweep_kernel(sizes, steps, start_ref, embed_ref, in_ref, head_ref, *refs):
    n_tm, time_each, rows, model = sizes
    noise_refs, refs = refs[:n_tm], refs[n_tm:]
    parts, refs = refs[:n_tm], refs[n_tm:]
    outs, held = refs[:n_tm], refs[n_tm]
    t = lax.axis_index("tm")
    times = n_tm * time_each
    start = start_ref[t]
    chan = start.shape[1]
    for s, ref in enumerate(noise_refs):
        held[t ^ s] = ref[...].astype(jnp.float32)

    def block(i):
        at = (i % time_each) * rows
        return i // time_each, slice(at, at + rows)

    noise = [steps[times + i] * held[block(i)] for i in range(times - 1)]
    width = in_ref.shape[1]
    opening = jnp.dot(start.astype(jnp.bfloat16), in_ref[...], preferred_element_type=jnp.float32)
    total = sum(p[...].astype(jnp.float32) for p in parts)
    squares = total[:, width : width + 1]
    for p in range(1, PIECES):
        squares = squares + total[:, width + p : width + p + 1]
    condition = total[:, :width] * lax.rsqrt(squares / model + 1e-06)

    def increments_at(first, products):
        last = first + len(products)
        inside = jnp.concatenate(
            [p + (condition + embed_ref[i : i + 1]) for i, p in enumerate(products, first)], axis=0
        )
        action = (inside * jax.nn.sigmoid(inside)).astype(jnp.bfloat16)
        drift = jnp.dot(action, head_ref[...], preferred_element_type=jnp.float32)
        return [
            steps[i] * drift[(i - first) * rows : (i - first + 1) * rows] + noise[i]
            for i in range(first, last)
        ]

    increments = increments_at(0, [opening] * (times - 1))
    for sweep in range(1, SWEEPS + 1):
        change = [jnp.zeros((rows, chan), jnp.float32)]
        for i in range(times - 1):
            change.append(change[-1] + increments[i])
        if sweep == SWEEPS or sweep >= times - 1:
            break
        states = jnp.concatenate([start + change[i] for i in range(sweep, times - 1)], axis=0)
        product = jnp.dot(
            states.astype(jnp.bfloat16), in_ref[...], preferred_element_type=jnp.float32
        )
        increments = increments[:sweep] + increments_at(
            sweep, [product[i * rows : (i + 1) * rows] for i in range(times - 1 - sweep)]
        )
    for i in range(times):
        held[block(i)] = change[i]
    for s, out_ref in enumerate(outs):
        out_ref[...] = held[t ^ s].astype(jnp.bfloat16)


def sweep_all(parts, noise, embedding, steps, start, in_weight, head_out, time_each, model):
    n_tm, rows, chan = start.shape
    block = (time_each * rows, chan)
    return pl.pallas_call(
        functools.partial(sweep_kernel, (n_tm, time_each, rows, model)),
        in_specs=[SMEM] + [VMEM] * (4 + 2 * n_tm),
        out_specs=[VMEM] * n_tm,
        out_shape=[jax.ShapeDtypeStruct(block, jnp.bfloat16)] * n_tm,
        scratch_shapes=[pltpu.VMEM((n_tm, *block), jnp.float32)],
        cost_estimate=cost(
            10 * n_tm * time_each * rows * chan * in_weight.shape[1], 0, in_weight, head_out
        ),
        compiler_params=mib(16),
        name="sweeps",
    )(steps, start, embedding, in_weight, head_out, *noise, *parts)


def noise_kernel(time_each, noise_ref, *outs):
    t = lax.axis_index("tm")
    rows = noise_ref.shape[1]
    for s, out_ref in enumerate(outs):
        block = noise_ref[t ^ s].astype(jnp.float32)
        for i in range(time_each):
            out_ref[i * rows : (i + 1) * rows] = block[:, i, :].astype(jnp.bfloat16)


def noise_blocks(noise_draws, n_tm):
    rows, time_each, chan = noise_draws.shape
    own_rows = rows // n_tm
    block = jax.ShapeDtypeStruct((time_each * own_rows, chan), noise_draws.dtype)
    return pl.pallas_call(
        functools.partial(noise_kernel, time_each),
        in_specs=[VMEM],
        out_specs=[VMEM] * n_tm,
        out_shape=[block] * n_tm,
        cost_estimate=cost(0, 0, noise_draws, noise_draws),
        compiler_params=mib(4),
        name="noise",
    )(noise_draws.reshape(n_tm, own_rows, time_each, chan))


def finish_kernel(sizes, start_ref, *refs):
    time_each, rows = sizes
    parts, out_ref = refs[:-1], refs[-1]
    t = lax.axis_index("tm")
    for s, part in enumerate(parts):
        start = start_ref[t ^ s]
        for i in range(time_each):
            out_ref[pl.ds((t ^ s) * rows, rows), i, :] = start + part[
                i * rows : (i + 1) * rows
            ].astype(jnp.float32)


def finish(start, parts, time_each):
    n_tm, rows, chan = start.shape
    return pl.pallas_call(
        functools.partial(finish_kernel, (time_each, rows)),
        in_specs=[VMEM] * (1 + len(parts)),
        out_specs=VMEM,
        out_shape=jax.ShapeDtypeStruct((n_tm * rows, time_each, chan), jnp.float32),
        cost_estimate=cost(n_tm * rows * time_each * chan, 0, start, *parts),
        compiler_params=mib(4),
        name="finish",
    )(start, *parts)


def shards(
    queries,
    cache_keys,
    cache_values,
    residual,
    out_weight,
    norm_gain,
    cond_weight,
    in_weight,
    head_out,
    start_state,
    noise_draws,
    positions,
    cache_length,
    plan,
):
    rows, width = queries.shape
    n_heads = lax.axis_size("heads")
    n_tm = lax.axis_size("tm")
    h = lax.axis_index("heads")
    t = lax.axis_index("tm")
    local_heads = width // HD
    model = out_weight.shape[1] * n_tm
    row_each, time_each, chan = noise_draws.shape
    own_rows = row_each // n_tm
    hidden_width = in_weight.shape[1]

    head_cuts = math.gcd(local_heads, n_tm)
    row_cuts = n_tm // head_cuts
    share = local_heads // head_cuts
    own_row_cut = t % row_cuts

    def cut(values, index, axis):
        if row_cuts == 1:
            return values
        size = values.shape[axis] // row_cuts
        return lax.dynamic_slice_in_dim(values, index * size, size, axis)

    chips = n_heads // 2
    far = []
    for s in range(1, chips):
        far.append(swap(cond_weight, "heads", 2 * s))
    near = swap(cond_weight, "heads", 1)

    order = list(range(head_cuts))[::-1]
    outs, stats = [None] * n_tm, [None] * n_tm
    for groups in calls_of(order):
        blocks = attend(
            queries, cache_keys, cache_values, positions, cache_length, groups, share, row_cuts
        )
        for a, (out, stat) in zip(groups, blocks):
            for b in range(row_cuts):
                s = a * row_cuts + b
                outs[s] = cut(out, own_row_cut ^ b, 0)
                stats[s] = None if stat is None else cut(stat, own_row_cut ^ b, 1)
                if s:
                    outs[s] = swap(outs[s], "tm", s)
                    stats[s] = None if stat is None else swap(stats[s], "tm", s)
    attended = merge(outs, stats, share, rows // row_cuts)
    parts = exchange([attended] * n_tm)
    by_cut = []
    for a in range(head_cuts):
        part = parts[a * row_cuts : (a + 1) * row_cuts]
        if row_cuts > 1:
            part = jnp.take(jnp.stack(part), jnp.arange(row_cuts) ^ own_row_cut, axis=0)
            part = part.reshape(rows, share * HD)
        else:
            part = part[0]
        by_cut.append(part)
    half = max(1, head_cuts // 2)
    cuts = list(range(head_cuts))
    total, kept = project(by_cut[:half], cuts[:half], cuts[half:], out_weight, row_cuts)
    keep, send = project_rest(total, kept, by_cut[half:], chips)

    far, send = lax.optimization_barrier((far, send))
    other = swap(send, "heads", 1)
    mine, far_rows = pair_sum(keep, other)
    got = []
    for s, r in enumerate(far_rows, 1):
        got.append(swap(r, "heads", 2 * s))

    cond_shards = [cond_weight, near]
    for s, w in enumerate(far, 1):
        cond_shards += [w, swap(w, "heads", 1)]

    cond = condition_parts(mine, got, residual, norm_gain, cond_shards, n_tm, h, t)
    cond = exchange(cond)

    noise = noise_blocks(noise_draws, n_tm)
    noise = exchange(noise)
    levels = plan.astype(jnp.float32)
    half_width = hidden_width // 2
    frequencies = jnp.exp(
        -math.log(10000.0) * jnp.arange(half_width, dtype=jnp.float32) / half_width
    )
    angles = levels[:-1, None] * frequencies[None, :]
    embedding = jnp.concatenate([jnp.sin(angles), jnp.cos(angles)], axis=1)
    step_size = (levels[:-1] - levels[1:]) / 1000.0
    steps = jnp.concatenate([step_size, jnp.sqrt(step_size)])
    start = start_state.reshape(n_tm, own_rows, chan)
    change = sweep_all(
        cond, noise, embedding, steps, start, in_weight, head_out, time_each, model
    )
    back = exchange(change)
    return finish(start, back, time_each)


def solution(mesh):
    placed = (
        P("groups", "heads"),
        P(("groups", "tm"), "heads"),
        P(("groups", "tm"), "heads"),
        P("groups", "tm"),
        P("heads", "tm"),
        P("tm"),
        P("tm", "heads"),
        P(),
        P(),
        P(("groups", "heads"), None),
        P(("groups", "heads"), "tm", None),
        P("groups"),
        P("groups"),
        P(),
    )

    return jax.shard_map(
        shards,
        mesh=mesh,
        in_specs=placed,
        out_specs=P(("groups", "heads"), "tm", None),
        check_vma=False,
    )
```

```python
import functools
import math

import jax
import jax.numpy as jnp
from jax import lax
from jax.experimental import pallas as pl
from jax.experimental.pallas import tpu as pltpu
from jax.sharding import PartitionSpec as P


HD = 128
SWEEPS = 3
LANES = 128


def swap(values, axis, distance):
    size = lax.axis_size(axis)
    return lax.ppermute(values, axis, [(i, i ^ distance) for i in range(size)])


def exchange(blocks):
    got = [blocks[0]]
    for s, block in enumerate(blocks[1:], 1):
        got.append(swap(block, "tm", s))
    return got


def pick(values, index):
    return lax.dynamic_index_in_dim(values, index, 0, False)


def cost(flops, transcendentals, *arrays):
    moved = sum(math.prod(a.shape) * jnp.dtype(a.dtype).itemsize for a in arrays)
    return pl.CostEstimate(flops=flops, bytes_accessed=moved, transcendentals=transcendentals)


def mib(count):
    return pltpu.CompilerParams(vmem_limit_bytes=count * 1024 * 1024)


VMEM = pl.BlockSpec(memory_space=pltpu.VMEM)
SMEM = pl.BlockSpec(memory_space=pltpu.SMEM)
HBM = pl.BlockSpec(memory_space=pltpu.HBM)
PIECES = 3
ATTEND_MIB = 44


def pieces_of(value):
    high = value.astype(jnp.bfloat16)
    rest = value - high.astype(jnp.float32)
    middle = rest.astype(jnp.bfloat16)
    return high, middle, (rest - middle.astype(jnp.float32)).astype(jnp.bfloat16)


def sum_pieces(pieces):
    high, middle, low = (p.astype(jnp.float32) for p in pieces)
    return high + (middle + low)


def packed(rows, width, share):
    return PIECES * rows <= width and 2 * share <= 8 and rows % LANES == 0


def calls_of(order):
    return [groups for groups in (order[:1], order[1:-1], order[-1:] if order[1:] else []) if groups]


def attend_heads(groups, share, per_copy, valid, q_of, k_of, v_of, cos_ref, sin_ref, outs, stats):
    rows = cos_ref.shape[0]
    even = lax.broadcasted_iota(jnp.int32, (rows, HD), 1) % 2 == 0
    lane = lax.broadcasted_iota(jnp.int32, (rows, LANES), 1)
    scale = 1.0 / math.sqrt(HD)
    held = jnp.zeros((rows, LANES), jnp.float32)
    parts = share // per_copy
    for slot in range(len(groups) * parts):
        g, part = divmod(slot, parts)
        for i in range(per_copy):
            head = part * per_copy + i
            at = slice(i * HD, (i + 1) * HD)
            to = slice(head * HD, (head + 1) * HD)
            wide = q_of(g, to).astype(jnp.float32)
            partner = jnp.where(even, pltpu.roll(wide, HD - 1, 1), pltpu.roll(wide, 1, 1))
            rotated = (wide * cos_ref[...] + partner * sin_ref[...]).astype(jnp.bfloat16)
            scores = lax.dot_general(
                rotated,
                k_of(slot, at),
                (((1,), (1,)), ((), ())),
                preferred_element_type=jnp.float32,
            )
            scores = jnp.where(valid, scores, jnp.float32(-1e30))
            block_max = jnp.maximum(jnp.max(scores, axis=1, keepdims=True), -1e29)
            weights = jnp.exp((scores - block_max) * scale)
            block_total = jnp.sum(weights, axis=1, keepdims=True)
            block_out = jnp.dot(
                weights.astype(jnp.bfloat16), v_of(slot, at), preferred_element_type=jnp.float32
            )
            outs[g][:rows, to] = block_out.astype(jnp.bfloat16)
            held = jnp.where(lane == head, block_max * scale, held)
            held = jnp.where(lane == share + head, block_total, held)
        if part == parts - 1:
            flat = held.T
            if stats:
                stats[g][...] = flat[: 2 * share]
            else:
                extra = outs[g].shape[0] - rows
                for p, piece in enumerate(pieces_of(flat[:extra])):
                    outs[g][rows:, p * rows : (p + 1) * rows] = piece


def valid_keys(length_ref, keys):
    return (
        lax.broadcasted_iota(jnp.int32, (1, keys), 1)
        < length_ref[0] - lax.axis_index("tm") * keys
    )


def attend_kernel(calls, share, per_copy, row_cuts, joined, *refs):
    length_ref, pos_ref, q_hbm, k_hbm, v_hbm = refs[:5]
    groups = calls[0]
    n = len(groups)
    outs, refs = refs[5 : 5 + n], refs[5 + n :]
    stats, refs = ([], refs) if joined else (refs[:n], refs[n:])
    cos_ref, sin_ref, refs = refs[0], refs[1], refs[2:]
    kept, refs = refs[: 3 * len(calls) - 3], refs[3 * len(calls) - 3 :]
    q_buf, k_buf, v_buf, sem = refs
    rows = q_hbm.shape[0]
    keys = k_hbm.shape[0]
    own = lax.axis_index("tm") // row_cuts
    width = per_copy * HD
    parts = share // per_copy
    copies = []

    def start(from_ref, to_ref):
        copies.append(pltpu.make_async_copy(from_ref, to_ref, sem.at[len(copies)]))
        copies[-1].start()
        return copies[-1]

    first_copies = []
    for c, call in enumerate(calls):
        to = (q_buf, k_buf, v_buf) if c == 0 else kept[3 * c - 3 : 3 * c]
        for g, a in enumerate(call):
            first = pl.multiple_of((own ^ a) * share * HD, HD)
            wanted = [start(q_hbm.at[:, pl.ds(first, share * HD)], to[0].at[g])]
            for part in range(parts):
                slot = g * parts + part
                column = pl.multiple_of(first + part * width, HD)
                wanted += [
                    start(hbm.at[:, pl.ds(column, width)], buf.at[slot])
                    for hbm, buf in ((k_hbm, to[1]), (v_hbm, to[2]))
                ]
                if c == 0:
                    first_copies.append(wanted)
                    wanted = []
    lane = lax.broadcasted_iota(jnp.int32, (8, HD), 1)
    sublane = lax.broadcasted_iota(jnp.int32, (8, HD), 0)
    pair = (lane - lane % 2).astype(jnp.float32)
    frequencies = jnp.exp(pair * (-math.log(10000.0) / HD))
    for r in range(0, rows, 8):
        place = jnp.full((8, HD), pos_ref[r], jnp.int32)
        for i in range(1, 8):
            place = jnp.where(sublane == i, pos_ref[r + i], place)
        angles = place.astype(jnp.float32) * frequencies
        cos_ref[r : r + 8] = jnp.cos(angles)
        sine = jnp.sin(angles)
        sin_ref[r : r + 8] = jnp.where(lane % 2 == 0, -sine, sine)
    done = set()

    def near(buf):
        def read(slot, at):
            if slot not in done:
                done.add(slot)
                for copy in first_copies[slot]:
                    copy.wait()
            return buf[slot, :, at]

        return read

    def query(g, at):
        if g * parts not in done:
            done.add(g * parts)
            for copy in first_copies[g * parts]:
                copy.wait()
        return q_buf[g, :, at]

    attend_heads(
        groups,
        share,
        per_copy,
        valid_keys(length_ref, keys),
        query,
        near(k_buf),
        near(v_buf),
        cos_ref,
        sin_ref,
        outs,
        stats,
    )
    for copy in copies[sum(len(wanted) for wanted in first_copies) :]:
        copy.wait()


def attend_near_kernel(groups, share, per_copy, joined, *refs):
    length_ref, cos_ref, sin_ref, q_ref, k_ref, v_ref = refs[:6]
    n = len(groups)
    outs, stats = refs[6 : 6 + n], [] if joined else refs[6 + n :]
    attend_heads(
        groups,
        share,
        per_copy,
        valid_keys(length_ref, k_ref.shape[1]),
        lambda g, at: q_ref[g, :, at],
        lambda slot, at: k_ref[slot, :, at],
        lambda slot, at: v_ref[slot, :, at],
        cos_ref,
        sin_ref,
        outs,
        stats,
    )


def attend(queries, keys, values, positions, cache_length, calls, share, row_cuts):
    rows = queries.shape[0]
    key_count = keys.shape[0]
    per_copy = 2 if share % 2 == 0 else 1
    wide = share * HD
    joined = row_cuts == 1 and packed(rows, wide, share)
    table = jax.ShapeDtypeStruct((rows, HD), jnp.float32)

    def blocks(n):
        shapes = [jax.ShapeDtypeStruct((rows + 8 * joined, wide), jnp.bfloat16)] * n
        if not joined:
            shapes = shapes + [jax.ShapeDtypeStruct((2 * share, rows), jnp.float32)] * n
        return shapes

    def near(n):
        cache = (n * share // per_copy, key_count, per_copy * HD)
        return [((n, rows, wide), jnp.bfloat16), (cache, jnp.bfloat16), (cache, jnp.bfloat16)]

    def price(n):
        return pl.CostEstimate(
            flops=4 * n * share * rows * key_count * HD,
            bytes_accessed=4 * n * share * key_count * HD,
            transcendentals=n * share * rows * key_count,
        )

    def found(result, n):
        return list(zip(result[:n], [None] * n if joined else result[n : 2 * n]))

    n = len(calls[0])
    out_shape = blocks(n) + [table] * 2
    for call in calls[1:]:
        out_shape = out_shape + [jax.ShapeDtypeStruct(*entry) for entry in near(len(call))]
    count = sum(len(call) for call in calls) * (1 + 2 * share // per_copy)
    result = pl.pallas_call(
        functools.partial(attend_kernel, calls, share, per_copy, row_cuts, joined),
        in_specs=[SMEM] * 2 + [HBM] * 3,
        out_specs=[VMEM] * len(out_shape),
        out_shape=out_shape,
        scratch_shapes=[pltpu.VMEM(*entry) for entry in near(n)]
        + [pltpu.SemaphoreType.DMA((count,))],
        cost_estimate=price(n),
        compiler_params=mib(ATTEND_MIB),
        name="attend",
    )(cache_length, positions, queries, keys, values)
    skip = len(blocks(n))
    tables, kept = result[skip : skip + 2], result[skip + 2 :]
    blocks_of = [found(result, n)]
    for c, call in enumerate(calls[1:]):
        n = len(call)
        result = pl.pallas_call(
            functools.partial(attend_near_kernel, call, share, per_copy, joined),
            in_specs=[SMEM] + [VMEM] * 5,
            out_specs=[VMEM] * len(blocks(n)),
            out_shape=blocks(n),
            cost_estimate=price(n),
            compiler_params=mib(16),
            name="attend_near",
        )(cache_length, *tables, *kept[3 * c : 3 * c + 3])
        blocks_of.append(found(result, n))
    return blocks_of


def merge_kernel(count, share, *refs):
    out_ref = refs[-1]
    rows = out_ref.shape[0]
    outs, stats = refs[:count], refs[count:-1]
    if stats:
        tables = [s[...] for s in stats]
    else:
        tables = [
            sum_pieces([o[rows:, p * rows : (p + 1) * rows] for p in range(PIECES)]) for o in outs
        ]
    maxima = [s[:share] for s in tables]
    totals = [s[share : 2 * share] for s in tables]
    top = functools.reduce(jnp.maximum, maxima)
    factors = [jnp.exp(m - top) for m in maxima]
    total = sum(f * s for f, s in zip(factors, totals))
    scales = [f / total for f in factors]
    pad = -(count * share) % LANES
    table = jnp.concatenate(scales + [jnp.zeros((pad, rows), jnp.float32)], axis=0).T
    for head in range(share):
        at = slice(head * HD, (head + 1) * HD)
        value = sum(
            o[:rows, at].astype(jnp.float32) * table[:, i * share + head : i * share + head + 1]
            for i, o in enumerate(outs)
        )
        out_ref[:, at] = value.astype(jnp.bfloat16)


def merge(outs, stats, share, rows):
    width = outs[0].shape[1]
    stats = [s for s in stats if s is not None]
    return pl.pallas_call(
        functools.partial(merge_kernel, len(outs), share),
        in_specs=[VMEM] * (len(outs) + len(stats)),
        out_specs=VMEM,
        out_shape=jax.ShapeDtypeStruct((rows, width), jnp.bfloat16),
        cost_estimate=cost(4 * len(outs) * rows * width, 0, *outs, *stats),
        compiler_params=mib(4),
        name="merge",
    )(*outs, *stats)


def project_kernel(cuts, later, row_cuts, *refs):
    parts, refs = refs[: len(cuts)], refs[len(cuts) :]
    w_hbm, total_ref, kept_ref, w_buf, sem = refs
    own = lax.axis_index("tm") // row_cuts
    depth = w_buf.shape[1]
    copies = []
    for i, a in enumerate((*cuts, *later)):
        first = pl.multiple_of((own ^ a) * depth, depth)
        to = w_buf.at[i] if i < len(cuts) else kept_ref.at[i - len(cuts)]
        copies.append(pltpu.make_async_copy(w_hbm.at[pl.ds(first, depth)], to, sem.at[i]))
        copies[i].start()
    for i, part in enumerate(parts):
        copies[i].wait()
        product = jnp.dot(part[...], w_buf[i], preferred_element_type=jnp.float32)
        total_ref[...] = product + total_ref[...] if i else product
    for copy in copies[len(cuts) :]:
        copy.wait()


def project(parts, cuts, later, weight, row_cuts):
    rows, depth = parts[0].shape
    columns = weight.shape[1]
    return pl.pallas_call(
        functools.partial(project_kernel, cuts, later, row_cuts),
        in_specs=[VMEM] * len(parts) + [HBM],
        out_specs=[VMEM, VMEM],
        out_shape=[
            jax.ShapeDtypeStruct((rows, columns), jnp.float32),
            jax.ShapeDtypeStruct((len(later), depth, columns), weight.dtype),
        ],
        scratch_shapes=[
            pltpu.VMEM((len(cuts), depth, columns), weight.dtype),
            pltpu.SemaphoreType.DMA((len(cuts) + len(later),)),
        ],
        cost_estimate=cost(2 * len(parts) * rows * depth * columns, 0, weight),
        compiler_params=mib(16),
        name="project",
    )(*parts, weight)


def project_rest_kernel(count, total_ref, kept_ref, *refs):
    parts, (keep_ref, send_ref, whole_ref) = refs[:count], refs[count:]
    value = total_ref[...]
    for i, part in enumerate(parts):
        value = value + jnp.dot(part[...], kept_ref[i], preferred_element_type=jnp.float32)
    chips, rows = keep_ref.shape[:2]
    core = lax.axis_index("heads") % 2
    for chip in range(chips):
        for c in range(2):
            first = (2 * chip + c) * rows
            whole_ref[c, chip] = value[first : first + rows]
    keep_ref[...] = whole_ref[core]
    send_ref[...] = whole_ref[1 - core].astype(jnp.bfloat16)


def project_rest(total, kept, parts, chips):
    rows, columns = total.shape
    block = (chips, rows // (2 * chips), columns)
    return pl.pallas_call(
        functools.partial(project_rest_kernel, len(parts)),
        in_specs=[VMEM] * (2 + len(parts)),
        out_specs=[VMEM, VMEM],
        out_shape=[
            jax.ShapeDtypeStruct(block, jnp.float32),
            jax.ShapeDtypeStruct(block, jnp.bfloat16),
        ],
        scratch_shapes=[pltpu.VMEM((2, *block), jnp.float32)],
        cost_estimate=cost(2 * rows * columns * kept.shape[0] * kept.shape[1], 0, kept),
        compiler_params=mib(16),
        name="project_rest",
    )(total, kept, *parts)


def pair_kernel(keep_ref, got_ref, mine_ref, *send_refs):
    chip = lax.axis_index("heads") // 2
    mine_ref[...] = keep_ref[chip] + got_ref[chip].astype(jnp.float32)
    for s, send_ref in enumerate(send_refs, 1):
        send_ref[...] = (keep_ref[chip ^ s] + got_ref[chip ^ s].astype(jnp.float32)).astype(
            jnp.bfloat16
        )


def pair_sum(keep, got):
    chips, rows, columns = keep.shape
    result = pl.pallas_call(
        pair_kernel,
        in_specs=[VMEM] * 2,
        out_specs=[VMEM] * chips,
        out_shape=[jax.ShapeDtypeStruct((rows, columns), jnp.float32)]
        + [jax.ShapeDtypeStruct((rows, columns), jnp.bfloat16)] * (chips - 1),
        cost_estimate=cost(chips * rows * columns, 0, keep, got),
        compiler_params=mib(8),
        name="pair",
    )(keep, got)
    return result[0], result[1:]


def condition_kernel(chips, shards, own_rows, mine_ref, residual_ref, gain_ref, *refs):
    got, refs = refs[: chips - 1], refs[chips - 1 :]
    weights, refs = refs[:shards], refs[shards:]
    rows = mine_ref.shape[0]
    h = lax.axis_index("heads")
    hidden = residual_ref[h].astype(jnp.float32) + mine_ref[...]
    for ref in got:
        hidden = hidden + ref[...].astype(jnp.float32)
    squares = jnp.sum(hidden * hidden, axis=1, keepdims=True)
    scaled = (hidden * gain_ref[...]).astype(jnp.bfloat16)
    width = weights[0].shape[1]
    products = [jnp.dot(scaled, w[...], preferred_element_type=jnp.float32) for w in weights]
    tail = jnp.zeros((rows, LANES), jnp.float32)
    lane = lax.broadcasted_iota(jnp.int32, (rows, LANES), 1)
    for p, piece in enumerate(pieces_of(squares)):
        tail = jnp.where(lane == p, piece.astype(jnp.float32), tail)
    if own_rows % 8 == 0 and width % LANES == 0:
        outs, held = refs[:-1], refs[-1]
        t = lax.axis_index("tm")
        for s, product in enumerate(products):
            held[:, pl.ds(pl.multiple_of((h ^ s) * width, LANES), width)] = product
        held[:, shards * width :] = tail
        for s, out_ref in enumerate(outs):
            first = pl.multiple_of((t ^ s) * own_rows, own_rows)
            out_ref[...] = held[pl.ds(first, own_rows), :].astype(jnp.bfloat16)
    else:
        for s, product in enumerate(products):
            refs[0][:, s * width : (s + 1) * width] = product.astype(jnp.bfloat16)
        refs[0][:, shards * width :] = tail.astype(jnp.bfloat16)


def condition_parts(mine, got, residual, gain, weights, n_tm, h, t):
    rows, depth = mine.shape
    shards = len(weights)
    width = weights[0].shape[1]
    full = shards * width + LANES
    own_rows = rows // n_tm
    aligned = own_rows % 8 == 0 and width % LANES == 0
    block = jax.ShapeDtypeStruct((own_rows, full), jnp.bfloat16)
    out_shape = [block] * n_tm if aligned else [jax.ShapeDtypeStruct((rows, full), jnp.bfloat16)]
    result = pl.pallas_call(
        functools.partial(condition_kernel, len(got) + 1, shards, own_rows),
        in_specs=[VMEM] * (3 + len(got) + shards),
        out_specs=[VMEM] * len(out_shape),
        out_shape=out_shape,
        scratch_shapes=[pltpu.VMEM((rows, full), jnp.float32)] * aligned,
        cost_estimate=cost(2 * rows * depth * full, 0, *weights),
        compiler_params=mib(12),
        name="condition",
    )(mine, residual.reshape(-1, rows, depth), gain[None, :], *got, *weights)
    if aligned:
        return result
    columns = result[0][:, :-LANES].reshape(rows, shards, width)
    columns = jnp.take(columns, jnp.arange(shards) ^ h, axis=1).reshape(rows, shards * width)
    result = jnp.concatenate([columns, result[0][:, -LANES:]], axis=1)
    result = result.reshape(n_tm, own_rows, full)
    return [pick(result, t ^ s) for s in range(n_tm)]


def sweep_kernel(sizes, steps, start_ref, embed_ref, in_ref, head_ref, *refs):
    n_tm, time_each, rows, model = sizes
    noise_refs, refs = refs[:n_tm], refs[n_tm:]
    parts, refs = refs[:n_tm], refs[n_tm:]
    outs, held = refs[:n_tm], refs[n_tm]
    t = lax.axis_index("tm")
    times = n_tm * time_each
    start = start_ref[t]
    chan = start.shape[1]
    for s, ref in enumerate(noise_refs):
        held[t ^ s] = ref[...].astype(jnp.float32)

    def block(i):
        at = (i % time_each) * rows
        return i // time_each, slice(at, at + rows)

    noise = [steps[times + i] * held[block(i)] for i in range(times - 1)]
    width = in_ref.shape[1]
    opening = jnp.dot(start.astype(jnp.bfloat16), in_ref[...], preferred_element_type=jnp.float32)
    total = sum(p[...].astype(jnp.float32) for p in parts)
    squares = total[:, width : width + 1]
    for p in range(1, PIECES):
        squares = squares + total[:, width + p : width + p + 1]
    condition = total[:, :width] * lax.rsqrt(squares / model + 1e-06)

    def increments_at(first, products):
        last = first + len(products)
        inside = jnp.concatenate(
            [p + (condition + embed_ref[i : i + 1]) for i, p in enumerate(products, first)], axis=0
        )
        action = (inside * jax.nn.sigmoid(inside)).astype(jnp.bfloat16)
        drift = jnp.dot(action, head_ref[...], preferred_element_type=jnp.float32)
        return [
            steps[i] * drift[(i - first) * rows : (i - first + 1) * rows] + noise[i]
            for i in range(first, last)
        ]

    increments = increments_at(0, [opening] * (times - 1))
    for sweep in range(1, SWEEPS + 1):
        change = [jnp.zeros((rows, chan), jnp.float32)]
        for i in range(times - 1):
            change.append(change[-1] + increments[i])
        if sweep == SWEEPS or sweep >= times - 1:
            break
        states = jnp.concatenate([start + change[i] for i in range(sweep, times - 1)], axis=0)
        product = jnp.dot(
            states.astype(jnp.bfloat16), in_ref[...], preferred_element_type=jnp.float32
        )
        increments = increments[:sweep] + increments_at(
            sweep, [product[i * rows : (i + 1) * rows] for i in range(times - 1 - sweep)]
        )
    for i in range(times):
        held[block(i)] = change[i]
    for s, out_ref in enumerate(outs):
        out_ref[...] = held[t ^ s].astype(jnp.bfloat16)


def sweep_all(parts, noise, embedding, steps, start, in_weight, head_out, time_each, model):
    n_tm, rows, chan = start.shape
    block = (time_each * rows, chan)
    return pl.pallas_call(
        functools.partial(sweep_kernel, (n_tm, time_each, rows, model)),
        in_specs=[SMEM] + [VMEM] * (4 + 2 * n_tm),
        out_specs=[VMEM] * n_tm,
        out_shape=[jax.ShapeDtypeStruct(block, jnp.bfloat16)] * n_tm,
        scratch_shapes=[pltpu.VMEM((n_tm, *block), jnp.float32)],
        cost_estimate=cost(
            10 * n_tm * time_each * rows * chan * in_weight.shape[1], 0, in_weight, head_out
        ),
        compiler_params=mib(16),
        name="sweeps",
    )(steps, start, embedding, in_weight, head_out, *noise, *parts)


def noise_kernel(time_each, noise_ref, *outs):
    t = lax.axis_index("tm")
    rows = noise_ref.shape[1]
    for s, out_ref in enumerate(outs):
        block = noise_ref[t ^ s].astype(jnp.float32)
        for i in range(time_each):
            out_ref[i * rows : (i + 1) * rows] = block[:, i, :].astype(jnp.bfloat16)


def noise_blocks(noise_draws, n_tm):
    rows, time_each, chan = noise_draws.shape
    own_rows = rows // n_tm
    block = jax.ShapeDtypeStruct((time_each * own_rows, chan), noise_draws.dtype)
    return pl.pallas_call(
        functools.partial(noise_kernel, time_each),
        in_specs=[VMEM],
        out_specs=[VMEM] * n_tm,
        out_shape=[block] * n_tm,
        cost_estimate=cost(0, 0, noise_draws, noise_draws),
        compiler_params=mib(4),
        name="noise",
    )(noise_draws.reshape(n_tm, own_rows, time_each, chan))


def finish_kernel(sizes, start_ref, *refs):
    time_each, rows = sizes
    parts, out_ref = refs[:-1], refs[-1]
    t = lax.axis_index("tm")
    for s, part in enumerate(parts):
        start = start_ref[t ^ s]
        for i in range(time_each):
            out_ref[pl.ds((t ^ s) * rows, rows), i, :] = start + part[
                i * rows : (i + 1) * rows
            ].astype(jnp.float32)


def finish(start, parts, time_each):
    n_tm, rows, chan = start.shape
    return pl.pallas_call(
        functools.partial(finish_kernel, (time_each, rows)),
        in_specs=[VMEM] * (1 + len(parts)),
        out_specs=VMEM,
        out_shape=jax.ShapeDtypeStruct((n_tm * rows, time_each, chan), jnp.float32),
        cost_estimate=cost(n_tm * rows * time_each * chan, 0, start, *parts),
        compiler_params=mib(4),
        name="finish",
    )(start, *parts)


def shards(
    queries,
    cache_keys,
    cache_values,
    residual,
    out_weight,
    norm_gain,
    cond_weight,
    in_weight,
    head_out,
    start_state,
    noise_draws,
    positions,
    cache_length,
    plan,
):
    rows, width = queries.shape
    n_heads = lax.axis_size("heads")
    n_tm = lax.axis_size("tm")
    h = lax.axis_index("heads")
    t = lax.axis_index("tm")
    local_heads = width // HD
    model = out_weight.shape[1] * n_tm
    row_each, time_each, chan = noise_draws.shape
    own_rows = row_each // n_tm
    hidden_width = in_weight.shape[1]

    head_cuts = math.gcd(local_heads, n_tm)
    row_cuts = n_tm // head_cuts
    share = local_heads // head_cuts
    own_row_cut = t % row_cuts

    def cut(values, index, axis):
        if row_cuts == 1:
            return values
        size = values.shape[axis] // row_cuts
        return lax.dynamic_slice_in_dim(values, index * size, size, axis)

    chips = n_heads // 2
    far = []
    for s in range(1, chips):
        far.append(swap(cond_weight, "heads", 2 * s))
    near = swap(cond_weight, "heads", 1)

    order = list(range(head_cuts))[::-1]
    outs, stats = [None] * n_tm, [None] * n_tm
    calls = calls_of(order)
    found = attend(
        queries, cache_keys, cache_values, positions, cache_length, calls, share, row_cuts
    )
    for groups, blocks in zip(calls, found):
        for a, (out, stat) in zip(groups, blocks):
            for b in range(row_cuts):
                s = a * row_cuts + b
                outs[s] = cut(out, own_row_cut ^ b, 0)
                stats[s] = None if stat is None else cut(stat, own_row_cut ^ b, 1)
                if s:
                    outs[s] = swap(outs[s], "tm", s)
                    stats[s] = None if stat is None else swap(stats[s], "tm", s)
    attended = merge(outs, stats, share, rows // row_cuts)
    parts = exchange([attended] * n_tm)
    by_cut = []
    for a in range(head_cuts):
        part = parts[a * row_cuts : (a + 1) * row_cuts]
        if row_cuts > 1:
            part = jnp.take(jnp.stack(part), jnp.arange(row_cuts) ^ own_row_cut, axis=0)
            part = part.reshape(rows, share * HD)
        else:
            part = part[0]
        by_cut.append(part)
    half = max(1, head_cuts // 2)
    cuts = list(range(head_cuts))
    total, kept = project(by_cut[:half], cuts[:half], cuts[half:], out_weight, row_cuts)
    keep, send = project_rest(total, kept, by_cut[half:], chips)

    far, send = lax.optimization_barrier((far, send))
    other = swap(send, "heads", 1)
    mine, far_rows = pair_sum(keep, other)
    got = []
    for s, r in enumerate(far_rows, 1):
        got.append(swap(r, "heads", 2 * s))

    cond_shards = [cond_weight, near]
    for s, w in enumerate(far, 1):
        cond_shards += [w, swap(w, "heads", 1)]

    cond = condition_parts(mine, got, residual, norm_gain, cond_shards, n_tm, h, t)
    cond = exchange(cond)

    noise = noise_blocks(noise_draws, n_tm)
    noise = exchange(noise)
    levels = plan.astype(jnp.float32)
    half_width = hidden_width // 2
    frequencies = jnp.exp(
        -math.log(10000.0) * jnp.arange(half_width, dtype=jnp.float32) / half_width
    )
    angles = levels[:-1, None] * frequencies[None, :]
    embedding = jnp.concatenate([jnp.sin(angles), jnp.cos(angles)], axis=1)
    step_size = (levels[:-1] - levels[1:]) / 1000.0
    steps = jnp.concatenate([step_size, jnp.sqrt(step_size)])
    start = start_state.reshape(n_tm, own_rows, chan)
    change = sweep_all(
        cond, noise, embedding, steps, start, in_weight, head_out, time_each, model
    )
    back = exchange(change)
    return finish(start, back, time_each)


def solution(mesh):
    placed = (
        P("groups", "heads"),
        P(("groups", "tm"), "heads"),
        P(("groups", "tm"), "heads"),
        P("groups", "tm"),
        P("heads", "tm"),
        P("tm"),
        P("tm", "heads"),
        P(),
        P(),
        P(("groups", "heads"), None),
        P(("groups", "heads"), "tm", None),
        P("groups"),
        P("groups"),
        P(),
    )

    return jax.shard_map(
        shards,
        mesh=mesh,
        in_specs=placed,
        out_specs=P(("groups", "heads"), "tm", None),
        check_vma=False,
    )
```

```python
import functools
import math

import jax
import jax.numpy as jnp
from jax import lax
from jax.experimental import pallas as pl
from jax.experimental.pallas import tpu as pltpu
from jax.sharding import PartitionSpec as P


HD = 128
SWEEPS = 3
LANES = 128


def swap(values, axis, distance):
    size = lax.axis_size(axis)
    return lax.ppermute(values, axis, [(i, i ^ distance) for i in range(size)])


def exchange(blocks):
    got = [blocks[0]]
    for s, block in enumerate(blocks[1:], 1):
        got.append(swap(block, "tm", s))
    return got


def pick(values, index):
    return lax.dynamic_index_in_dim(values, index, 0, False)


def cost(flops, transcendentals, *arrays):
    moved = sum(math.prod(a.shape) * jnp.dtype(a.dtype).itemsize for a in arrays)
    return pl.CostEstimate(flops=flops, bytes_accessed=moved, transcendentals=transcendentals)


def mib(count):
    return pltpu.CompilerParams(vmem_limit_bytes=count * 1024 * 1024)


VMEM = pl.BlockSpec(memory_space=pltpu.VMEM)
SMEM = pl.BlockSpec(memory_space=pltpu.SMEM)
HBM = pl.BlockSpec(memory_space=pltpu.HBM)
PIECES = 3
ATTEND_MIB = 44


def pieces_of(value):
    high = value.astype(jnp.bfloat16)
    rest = value - high.astype(jnp.float32)
    middle = rest.astype(jnp.bfloat16)
    return high, middle, (rest - middle.astype(jnp.float32)).astype(jnp.bfloat16)


def sum_pieces(pieces):
    high, middle, low = (p.astype(jnp.float32) for p in pieces)
    return high + (middle + low)


def packed(rows, width, share):
    return PIECES * rows <= width and 2 * share <= 8 and rows % LANES == 0


def calls_of(order):
    return [groups for groups in (order[:1], order[1:-1], order[-1:] if order[1:] else []) if groups]


def attend_heads(groups, share, per_copy, valid, q_of, k_of, v_of, cos_ref, sin_ref, outs, stats):
    rows = cos_ref.shape[0]
    even = lax.broadcasted_iota(jnp.int32, (rows, HD), 1) % 2 == 0
    lane = lax.broadcasted_iota(jnp.int32, (rows, LANES), 1)
    scale = 1.0 / math.sqrt(HD)
    held = jnp.zeros((rows, LANES), jnp.float32)
    parts = share // per_copy
    for slot in range(len(groups) * parts):
        g, part = divmod(slot, parts)
        for i in range(per_copy):
            head = part * per_copy + i
            at = slice(i * HD, (i + 1) * HD)
            to = slice(head * HD, (head + 1) * HD)
            wide = q_of(g, to).astype(jnp.float32)
            partner = jnp.where(even, pltpu.roll(wide, HD - 1, 1), pltpu.roll(wide, 1, 1))
            rotated = (wide * cos_ref[...] + partner * sin_ref[...]).astype(jnp.bfloat16)
            scores = lax.dot_general(
                rotated,
                k_of(slot, at),
                (((1,), (1,)), ((), ())),
                preferred_element_type=jnp.float32,
            )
            scores = jnp.where(valid, scores, jnp.float32(-1e30))
            block_max = jnp.maximum(jnp.max(scores, axis=1, keepdims=True), -1e29)
            weights = jnp.exp((scores - block_max) * scale)
            block_total = jnp.sum(weights, axis=1, keepdims=True)
            block_out = jnp.dot(
                weights.astype(jnp.bfloat16), v_of(slot, at), preferred_element_type=jnp.float32
            )
            outs[g][:rows, to] = block_out.astype(jnp.bfloat16)
            held = jnp.where(lane == head, block_max * scale, held)
            held = jnp.where(lane == share + head, block_total, held)
        if part == parts - 1:
            flat = held.T
            if stats:
                stats[g][...] = flat[: 2 * share]
            else:
                extra = outs[g].shape[0] - rows
                for p, piece in enumerate(pieces_of(flat[:extra])):
                    outs[g][rows:, p * rows : (p + 1) * rows] = piece


def valid_keys(length_ref, keys):
    return (
        lax.broadcasted_iota(jnp.int32, (1, keys), 1)
        < length_ref[0] - lax.axis_index("tm") * keys
    )


def attend_kernel(calls, share, per_copy, row_cuts, joined, *refs):
    length_ref, pos_ref, q_hbm, k_hbm, v_hbm = refs[:5]
    groups = calls[0]
    n = len(groups)
    outs, refs = refs[5 : 5 + n], refs[5 + n :]
    stats, refs = ([], refs) if joined else (refs[:n], refs[n:])
    cos_ref, sin_ref, refs = refs[0], refs[1], refs[2:]
    kept, refs = refs[: 3 * len(calls) - 3], refs[3 * len(calls) - 3 :]
    q_buf, k_buf, v_buf, sem = refs
    rows = q_hbm.shape[0]
    keys = k_hbm.shape[0]
    own = lax.axis_index("tm") // row_cuts
    width = per_copy * HD
    parts = share // per_copy
    copies = []

    def start(from_ref, to_ref):
        copies.append(pltpu.make_async_copy(from_ref, to_ref, sem.at[len(copies)]))
        copies[-1].start()
        return copies[-1]

    first_copies = []
    for c, call in enumerate(calls):
        to = (q_buf, k_buf, v_buf) if c == 0 else kept[3 * c - 3 : 3 * c]
        for g, a in enumerate(call):
            first = pl.multiple_of((own ^ a) * share * HD, HD)
            wanted = [start(q_hbm.at[:, pl.ds(first, share * HD)], to[0].at[g])]
            for part in range(parts):
                slot = g * parts + part
                column = pl.multiple_of(first + part * width, HD)
                wanted += [
                    start(hbm.at[:, pl.ds(column, width)], buf.at[slot])
                    for hbm, buf in ((k_hbm, to[1]), (v_hbm, to[2]))
                ]
                if c == 0:
                    first_copies.append(wanted)
                    wanted = []
    lane = lax.broadcasted_iota(jnp.int32, (1, HD), 1)
    frequencies = jnp.exp((lane - lane % 2).astype(jnp.float32) * (-math.log(10000.0) / HD))
    place = jnp.broadcast_to(pos_ref[...].astype(jnp.float32), (HD, rows)).T
    angles = place * frequencies
    cos_ref[...] = jnp.cos(angles)
    sine = jnp.sin(angles)
    sin_ref[...] = jnp.where(lane % 2 == 0, -sine, sine)
    done = set()

    def near(buf):
        def read(slot, at):
            if slot not in done:
                done.add(slot)
                for copy in first_copies[slot]:
                    copy.wait()
            return buf[slot, :, at]

        return read

    def query(g, at):
        if g * parts not in done:
            done.add(g * parts)
            for copy in first_copies[g * parts]:
                copy.wait()
        return q_buf[g, :, at]

    attend_heads(
        groups,
        share,
        per_copy,
        valid_keys(length_ref, keys),
        query,
        near(k_buf),
        near(v_buf),
        cos_ref,
        sin_ref,
        outs,
        stats,
    )
    for copy in copies[sum(len(wanted) for wanted in first_copies) :]:
        copy.wait()


def attend_near_kernel(groups, share, per_copy, joined, *refs):
    length_ref, cos_ref, sin_ref, q_ref, k_ref, v_ref = refs[:6]
    n = len(groups)
    outs, stats = refs[6 : 6 + n], [] if joined else refs[6 + n :]
    attend_heads(
        groups,
        share,
        per_copy,
        valid_keys(length_ref, k_ref.shape[1]),
        lambda g, at: q_ref[g, :, at],
        lambda slot, at: k_ref[slot, :, at],
        lambda slot, at: v_ref[slot, :, at],
        cos_ref,
        sin_ref,
        outs,
        stats,
    )


def attend(queries, keys, values, positions, cache_length, calls, share, row_cuts):
    rows = queries.shape[0]
    key_count = keys.shape[0]
    per_copy = 2 if share % 2 == 0 else 1
    wide = share * HD
    joined = row_cuts == 1 and packed(rows, wide, share)
    table = jax.ShapeDtypeStruct((rows, HD), jnp.float32)

    def blocks(n):
        shapes = [jax.ShapeDtypeStruct((rows + 8 * joined, wide), jnp.bfloat16)] * n
        if not joined:
            shapes = shapes + [jax.ShapeDtypeStruct((2 * share, rows), jnp.float32)] * n
        return shapes

    def near(n):
        cache = (n * share // per_copy, key_count, per_copy * HD)
        return [((n, rows, wide), jnp.bfloat16), (cache, jnp.bfloat16), (cache, jnp.bfloat16)]

    def price(n):
        return pl.CostEstimate(
            flops=4 * n * share * rows * key_count * HD,
            bytes_accessed=4 * n * share * key_count * HD,
            transcendentals=n * share * rows * key_count,
        )

    def found(result, n):
        return list(zip(result[:n], [None] * n if joined else result[n : 2 * n]))

    n = len(calls[0])
    out_shape = blocks(n) + [table] * 2
    for call in calls[1:]:
        out_shape = out_shape + [jax.ShapeDtypeStruct(*entry) for entry in near(len(call))]
    count = sum(len(call) for call in calls) * (1 + 2 * share // per_copy)
    result = pl.pallas_call(
        functools.partial(attend_kernel, calls, share, per_copy, row_cuts, joined),
        in_specs=[SMEM, VMEM] + [HBM] * 3,
        out_specs=[VMEM] * len(out_shape),
        out_shape=out_shape,
        scratch_shapes=[pltpu.VMEM(*entry) for entry in near(n)]
        + [pltpu.SemaphoreType.DMA((count,))],
        cost_estimate=price(n),
        compiler_params=mib(ATTEND_MIB),
        name="attend",
    )(cache_length, positions[None], queries, keys, values)
    skip = len(blocks(n))
    tables, kept = result[skip : skip + 2], result[skip + 2 :]
    blocks_of = [found(result, n)]
    for c, call in enumerate(calls[1:]):
        n = len(call)
        result = pl.pallas_call(
            functools.partial(attend_near_kernel, call, share, per_copy, joined),
            in_specs=[SMEM] + [VMEM] * 5,
            out_specs=[VMEM] * len(blocks(n)),
            out_shape=blocks(n),
            cost_estimate=price(n),
            compiler_params=mib(16),
            name="attend_near",
        )(cache_length, *tables, *kept[3 * c : 3 * c + 3])
        blocks_of.append(found(result, n))
    return blocks_of


def merge_kernel(count, share, *refs):
    out_ref = refs[-1]
    rows = out_ref.shape[0]
    outs, stats = refs[:count], refs[count:-1]
    if stats:
        tables = [s[...] for s in stats]
    else:
        tables = [
            sum_pieces([o[rows:, p * rows : (p + 1) * rows] for p in range(PIECES)]) for o in outs
        ]
    maxima = [s[:share] for s in tables]
    totals = [s[share : 2 * share] for s in tables]
    top = functools.reduce(jnp.maximum, maxima)
    factors = [jnp.exp(m - top) for m in maxima]
    total = sum(f * s for f, s in zip(factors, totals))
    scales = [f / total for f in factors]
    pad = -(count * share) % LANES
    table = jnp.concatenate(scales + [jnp.zeros((pad, rows), jnp.float32)], axis=0).T
    for head in range(share):
        at = slice(head * HD, (head + 1) * HD)
        value = sum(
            o[:rows, at].astype(jnp.float32) * table[:, i * share + head : i * share + head + 1]
            for i, o in enumerate(outs)
        )
        out_ref[:, at] = value.astype(jnp.bfloat16)


def merge(outs, stats, share, rows):
    width = outs[0].shape[1]
    stats = [s for s in stats if s is not None]
    return pl.pallas_call(
        functools.partial(merge_kernel, len(outs), share),
        in_specs=[VMEM] * (len(outs) + len(stats)),
        out_specs=VMEM,
        out_shape=jax.ShapeDtypeStruct((rows, width), jnp.bfloat16),
        cost_estimate=cost(4 * len(outs) * rows * width, 0, *outs, *stats),
        compiler_params=mib(4),
        name="merge",
    )(*outs, *stats)


def project_kernel(cuts, later, row_cuts, *refs):
    parts, refs = refs[: len(cuts)], refs[len(cuts) :]
    w_hbm, total_ref, kept_ref, w_buf, sem = refs
    own = lax.axis_index("tm") // row_cuts
    depth = w_buf.shape[1]
    copies = []
    for i, a in enumerate((*cuts, *later)):
        first = pl.multiple_of((own ^ a) * depth, depth)
        to = w_buf.at[i] if i < len(cuts) else kept_ref.at[i - len(cuts)]
        copies.append(pltpu.make_async_copy(w_hbm.at[pl.ds(first, depth)], to, sem.at[i]))
        copies[i].start()
    for i, part in enumerate(parts):
        copies[i].wait()
        product = jnp.dot(part[...], w_buf[i], preferred_element_type=jnp.float32)
        total_ref[...] = product + total_ref[...] if i else product
    for copy in copies[len(cuts) :]:
        copy.wait()


def project(parts, cuts, later, weight, row_cuts):
    rows, depth = parts[0].shape
    columns = weight.shape[1]
    return pl.pallas_call(
        functools.partial(project_kernel, cuts, later, row_cuts),
        in_specs=[VMEM] * len(parts) + [HBM],
        out_specs=[VMEM, VMEM],
        out_shape=[
            jax.ShapeDtypeStruct((rows, columns), jnp.float32),
            jax.ShapeDtypeStruct((len(later), depth, columns), weight.dtype),
        ],
        scratch_shapes=[
            pltpu.VMEM((len(cuts), depth, columns), weight.dtype),
            pltpu.SemaphoreType.DMA((len(cuts) + len(later),)),
        ],
        cost_estimate=cost(2 * len(parts) * rows * depth * columns, 0, weight),
        compiler_params=mib(16),
        name="project",
    )(*parts, weight)


def project_rest_kernel(count, total_ref, kept_ref, *refs):
    parts, (keep_ref, send_ref, whole_ref) = refs[:count], refs[count:]
    value = total_ref[...]
    for i, part in enumerate(parts):
        value = value + jnp.dot(part[...], kept_ref[i], preferred_element_type=jnp.float32)
    chips, rows = keep_ref.shape[:2]
    core = lax.axis_index("heads") % 2
    for chip in range(chips):
        for c in range(2):
            first = (2 * chip + c) * rows
            whole_ref[c, chip] = value[first : first + rows]
    keep_ref[...] = whole_ref[core]
    send_ref[...] = whole_ref[1 - core].astype(jnp.bfloat16)


def project_rest(total, kept, parts, chips):
    rows, columns = total.shape
    block = (chips, rows // (2 * chips), columns)
    return pl.pallas_call(
        functools.partial(project_rest_kernel, len(parts)),
        in_specs=[VMEM] * (2 + len(parts)),
        out_specs=[VMEM, VMEM],
        out_shape=[
            jax.ShapeDtypeStruct(block, jnp.float32),
            jax.ShapeDtypeStruct(block, jnp.bfloat16),
        ],
        scratch_shapes=[pltpu.VMEM((2, *block), jnp.float32)],
        cost_estimate=cost(2 * rows * columns * kept.shape[0] * kept.shape[1], 0, kept),
        compiler_params=mib(16),
        name="project_rest",
    )(total, kept, *parts)


def pair_kernel(keep_ref, got_ref, mine_ref, *send_refs):
    chip = lax.axis_index("heads") // 2
    mine_ref[...] = keep_ref[chip] + got_ref[chip].astype(jnp.float32)
    for s, send_ref in enumerate(send_refs, 1):
        send_ref[...] = (keep_ref[chip ^ s] + got_ref[chip ^ s].astype(jnp.float32)).astype(
            jnp.bfloat16
        )


def pair_sum(keep, got):
    chips, rows, columns = keep.shape
    result = pl.pallas_call(
        pair_kernel,
        in_specs=[VMEM] * 2,
        out_specs=[VMEM] * chips,
        out_shape=[jax.ShapeDtypeStruct((rows, columns), jnp.float32)]
        + [jax.ShapeDtypeStruct((rows, columns), jnp.bfloat16)] * (chips - 1),
        cost_estimate=cost(chips * rows * columns, 0, keep, got),
        compiler_params=mib(8),
        name="pair",
    )(keep, got)
    return result[0], result[1:]


def condition_kernel(chips, shards, own_rows, mine_ref, residual_ref, gain_ref, *refs):
    got, refs = refs[: chips - 1], refs[chips - 1 :]
    weights, refs = refs[:shards], refs[shards:]
    rows = mine_ref.shape[0]
    h = lax.axis_index("heads")
    hidden = residual_ref[h].astype(jnp.float32) + mine_ref[...]
    for ref in got:
        hidden = hidden + ref[...].astype(jnp.float32)
    squares = jnp.sum(hidden * hidden, axis=1, keepdims=True)
    scaled = (hidden * gain_ref[...]).astype(jnp.bfloat16)
    width = weights[0].shape[1]
    products = [jnp.dot(scaled, w[...], preferred_element_type=jnp.float32) for w in weights]
    tail = jnp.zeros((rows, LANES), jnp.float32)
    lane = lax.broadcasted_iota(jnp.int32, (rows, LANES), 1)
    for p, piece in enumerate(pieces_of(squares)):
        tail = jnp.where(lane == p, piece.astype(jnp.float32), tail)
    if own_rows % 8 == 0 and width % LANES == 0:
        outs, held = refs[:-1], refs[-1]
        t = lax.axis_index("tm")
        for s, product in enumerate(products):
            held[:, pl.ds(pl.multiple_of((h ^ s) * width, LANES), width)] = product
        held[:, shards * width :] = tail
        for s, out_ref in enumerate(outs):
            first = pl.multiple_of((t ^ s) * own_rows, own_rows)
            out_ref[...] = held[pl.ds(first, own_rows), :].astype(jnp.bfloat16)
    else:
        for s, product in enumerate(products):
            refs[0][:, s * width : (s + 1) * width] = product.astype(jnp.bfloat16)
        refs[0][:, shards * width :] = tail.astype(jnp.bfloat16)


def condition_parts(mine, got, residual, gain, weights, n_tm, h, t):
    rows, depth = mine.shape
    shards = len(weights)
    width = weights[0].shape[1]
    full = shards * width + LANES
    own_rows = rows // n_tm
    aligned = own_rows % 8 == 0 and width % LANES == 0
    block = jax.ShapeDtypeStruct((own_rows, full), jnp.bfloat16)
    out_shape = [block] * n_tm if aligned else [jax.ShapeDtypeStruct((rows, full), jnp.bfloat16)]
    result = pl.pallas_call(
        functools.partial(condition_kernel, len(got) + 1, shards, own_rows),
        in_specs=[VMEM] * (3 + len(got) + shards),
        out_specs=[VMEM] * len(out_shape),
        out_shape=out_shape,
        scratch_shapes=[pltpu.VMEM((rows, full), jnp.float32)] * aligned,
        cost_estimate=cost(2 * rows * depth * full, 0, *weights),
        compiler_params=mib(12),
        name="condition",
    )(mine, residual.reshape(-1, rows, depth), gain[None, :], *got, *weights)
    if aligned:
        return result
    columns = result[0][:, :-LANES].reshape(rows, shards, width)
    columns = jnp.take(columns, jnp.arange(shards) ^ h, axis=1).reshape(rows, shards * width)
    result = jnp.concatenate([columns, result[0][:, -LANES:]], axis=1)
    result = result.reshape(n_tm, own_rows, full)
    return [pick(result, t ^ s) for s in range(n_tm)]


def sweep_kernel(sizes, steps, start_ref, embed_ref, in_ref, head_ref, *refs):
    n_tm, time_each, rows, model = sizes
    noise_refs, refs = refs[:n_tm], refs[n_tm:]
    parts, refs = refs[:n_tm], refs[n_tm:]
    outs, held = refs[:n_tm], refs[n_tm]
    t = lax.axis_index("tm")
    times = n_tm * time_each
    start = start_ref[t]
    chan = start.shape[1]
    for s, ref in enumerate(noise_refs):
        held[t ^ s] = ref[...].astype(jnp.float32)

    def block(i):
        at = (i % time_each) * rows
        return i // time_each, slice(at, at + rows)

    noise = [steps[times + i] * held[block(i)] for i in range(times - 1)]
    width = in_ref.shape[1]
    opening = jnp.dot(start.astype(jnp.bfloat16), in_ref[...], preferred_element_type=jnp.float32)
    total = sum(p[...].astype(jnp.float32) for p in parts)
    squares = total[:, width : width + 1]
    for p in range(1, PIECES):
        squares = squares + total[:, width + p : width + p + 1]
    condition = total[:, :width] * lax.rsqrt(squares / model + 1e-06)

    def increments_at(first, products):
        last = first + len(products)
        inside = jnp.concatenate(
            [p + (condition + embed_ref[i : i + 1]) for i, p in enumerate(products, first)], axis=0
        )
        action = (inside * jax.nn.sigmoid(inside)).astype(jnp.bfloat16)
        drift = jnp.dot(action, head_ref[...], preferred_element_type=jnp.float32)
        return [
            steps[i] * drift[(i - first) * rows : (i - first + 1) * rows] + noise[i]
            for i in range(first, last)
        ]

    increments = increments_at(0, [opening] * (times - 1))
    for sweep in range(1, SWEEPS + 1):
        change = [jnp.zeros((rows, chan), jnp.float32)]
        for i in range(times - 1):
            change.append(change[-1] + increments[i])
        if sweep == SWEEPS or sweep >= times - 1:
            break
        states = jnp.concatenate([start + change[i] for i in range(sweep, times - 1)], axis=0)
        product = jnp.dot(
            states.astype(jnp.bfloat16), in_ref[...], preferred_element_type=jnp.float32
        )
        increments = increments[:sweep] + increments_at(
            sweep, [product[i * rows : (i + 1) * rows] for i in range(times - 1 - sweep)]
        )
    for i in range(times):
        held[block(i)] = change[i]
    for s, out_ref in enumerate(outs):
        out_ref[...] = held[t ^ s].astype(jnp.bfloat16)


def sweep_all(parts, noise, embedding, steps, start, in_weight, head_out, time_each, model):
    n_tm, rows, chan = start.shape
    block = (time_each * rows, chan)
    return pl.pallas_call(
        functools.partial(sweep_kernel, (n_tm, time_each, rows, model)),
        in_specs=[SMEM] + [VMEM] * (4 + 2 * n_tm),
        out_specs=[VMEM] * n_tm,
        out_shape=[jax.ShapeDtypeStruct(block, jnp.bfloat16)] * n_tm,
        scratch_shapes=[pltpu.VMEM((n_tm, *block), jnp.float32)],
        cost_estimate=cost(
            10 * n_tm * time_each * rows * chan * in_weight.shape[1], 0, in_weight, head_out
        ),
        compiler_params=mib(16),
        name="sweeps",
    )(steps, start, embedding, in_weight, head_out, *noise, *parts)


def noise_kernel(time_each, noise_ref, *outs):
    t = lax.axis_index("tm")
    rows = noise_ref.shape[1]
    for s, out_ref in enumerate(outs):
        block = noise_ref[t ^ s].astype(jnp.float32)
        for i in range(time_each):
            out_ref[i * rows : (i + 1) * rows] = block[:, i, :].astype(jnp.bfloat16)


def noise_blocks(noise_draws, n_tm):
    rows, time_each, chan = noise_draws.shape
    own_rows = rows // n_tm
    block = jax.ShapeDtypeStruct((time_each * own_rows, chan), noise_draws.dtype)
    return pl.pallas_call(
        functools.partial(noise_kernel, time_each),
        in_specs=[VMEM],
        out_specs=[VMEM] * n_tm,
        out_shape=[block] * n_tm,
        cost_estimate=cost(0, 0, noise_draws, noise_draws),
        compiler_params=mib(4),
        name="noise",
    )(noise_draws.reshape(n_tm, own_rows, time_each, chan))


def finish_kernel(sizes, start_ref, *refs):
    time_each, rows = sizes
    parts, out_ref = refs[:-1], refs[-1]
    t = lax.axis_index("tm")
    for s, part in enumerate(parts):
        start = start_ref[t ^ s]
        for i in range(time_each):
            out_ref[pl.ds((t ^ s) * rows, rows), i, :] = start + part[
                i * rows : (i + 1) * rows
            ].astype(jnp.float32)


def finish(start, parts, time_each):
    n_tm, rows, chan = start.shape
    return pl.pallas_call(
        functools.partial(finish_kernel, (time_each, rows)),
        in_specs=[VMEM] * (1 + len(parts)),
        out_specs=VMEM,
        out_shape=jax.ShapeDtypeStruct((n_tm * rows, time_each, chan), jnp.float32),
        cost_estimate=cost(n_tm * rows * time_each * chan, 0, start, *parts),
        compiler_params=mib(4),
        name="finish",
    )(start, *parts)


def shards(
    queries,
    cache_keys,
    cache_values,
    residual,
    out_weight,
    norm_gain,
    cond_weight,
    in_weight,
    head_out,
    start_state,
    noise_draws,
    positions,
    cache_length,
    plan,
):
    rows, width = queries.shape
    n_heads = lax.axis_size("heads")
    n_tm = lax.axis_size("tm")
    h = lax.axis_index("heads")
    t = lax.axis_index("tm")
    local_heads = width // HD
    model = out_weight.shape[1] * n_tm
    row_each, time_each, chan = noise_draws.shape
    own_rows = row_each // n_tm
    hidden_width = in_weight.shape[1]

    head_cuts = math.gcd(local_heads, n_tm)
    row_cuts = n_tm // head_cuts
    share = local_heads // head_cuts
    own_row_cut = t % row_cuts

    def cut(values, index, axis):
        if row_cuts == 1:
            return values
        size = values.shape[axis] // row_cuts
        return lax.dynamic_slice_in_dim(values, index * size, size, axis)

    chips = n_heads // 2
    far = []
    for s in range(1, chips):
        far.append(swap(cond_weight, "heads", 2 * s))
    near = swap(cond_weight, "heads", 1)

    order = list(range(head_cuts))[::-1]
    outs, stats = [None] * n_tm, [None] * n_tm
    calls = calls_of(order)
    found = attend(
        queries, cache_keys, cache_values, positions, cache_length, calls, share, row_cuts
    )
    for groups, blocks in zip(calls, found):
        for a, (out, stat) in zip(groups, blocks):
            for b in range(row_cuts):
                s = a * row_cuts + b
                outs[s] = cut(out, own_row_cut ^ b, 0)
                stats[s] = None if stat is None else cut(stat, own_row_cut ^ b, 1)
                if s:
                    outs[s] = swap(outs[s], "tm", s)
                    stats[s] = None if stat is None else swap(stats[s], "tm", s)
    attended = merge(outs, stats, share, rows // row_cuts)
    parts = exchange([attended] * n_tm)
    by_cut = []
    for a in range(head_cuts):
        part = parts[a * row_cuts : (a + 1) * row_cuts]
        if row_cuts > 1:
            part = jnp.take(jnp.stack(part), jnp.arange(row_cuts) ^ own_row_cut, axis=0)
            part = part.reshape(rows, share * HD)
        else:
            part = part[0]
        by_cut.append(part)
    half = max(1, head_cuts // 2)
    cuts = list(range(head_cuts))
    total, kept = project(by_cut[:half], cuts[:half], cuts[half:], out_weight, row_cuts)
    keep, send = project_rest(total, kept, by_cut[half:], chips)

    far, send = lax.optimization_barrier((far, send))
    other = swap(send, "heads", 1)
    mine, far_rows = pair_sum(keep, other)
    got = []
    for s, r in enumerate(far_rows, 1):
        got.append(swap(r, "heads", 2 * s))

    cond_shards = [cond_weight, near]
    for s, w in enumerate(far, 1):
        cond_shards += [w, swap(w, "heads", 1)]

    cond = condition_parts(mine, got, residual, norm_gain, cond_shards, n_tm, h, t)
    cond = exchange(cond)

    noise = noise_blocks(noise_draws, n_tm)
    noise = exchange(noise)
    levels = plan.astype(jnp.float32)
    half_width = hidden_width // 2
    frequencies = jnp.exp(
        -math.log(10000.0) * jnp.arange(half_width, dtype=jnp.float32) / half_width
    )
    angles = levels[:-1, None] * frequencies[None, :]
    embedding = jnp.concatenate([jnp.sin(angles), jnp.cos(angles)], axis=1)
    step_size = (levels[:-1] - levels[1:]) / 1000.0
    steps = jnp.concatenate([step_size, jnp.sqrt(step_size)])
    start = start_state.reshape(n_tm, own_rows, chan)
    change = sweep_all(
        cond, noise, embedding, steps, start, in_weight, head_out, time_each, model
    )
    back = exchange(change)
    return finish(start, back, time_each)


def solution(mesh):
    placed = (
        P("groups", "heads"),
        P(("groups", "tm"), "heads"),
        P(("groups", "tm"), "heads"),
        P("groups", "tm"),
        P("heads", "tm"),
        P("tm"),
        P("tm", "heads"),
        P(),
        P(),
        P(("groups", "heads"), None),
        P(("groups", "heads"), "tm", None),
        P("groups"),
        P("groups"),
        P(),
    )

    return jax.shard_map(
        shards,
        mesh=mesh,
        in_specs=placed,
        out_specs=P(("groups", "heads"), "tm", None),
        check_vma=False,
    )
```

```python
import functools
import math

import jax
import jax.numpy as jnp
from jax import lax
from jax.experimental import pallas as pl
from jax.experimental.pallas import tpu as pltpu
from jax.sharding import PartitionSpec as P


HD = 128
SWEEPS = 3
LANES = 128


def swap(values, axis, distance):
    size = lax.axis_size(axis)
    return lax.ppermute(values, axis, [(i, i ^ distance) for i in range(size)])


def exchange(blocks):
    got = [blocks[0]]
    for s, block in enumerate(blocks[1:], 1):
        got.append(swap(block, "tm", s))
    return got


def pick(values, index):
    return lax.dynamic_index_in_dim(values, index, 0, False)


def cost(flops, transcendentals, *arrays):
    moved = sum(math.prod(a.shape) * jnp.dtype(a.dtype).itemsize for a in arrays)
    return pl.CostEstimate(flops=flops, bytes_accessed=moved, transcendentals=transcendentals)


def mib(count):
    return pltpu.CompilerParams(vmem_limit_bytes=count * 1024 * 1024)


VMEM = pl.BlockSpec(memory_space=pltpu.VMEM)
SMEM = pl.BlockSpec(memory_space=pltpu.SMEM)
HBM = pl.BlockSpec(memory_space=pltpu.HBM)
PIECES = 3
ATTEND_MIB = 44


def pieces_of(value):
    high = value.astype(jnp.bfloat16)
    rest = value - high.astype(jnp.float32)
    middle = rest.astype(jnp.bfloat16)
    return high, middle, (rest - middle.astype(jnp.float32)).astype(jnp.bfloat16)


def sum_pieces(pieces):
    high, middle, low = (p.astype(jnp.float32) for p in pieces)
    return high + (middle + low)


def packed(rows, width, share):
    return PIECES * rows <= width and 2 * share <= 8 and rows % LANES == 0


def calls_of(order):
    return [groups for groups in (order[:1], order[1:-1], order[-1:] if order[1:] else []) if groups]


def attend_heads(groups, share, per_copy, valid, q_of, k_of, v_of, cos_ref, sin_ref, outs, stats):
    rows = cos_ref.shape[0]
    even = lax.broadcasted_iota(jnp.int32, (rows, HD), 1) % 2 == 0
    lane = lax.broadcasted_iota(jnp.int32, (rows, LANES), 1)
    scale = 1.0 / math.sqrt(HD)
    held = jnp.zeros((rows, LANES), jnp.float32)
    parts = share // per_copy
    for slot in range(len(groups) * parts):
        g, part = divmod(slot, parts)
        for i in range(per_copy):
            head = part * per_copy + i
            at = slice(i * HD, (i + 1) * HD)
            to = slice(head * HD, (head + 1) * HD)
            wide = q_of(g, to).astype(jnp.float32)
            partner = jnp.where(even, pltpu.roll(wide, HD - 1, 1), pltpu.roll(wide, 1, 1))
            rotated = (wide * cos_ref[...] + partner * sin_ref[...]).astype(jnp.bfloat16)
            scores = lax.dot_general(
                rotated,
                k_of(slot, at),
                (((1,), (1,)), ((), ())),
                preferred_element_type=jnp.float32,
            )
            scores = jnp.where(valid, scores, jnp.float32(-1e30))
            block_max = jnp.maximum(jnp.max(scores, axis=1, keepdims=True), -1e29)
            weights = jnp.exp((scores - block_max) * scale)
            block_total = jnp.sum(weights, axis=1, keepdims=True)
            block_out = jnp.dot(
                weights.astype(jnp.bfloat16), v_of(slot, at), preferred_element_type=jnp.float32
            )
            outs[g][:rows, to] = block_out.astype(jnp.bfloat16)
            held = jnp.where(lane == head, block_max * scale, held)
            held = jnp.where(lane == share + head, block_total, held)
        if part == parts - 1:
            flat = held.T
            if stats:
                stats[g][...] = flat[: 2 * share]
            else:
                extra = outs[g].shape[0] - rows
                for p, piece in enumerate(pieces_of(flat[:extra])):
                    outs[g][rows:, p * rows : (p + 1) * rows] = piece


def valid_keys(length_ref, keys):
    return (
        lax.broadcasted_iota(jnp.int32, (1, keys), 1)
        < length_ref[0] - lax.axis_index("tm") * keys
    )


def attend_kernel(calls, share, per_copy, row_cuts, joined, *refs):
    length_ref, pos_ref, q_hbm, k_hbm, v_hbm = refs[:5]
    groups = calls[0]
    n = len(groups)
    outs, refs = refs[5 : 5 + n], refs[5 + n :]
    stats, refs = ([], refs) if joined else (refs[:n], refs[n:])
    cos_ref, sin_ref, refs = refs[0], refs[1], refs[2:]
    kept, refs = refs[: 3 * len(calls) - 3], refs[3 * len(calls) - 3 :]
    q_buf, k_buf, v_buf, sem = refs
    rows = q_hbm.shape[0]
    keys = k_hbm.shape[0]
    own = lax.axis_index("tm") // row_cuts
    width = per_copy * HD
    parts = share // per_copy
    copies = []

    def start(from_ref, to_ref):
        copies.append(pltpu.make_async_copy(from_ref, to_ref, sem.at[len(copies)]))
        copies[-1].start()
        return copies[-1]

    first_copies = []
    for c, call in enumerate(calls):
        to = (q_buf, k_buf, v_buf) if c == 0 else kept[3 * c - 3 : 3 * c]
        for g, a in enumerate(call):
            first = pl.multiple_of((own ^ a) * share * HD, HD)
            wanted = [start(q_hbm.at[:, pl.ds(first, share * HD)], to[0].at[g])]
            for part in range(parts):
                slot = g * parts + part
                column = pl.multiple_of(first + part * width, HD)
                wanted += [
                    start(hbm.at[:, pl.ds(column, width)], buf.at[slot])
                    for hbm, buf in ((k_hbm, to[1]), (v_hbm, to[2]))
                ]
                if c == 0:
                    first_copies.append(wanted)
                    wanted = []
    lane = lax.broadcasted_iota(jnp.int32, (1, HD), 1)
    frequencies = jnp.exp((lane - lane % 2).astype(jnp.float32) * (-math.log(10000.0) / HD))
    place = jnp.broadcast_to(pos_ref[...].astype(jnp.float32), (HD, rows)).T
    angles = place * frequencies
    cos_ref[...] = jnp.cos(angles)
    sine = jnp.sin(angles)
    sin_ref[...] = jnp.where(lane % 2 == 0, -sine, sine)
    done = set()

    def near(buf):
        def read(slot, at):
            if slot not in done:
                done.add(slot)
                for copy in first_copies[slot]:
                    copy.wait()
            return buf[slot, :, at]

        return read

    def query(g, at):
        if g * parts not in done:
            done.add(g * parts)
            for copy in first_copies[g * parts]:
                copy.wait()
        return q_buf[g, :, at]

    attend_heads(
        groups,
        share,
        per_copy,
        valid_keys(length_ref, keys),
        query,
        near(k_buf),
        near(v_buf),
        cos_ref,
        sin_ref,
        outs,
        stats,
    )
    for copy in copies[sum(len(wanted) for wanted in first_copies) :]:
        copy.wait()


def attend_near_kernel(groups, share, per_copy, joined, *refs):
    length_ref, cos_ref, sin_ref, q_ref, k_ref, v_ref = refs[:6]
    n = len(groups)
    outs, stats = refs[6 : 6 + n], [] if joined else refs[6 + n :]
    attend_heads(
        groups,
        share,
        per_copy,
        valid_keys(length_ref, k_ref.shape[1]),
        lambda g, at: q_ref[g, :, at],
        lambda slot, at: k_ref[slot, :, at],
        lambda slot, at: v_ref[slot, :, at],
        cos_ref,
        sin_ref,
        outs,
        stats,
    )


def attend(queries, keys, values, positions, cache_length, calls, share, row_cuts):
    rows = queries.shape[0]
    key_count = keys.shape[0]
    per_copy = 2 if share % 2 == 0 else 1
    wide = share * HD
    joined = row_cuts == 1 and packed(rows, wide, share)
    table = jax.ShapeDtypeStruct((rows, HD), jnp.float32)

    def blocks(n):
        shapes = [jax.ShapeDtypeStruct((rows + 8 * joined, wide), jnp.bfloat16)] * n
        if not joined:
            shapes = shapes + [jax.ShapeDtypeStruct((2 * share, rows), jnp.float32)] * n
        return shapes

    def near(n):
        cache = (n * share // per_copy, key_count, per_copy * HD)
        return [((n, rows, wide), jnp.bfloat16), (cache, jnp.bfloat16), (cache, jnp.bfloat16)]

    def price(n):
        return pl.CostEstimate(
            flops=4 * n * share * rows * key_count * HD,
            bytes_accessed=4 * n * share * key_count * HD,
            transcendentals=n * share * rows * key_count,
        )

    def found(result, n):
        return list(zip(result[:n], [None] * n if joined else result[n : 2 * n]))

    n = len(calls[0])
    out_shape = blocks(n) + [table] * 2
    for call in calls[1:]:
        out_shape = out_shape + [jax.ShapeDtypeStruct(*entry) for entry in near(len(call))]
    count = sum(len(call) for call in calls) * (1 + 2 * share // per_copy)
    result = pl.pallas_call(
        functools.partial(attend_kernel, calls, share, per_copy, row_cuts, joined),
        in_specs=[SMEM, VMEM] + [HBM] * 3,
        out_specs=[VMEM] * len(out_shape),
        out_shape=out_shape,
        scratch_shapes=[pltpu.VMEM(*entry) for entry in near(n)]
        + [pltpu.SemaphoreType.DMA((count,))],
        cost_estimate=price(n),
        compiler_params=mib(ATTEND_MIB),
        name="attend",
    )(cache_length, positions[None], queries, keys, values)
    skip = len(blocks(n))
    tables, kept = result[skip : skip + 2], result[skip + 2 :]
    blocks_of = [found(result, n)]
    for c, call in enumerate(calls[1:]):
        n = len(call)
        result = pl.pallas_call(
            functools.partial(attend_near_kernel, call, share, per_copy, joined),
            in_specs=[SMEM] + [VMEM] * 5,
            out_specs=[VMEM] * len(blocks(n)),
            out_shape=blocks(n),
            cost_estimate=price(n),
            compiler_params=mib(16),
            name="attend_near",
        )(cache_length, *tables, *kept[3 * c : 3 * c + 3])
        blocks_of.append(found(result, n))
    return blocks_of


def merge_kernel(count, share, *refs):
    out_ref = refs[-1]
    rows = out_ref.shape[0]
    outs, stats = refs[:count], refs[count:-1]
    if stats:
        tables = [s[...] for s in stats]
    else:
        tables = [
            sum_pieces([o[rows:, p * rows : (p + 1) * rows] for p in range(PIECES)]) for o in outs
        ]
    maxima = [s[:share] for s in tables]
    totals = [s[share : 2 * share] for s in tables]
    top = functools.reduce(jnp.maximum, maxima)
    factors = [jnp.exp(m - top) for m in maxima]
    total = sum(f * s for f, s in zip(factors, totals))
    scales = [f / total for f in factors]
    pad = -(count * share) % LANES
    table = jnp.concatenate(scales + [jnp.zeros((pad, rows), jnp.float32)], axis=0).T
    for head in range(share):
        at = slice(head * HD, (head + 1) * HD)
        value = sum(
            o[:rows, at].astype(jnp.float32) * table[:, i * share + head : i * share + head + 1]
            for i, o in enumerate(outs)
        )
        out_ref[:, at] = value.astype(jnp.bfloat16)


def merge(outs, stats, share, rows):
    width = outs[0].shape[1]
    stats = [s for s in stats if s is not None]
    return pl.pallas_call(
        functools.partial(merge_kernel, len(outs), share),
        in_specs=[VMEM] * (len(outs) + len(stats)),
        out_specs=VMEM,
        out_shape=jax.ShapeDtypeStruct((rows, width), jnp.bfloat16),
        cost_estimate=cost(4 * len(outs) * rows * width, 0, *outs, *stats),
        compiler_params=mib(4),
        name="merge",
    )(*outs, *stats)


def project_kernel(cuts, later, row_cuts, *refs):
    parts, refs = refs[: len(cuts)], refs[len(cuts) :]
    w_hbm, total_ref, kept_ref, w_buf, sem = refs
    own = lax.axis_index("tm") // row_cuts
    depth = w_buf.shape[1]
    copies = []
    for i, a in enumerate((*cuts, *later)):
        first = pl.multiple_of((own ^ a) * depth, depth)
        to = w_buf.at[i] if i < len(cuts) else kept_ref.at[i - len(cuts)]
        copies.append(pltpu.make_async_copy(w_hbm.at[pl.ds(first, depth)], to, sem.at[i]))
        copies[i].start()
    for i, part in enumerate(parts):
        copies[i].wait()
        product = jnp.dot(part[...], w_buf[i], preferred_element_type=jnp.float32)
        total_ref[...] = product + total_ref[...] if i else product
    for copy in copies[len(cuts) :]:
        copy.wait()


def project(parts, cuts, later, weight, row_cuts):
    rows, depth = parts[0].shape
    columns = weight.shape[1]
    return pl.pallas_call(
        functools.partial(project_kernel, cuts, later, row_cuts),
        in_specs=[VMEM] * len(parts) + [HBM],
        out_specs=[VMEM, VMEM],
        out_shape=[
            jax.ShapeDtypeStruct((rows, columns), jnp.float32),
            jax.ShapeDtypeStruct((len(later), depth, columns), weight.dtype),
        ],
        scratch_shapes=[
            pltpu.VMEM((len(cuts), depth, columns), weight.dtype),
            pltpu.SemaphoreType.DMA((len(cuts) + len(later),)),
        ],
        cost_estimate=cost(2 * len(parts) * rows * depth * columns, 0, weight),
        compiler_params=mib(16),
        name="project",
    )(*parts, weight)


def project_rest_kernel(count, total_ref, kept_ref, *refs):
    parts, (keep_ref, send_ref, whole_ref) = refs[:count], refs[count:]
    value = total_ref[...]
    for i, part in enumerate(parts):
        value = value + jnp.dot(part[...], kept_ref[i], preferred_element_type=jnp.float32)
    chips, rows = keep_ref.shape[:2]
    core = lax.axis_index("heads") % 2
    for chip in range(chips):
        for c in range(2):
            first = (2 * chip + c) * rows
            whole_ref[c, chip] = value[first : first + rows]
    keep_ref[...] = whole_ref[core]
    send_ref[...] = whole_ref[1 - core].astype(jnp.bfloat16)


def project_rest(total, kept, parts, chips):
    rows, columns = total.shape
    block = (chips, rows // (2 * chips), columns)
    return pl.pallas_call(
        functools.partial(project_rest_kernel, len(parts)),
        in_specs=[VMEM] * (2 + len(parts)),
        out_specs=[VMEM, VMEM],
        out_shape=[
            jax.ShapeDtypeStruct(block, jnp.float32),
            jax.ShapeDtypeStruct(block, jnp.bfloat16),
        ],
        scratch_shapes=[pltpu.VMEM((2, *block), jnp.float32)],
        cost_estimate=cost(2 * rows * columns * kept.shape[0] * kept.shape[1], 0, kept),
        compiler_params=mib(16),
        name="project_rest",
    )(total, kept, *parts)


def pair_kernel(keep_ref, got_ref, mine_ref, *send_refs):
    chip = lax.axis_index("heads") // 2
    mine_ref[...] = keep_ref[chip] + got_ref[chip].astype(jnp.float32)
    for s, send_ref in enumerate(send_refs, 1):
        send_ref[...] = (keep_ref[chip ^ s] + got_ref[chip ^ s].astype(jnp.float32)).astype(
            jnp.bfloat16
        )


def pair_sum(keep, got):
    chips, rows, columns = keep.shape
    result = pl.pallas_call(
        pair_kernel,
        in_specs=[VMEM] * 2,
        out_specs=[VMEM] * chips,
        out_shape=[jax.ShapeDtypeStruct((rows, columns), jnp.float32)]
        + [jax.ShapeDtypeStruct((rows, columns), jnp.bfloat16)] * (chips - 1),
        cost_estimate=cost(chips * rows * columns, 0, keep, got),
        compiler_params=mib(8),
        name="pair",
    )(keep, got)
    return result[0], result[1:]


def condition_kernel(chips, shards, own_rows, mine_ref, residual_ref, gain_ref, *refs):
    got, refs = refs[: chips - 1], refs[chips - 1 :]
    weights, refs = refs[:shards], refs[shards:]
    rows = mine_ref.shape[0]
    h = lax.axis_index("heads")
    hidden = residual_ref[h].astype(jnp.float32) + mine_ref[...]
    for ref in got:
        hidden = hidden + ref[...].astype(jnp.float32)
    squares = jnp.sum(hidden * hidden, axis=1, keepdims=True)
    scaled = (hidden * gain_ref[...]).astype(jnp.bfloat16)
    width = weights[0].shape[1]
    products = [jnp.dot(scaled, w[...], preferred_element_type=jnp.float32) for w in weights]
    tail = jnp.zeros((rows, LANES), jnp.float32)
    lane = lax.broadcasted_iota(jnp.int32, (rows, LANES), 1)
    for p, piece in enumerate(pieces_of(squares)):
        tail = jnp.where(lane == p, piece.astype(jnp.float32), tail)
    if own_rows % 8 == 0 and width % LANES == 0:
        outs, held = refs[:-1], refs[-1]
        t = lax.axis_index("tm")
        for s, product in enumerate(products):
            held[:, pl.ds(pl.multiple_of((h ^ s) * width, LANES), width)] = product
        held[:, shards * width :] = tail
        for s, out_ref in enumerate(outs):
            first = pl.multiple_of((t ^ s) * own_rows, own_rows)
            out_ref[...] = held[pl.ds(first, own_rows), :].astype(jnp.bfloat16)
    else:
        for s, product in enumerate(products):
            refs[0][:, s * width : (s + 1) * width] = product.astype(jnp.bfloat16)
        refs[0][:, shards * width :] = tail.astype(jnp.bfloat16)


def condition_parts(mine, got, residual, gain, weights, n_tm, h, t):
    rows, depth = mine.shape
    shards = len(weights)
    width = weights[0].shape[1]
    full = shards * width + LANES
    own_rows = rows // n_tm
    aligned = own_rows % 8 == 0 and width % LANES == 0
    block = jax.ShapeDtypeStruct((own_rows, full), jnp.bfloat16)
    out_shape = [block] * n_tm if aligned else [jax.ShapeDtypeStruct((rows, full), jnp.bfloat16)]
    result = pl.pallas_call(
        functools.partial(condition_kernel, len(got) + 1, shards, own_rows),
        in_specs=[VMEM] * (3 + len(got) + shards),
        out_specs=[VMEM] * len(out_shape),
        out_shape=out_shape,
        scratch_shapes=[pltpu.VMEM((rows, full), jnp.float32)] * aligned,
        cost_estimate=cost(2 * rows * depth * full, 0, *weights),
        compiler_params=mib(12),
        name="condition",
    )(mine, residual.reshape(-1, rows, depth), gain[None, :], *got, *weights)
    if aligned:
        return result
    columns = result[0][:, :-LANES].reshape(rows, shards, width)
    columns = jnp.take(columns, jnp.arange(shards) ^ h, axis=1).reshape(rows, shards * width)
    result = jnp.concatenate([columns, result[0][:, -LANES:]], axis=1)
    result = result.reshape(n_tm, own_rows, full)
    return [pick(result, t ^ s) for s in range(n_tm)]


def opening_kernel(start_ref, in_ref, out_ref):
    start = start_ref[lax.axis_index("tm")].astype(jnp.bfloat16)
    out_ref[...] = jnp.dot(start, in_ref[...], preferred_element_type=jnp.float32)


def opening_product(start, in_weight):
    rows, width = start.shape[1], in_weight.shape[1]
    return pl.pallas_call(
        opening_kernel,
        in_specs=[VMEM] * 2,
        out_specs=VMEM,
        out_shape=jax.ShapeDtypeStruct((rows, width), jnp.float32),
        cost_estimate=cost(2 * rows * in_weight.size, 0, in_weight),
        compiler_params=mib(8),
        name="opening",
    )(start, in_weight)


def sweep_kernel(sizes, steps, start_ref, embed_ref, in_ref, head_ref, opening_ref, *refs):
    n_tm, time_each, rows, model = sizes
    noise_refs, refs = refs[:n_tm], refs[n_tm:]
    parts, refs = refs[:n_tm], refs[n_tm:]
    outs, held = refs[:n_tm], refs[n_tm]
    t = lax.axis_index("tm")
    times = n_tm * time_each
    start = start_ref[t]
    chan = start.shape[1]
    for s, ref in enumerate(noise_refs):
        held[t ^ s] = ref[...].astype(jnp.float32)

    def block(i):
        at = (i % time_each) * rows
        return i // time_each, slice(at, at + rows)

    noise = [steps[times + i] * held[block(i)] for i in range(times - 1)]
    width = in_ref.shape[1]
    opening = opening_ref[...]
    total = sum(p[...].astype(jnp.float32) for p in parts)
    squares = total[:, width : width + 1]
    for p in range(1, PIECES):
        squares = squares + total[:, width + p : width + p + 1]
    condition = total[:, :width] * lax.rsqrt(squares / model + 1e-06)

    def increments_at(first, products):
        last = first + len(products)
        inside = jnp.concatenate(
            [p + (condition + embed_ref[i : i + 1]) for i, p in enumerate(products, first)], axis=0
        )
        action = (inside * jax.nn.sigmoid(inside)).astype(jnp.bfloat16)
        drift = jnp.dot(action, head_ref[...], preferred_element_type=jnp.float32)
        return [
            steps[i] * drift[(i - first) * rows : (i - first + 1) * rows] + noise[i]
            for i in range(first, last)
        ]

    increments = increments_at(0, [opening] * (times - 1))
    for sweep in range(1, SWEEPS + 1):
        change = [jnp.zeros((rows, chan), jnp.float32)]
        for i in range(times - 1):
            change.append(change[-1] + increments[i])
        if sweep == SWEEPS or sweep >= times - 1:
            break
        states = jnp.concatenate([start + change[i] for i in range(sweep, times - 1)], axis=0)
        product = jnp.dot(
            states.astype(jnp.bfloat16), in_ref[...], preferred_element_type=jnp.float32
        )
        increments = increments[:sweep] + increments_at(
            sweep, [product[i * rows : (i + 1) * rows] for i in range(times - 1 - sweep)]
        )
    for i in range(times):
        held[block(i)] = change[i]
    for s, out_ref in enumerate(outs):
        out_ref[...] = held[t ^ s].astype(jnp.bfloat16)


def sweep_all(parts, noise, embedding, steps, start, in_weight, head_out, time_each, model):
    n_tm, rows, chan = start.shape
    block = (time_each * rows, chan)
    opening = opening_product(start, in_weight)
    return pl.pallas_call(
        functools.partial(sweep_kernel, (n_tm, time_each, rows, model)),
        in_specs=[SMEM] + [VMEM] * (5 + 2 * n_tm),
        out_specs=[VMEM] * n_tm,
        out_shape=[jax.ShapeDtypeStruct(block, jnp.bfloat16)] * n_tm,
        scratch_shapes=[pltpu.VMEM((n_tm, *block), jnp.float32)],
        cost_estimate=cost(
            10 * n_tm * time_each * rows * chan * in_weight.shape[1], 0, in_weight, head_out
        ),
        compiler_params=mib(16),
        name="sweeps",
    )(steps, start, embedding, in_weight, head_out, opening, *noise, *parts)


def noise_kernel(time_each, noise_ref, *outs):
    t = lax.axis_index("tm")
    rows = noise_ref.shape[1]
    for s, out_ref in enumerate(outs):
        block = noise_ref[t ^ s].astype(jnp.float32)
        for i in range(time_each):
            out_ref[i * rows : (i + 1) * rows] = block[:, i, :].astype(jnp.bfloat16)


def noise_blocks(noise_draws, n_tm):
    rows, time_each, chan = noise_draws.shape
    own_rows = rows // n_tm
    block = jax.ShapeDtypeStruct((time_each * own_rows, chan), noise_draws.dtype)
    return pl.pallas_call(
        functools.partial(noise_kernel, time_each),
        in_specs=[VMEM],
        out_specs=[VMEM] * n_tm,
        out_shape=[block] * n_tm,
        cost_estimate=cost(0, 0, noise_draws, noise_draws),
        compiler_params=mib(4),
        name="noise",
    )(noise_draws.reshape(n_tm, own_rows, time_each, chan))


def finish_kernel(sizes, start_ref, *refs):
    time_each, rows = sizes
    parts, out_ref = refs[:-1], refs[-1]
    t = lax.axis_index("tm")
    for s, part in enumerate(parts):
        start = start_ref[t ^ s]
        for i in range(time_each):
            out_ref[pl.ds((t ^ s) * rows, rows), i, :] = start + part[
                i * rows : (i + 1) * rows
            ].astype(jnp.float32)


def finish(start, parts, time_each):
    n_tm, rows, chan = start.shape
    return pl.pallas_call(
        functools.partial(finish_kernel, (time_each, rows)),
        in_specs=[VMEM] * (1 + len(parts)),
        out_specs=VMEM,
        out_shape=jax.ShapeDtypeStruct((n_tm * rows, time_each, chan), jnp.float32),
        cost_estimate=cost(n_tm * rows * time_each * chan, 0, start, *parts),
        compiler_params=mib(4),
        name="finish",
    )(start, *parts)


def shards(
    queries,
    cache_keys,
    cache_values,
    residual,
    out_weight,
    norm_gain,
    cond_weight,
    in_weight,
    head_out,
    start_state,
    noise_draws,
    positions,
    cache_length,
    plan,
):
    rows, width = queries.shape
    n_heads = lax.axis_size("heads")
    n_tm = lax.axis_size("tm")
    h = lax.axis_index("heads")
    t = lax.axis_index("tm")
    local_heads = width // HD
    model = out_weight.shape[1] * n_tm
    row_each, time_each, chan = noise_draws.shape
    own_rows = row_each // n_tm
    hidden_width = in_weight.shape[1]

    head_cuts = math.gcd(local_heads, n_tm)
    row_cuts = n_tm // head_cuts
    share = local_heads // head_cuts
    own_row_cut = t % row_cuts

    def cut(values, index, axis):
        if row_cuts == 1:
            return values
        size = values.shape[axis] // row_cuts
        return lax.dynamic_slice_in_dim(values, index * size, size, axis)

    chips = n_heads // 2
    far = []
    for s in range(1, chips):
        far.append(swap(cond_weight, "heads", 2 * s))
    near = swap(cond_weight, "heads", 1)

    order = list(range(head_cuts))[::-1]
    outs, stats = [None] * n_tm, [None] * n_tm
    calls = calls_of(order)
    found = attend(
        queries, cache_keys, cache_values, positions, cache_length, calls, share, row_cuts
    )
    for groups, blocks in zip(calls, found):
        for a, (out, stat) in zip(groups, blocks):
            for b in range(row_cuts):
                s = a * row_cuts + b
                outs[s] = cut(out, own_row_cut ^ b, 0)
                stats[s] = None if stat is None else cut(stat, own_row_cut ^ b, 1)
                if s:
                    outs[s] = swap(outs[s], "tm", s)
                    stats[s] = None if stat is None else swap(stats[s], "tm", s)
    attended = merge(outs, stats, share, rows // row_cuts)
    parts = exchange([attended] * n_tm)
    by_cut = []
    for a in range(head_cuts):
        part = parts[a * row_cuts : (a + 1) * row_cuts]
        if row_cuts > 1:
            part = jnp.take(jnp.stack(part), jnp.arange(row_cuts) ^ own_row_cut, axis=0)
            part = part.reshape(rows, share * HD)
        else:
            part = part[0]
        by_cut.append(part)
    half = max(1, head_cuts // 2)
    cuts = list(range(head_cuts))
    total, kept = project(by_cut[:half], cuts[:half], cuts[half:], out_weight, row_cuts)
    keep, send = project_rest(total, kept, by_cut[half:], chips)

    far, send = lax.optimization_barrier((far, send))
    other = swap(send, "heads", 1)
    mine, far_rows = pair_sum(keep, other)
    got = []
    for s, r in enumerate(far_rows, 1):
        got.append(swap(r, "heads", 2 * s))

    cond_shards = [cond_weight, near]
    for s, w in enumerate(far, 1):
        cond_shards += [w, swap(w, "heads", 1)]

    cond = condition_parts(mine, got, residual, norm_gain, cond_shards, n_tm, h, t)
    cond = exchange(cond)

    noise = noise_blocks(noise_draws, n_tm)
    noise = exchange(noise)
    levels = plan.astype(jnp.float32)
    half_width = hidden_width // 2
    frequencies = jnp.exp(
        -math.log(10000.0) * jnp.arange(half_width, dtype=jnp.float32) / half_width
    )
    angles = levels[:-1, None] * frequencies[None, :]
    embedding = jnp.concatenate([jnp.sin(angles), jnp.cos(angles)], axis=1)
    step_size = (levels[:-1] - levels[1:]) / 1000.0
    steps = jnp.concatenate([step_size, jnp.sqrt(step_size)])
    start = start_state.reshape(n_tm, own_rows, chan)
    change = sweep_all(
        cond, noise, embedding, steps, start, in_weight, head_out, time_each, model
    )
    back = exchange(change)
    return finish(start, back, time_each)


def solution(mesh):
    placed = (
        P("groups", "heads"),
        P(("groups", "tm"), "heads"),
        P(("groups", "tm"), "heads"),
        P("groups", "tm"),
        P("heads", "tm"),
        P("tm"),
        P("tm", "heads"),
        P(),
        P(),
        P(("groups", "heads"), None),
        P(("groups", "heads"), "tm", None),
        P("groups"),
        P("groups"),
        P(),
    )

    return jax.shard_map(
        shards,
        mesh=mesh,
        in_specs=placed,
        out_specs=P(("groups", "heads"), "tm", None),
        check_vma=False,
    )
```

```python
import functools
import math

import jax
import jax.numpy as jnp
from jax import lax
from jax.experimental import pallas as pl
from jax.experimental.pallas import tpu as pltpu
from jax.sharding import PartitionSpec as P


HD = 128
SWEEPS = 3
LANES = 128


def swap(values, axis, distance):
    size = lax.axis_size(axis)
    return lax.ppermute(values, axis, [(i, i ^ distance) for i in range(size)])


def exchange(blocks):
    got = [blocks[0]]
    for s, block in enumerate(blocks[1:], 1):
        got.append(swap(block, "tm", s))
    return got


def pick(values, index):
    return lax.dynamic_index_in_dim(values, index, 0, False)


def cost(flops, transcendentals, *arrays):
    moved = sum(math.prod(a.shape) * jnp.dtype(a.dtype).itemsize for a in arrays)
    return pl.CostEstimate(flops=flops, bytes_accessed=moved, transcendentals=transcendentals)


def mib(count):
    return pltpu.CompilerParams(vmem_limit_bytes=count * 1024 * 1024)


VMEM = pl.BlockSpec(memory_space=pltpu.VMEM)
SMEM = pl.BlockSpec(memory_space=pltpu.SMEM)
HBM = pl.BlockSpec(memory_space=pltpu.HBM)
PIECES = 3
FIRST_MIB = 50
NEXT_MIB = 46


def pieces_of(value):
    high = value.astype(jnp.bfloat16)
    rest = value - high.astype(jnp.float32)
    middle = rest.astype(jnp.bfloat16)
    return high, middle, (rest - middle.astype(jnp.float32)).astype(jnp.bfloat16)


def sum_pieces(pieces):
    high, middle, low = (p.astype(jnp.float32) for p in pieces)
    return high + (middle + low)


def packed(rows, width, share):
    return PIECES * rows <= width and 2 * share <= 8 and rows % LANES == 0


def calls_of(order):
    return [groups for groups in (order[:1], order[1:-1], order[-1:] if order[1:] else []) if groups]


def attend_heads(groups, share, per_copy, valid, q_of, k_of, v_of, cos_ref, sin_ref, outs, stats):
    rows = cos_ref.shape[0]
    even = lax.broadcasted_iota(jnp.int32, (rows, HD), 1) % 2 == 0
    lane = lax.broadcasted_iota(jnp.int32, (rows, LANES), 1)
    scale = 1.0 / math.sqrt(HD)
    held = jnp.zeros((rows, LANES), jnp.float32)
    parts = share // per_copy
    for slot in range(len(groups) * parts):
        g, part = divmod(slot, parts)
        for i in range(per_copy):
            head = part * per_copy + i
            at = slice(i * HD, (i + 1) * HD)
            to = slice(head * HD, (head + 1) * HD)
            wide = q_of(g, to).astype(jnp.float32)
            partner = jnp.where(even, pltpu.roll(wide, HD - 1, 1), pltpu.roll(wide, 1, 1))
            rotated = (wide * cos_ref[...] + partner * sin_ref[...]).astype(jnp.bfloat16)
            scores = lax.dot_general(
                rotated,
                k_of(slot, at),
                (((1,), (1,)), ((), ())),
                preferred_element_type=jnp.float32,
            )
            scores = jnp.where(valid, scores, jnp.float32(-1e30))
            block_max = jnp.maximum(jnp.max(scores, axis=1, keepdims=True), -1e29)
            weights = jnp.exp((scores - block_max) * scale)
            block_total = jnp.sum(weights, axis=1, keepdims=True)
            block_out = jnp.dot(
                weights.astype(jnp.bfloat16), v_of(slot, at), preferred_element_type=jnp.float32
            )
            outs[g][:rows, to] = block_out.astype(jnp.bfloat16)
            held = jnp.where(lane == head, block_max * scale, held)
            held = jnp.where(lane == share + head, block_total, held)
        if part == parts - 1:
            flat = held.T
            if stats:
                stats[g][...] = flat[: 2 * share]
            else:
                extra = outs[g].shape[0] - rows
                for p, piece in enumerate(pieces_of(flat[:extra])):
                    outs[g][rows:, p * rows : (p + 1) * rows] = piece


def valid_keys(length_ref, keys):
    return (
        lax.broadcasted_iota(jnp.int32, (1, keys), 1)
        < length_ref[0] - lax.axis_index("tm") * keys
    )


def attend_kernel(calls, share, per_copy, row_cuts, joined, *refs):
    length_ref, pos_ref, q_hbm, k_hbm, v_hbm = refs[:5]
    groups = calls[0]
    n = len(groups)
    outs, refs = refs[5 : 5 + n], refs[5 + n :]
    stats, refs = ([], refs) if joined else (refs[:n], refs[n:])
    cos_ref, sin_ref, refs = refs[0], refs[1], refs[2:]
    kept, refs = refs[: 3 * len(calls) - 3], refs[3 * len(calls) - 3 :]
    q_buf, k_buf, v_buf, sem = refs
    rows = q_hbm.shape[0]
    keys = k_hbm.shape[0]
    own = lax.axis_index("tm") // row_cuts
    width = per_copy * HD
    parts = share // per_copy
    copies = []

    def start(from_ref, to_ref):
        copies.append(pltpu.make_async_copy(from_ref, to_ref, sem.at[len(copies)]))
        copies[-1].start()
        return copies[-1]

    first_copies = []
    for c, call in enumerate(calls):
        to = (q_buf, k_buf, v_buf) if c == 0 else kept[3 * c - 3 : 3 * c]
        for g, a in enumerate(call):
            first = pl.multiple_of((own ^ a) * share * HD, HD)
            wanted = [start(q_hbm.at[:, pl.ds(first, share * HD)], to[0].at[g])]
            for part in range(parts):
                slot = g * parts + part
                column = pl.multiple_of(first + part * width, HD)
                wanted += [
                    start(hbm.at[:, pl.ds(column, width)], buf.at[slot])
                    for hbm, buf in ((k_hbm, to[1]), (v_hbm, to[2]))
                ]
                if c == 0:
                    first_copies.append(wanted)
                    wanted = []
    lane = lax.broadcasted_iota(jnp.int32, (1, HD), 1)
    frequencies = jnp.exp((lane - lane % 2).astype(jnp.float32) * (-math.log(10000.0) / HD))
    place = jnp.broadcast_to(pos_ref[...].astype(jnp.float32), (HD, rows)).T
    angles = place * frequencies
    cos_ref[...] = jnp.cos(angles)
    sine = jnp.sin(angles)
    sin_ref[...] = jnp.where(lane % 2 == 0, -sine, sine)
    done = set()

    def near(buf):
        def read(slot, at):
            if slot not in done:
                done.add(slot)
                for copy in first_copies[slot]:
                    copy.wait()
            return buf[slot, :, at]

        return read

    def query(g, at):
        if g * parts not in done:
            done.add(g * parts)
            for copy in first_copies[g * parts]:
                copy.wait()
        return q_buf[g, :, at]

    attend_heads(
        groups,
        share,
        per_copy,
        valid_keys(length_ref, keys),
        query,
        near(k_buf),
        near(v_buf),
        cos_ref,
        sin_ref,
        outs,
        stats,
    )
    for copy in copies[sum(len(wanted) for wanted in first_copies) :]:
        copy.wait()


def attend_near_kernel(groups, fresh, later, share, per_copy, row_cuts, joined, *refs):
    length_ref, cos_ref, sin_ref, q_ref, k_ref, v_ref = refs[:6]
    refs = refs[6:]
    hbm, refs = (refs[:3], refs[3:]) if fresh or later else ([], refs)
    n = len(groups) + len(fresh)
    outs, refs = refs[:n], refs[n:]
    stats, refs = ([], refs) if joined else (refs[:n], refs[n:])
    kept, refs = (refs[:3], refs[3:]) if later else ([], refs)
    parts = share // per_copy
    copies, waiting = [], {}
    if hbm:
        sem = refs[-1]
        own = lax.axis_index("tm") // row_cuts
        for to, call in ((refs[:3] if fresh else [], fresh), (kept, later)):
            for g, a in enumerate(call):
                first = pl.multiple_of((own ^ a) * share * HD, HD)
                for part in range(parts):
                    slot = g * parts + part
                    column = pl.multiple_of(first + part * per_copy * HD, HD)
                    wanted = [(hbm[0].at[:, pl.ds(first, share * HD)], to[0].at[g])] * (part == 0)
                    for from_ref, to_ref in zip(hbm[1:], to[1:]):
                        wanted.append(
                            (from_ref.at[:, pl.ds(column, per_copy * HD)], to_ref.at[slot])
                        )
                    started = []
                    for pair in wanted:
                        copies.append(pltpu.make_async_copy(*pair, sem.at[len(copies)]))
                        copies[-1].start()
                        started.append(copies[-1])
                    if call is fresh:
                        waiting[len(groups) * parts + slot] = started
    late = copies[sum(len(started) for started in waiting.values()) :]
    near_slots = len(groups) * parts

    def arrive(slot):
        for copy in waiting.pop(slot, []):
            copy.wait()

    def query(g, at):
        arrive(g * parts)
        return q_ref[g, :, at] if g < len(groups) else refs[0][g - len(groups), :, at]

    def reader(near_ref, index):
        def read(slot, at):
            arrive(slot)
            return near_ref[slot, :, at] if slot < near_slots else refs[index][slot - near_slots, :, at]

        return read

    attend_heads(
        (*groups, *fresh),
        share,
        per_copy,
        valid_keys(length_ref, k_ref.shape[1]),
        query,
        reader(k_ref, 1),
        reader(v_ref, 2),
        cos_ref,
        sin_ref,
        outs,
        stats,
    )
    for copy in late:
        copy.wait()


def attend(queries, keys, values, positions, cache_length, calls, share, row_cuts):
    rows = queries.shape[0]
    key_count = keys.shape[0]
    per_copy = 2 if share % 2 == 0 else 1
    wide = share * HD
    joined = row_cuts == 1 and packed(rows, wide, share)
    table = jax.ShapeDtypeStruct((rows, HD), jnp.float32)

    def blocks(n):
        shapes = [jax.ShapeDtypeStruct((rows + 8 * joined, wide), jnp.bfloat16)] * n
        if not joined:
            shapes = shapes + [jax.ShapeDtypeStruct((2 * share, rows), jnp.float32)] * n
        return shapes

    def near(n):
        cache = (n * share // per_copy, key_count, per_copy * HD)
        return [((n, rows, wide), jnp.bfloat16), (cache, jnp.bfloat16), (cache, jnp.bfloat16)]

    def price(n):
        return pl.CostEstimate(
            flops=4 * n * share * rows * key_count * HD,
            bytes_accessed=4 * n * share * key_count * HD,
            transcendentals=n * share * rows * key_count,
        )

    def found(result, n):
        return list(zip(result[:n], [None] * n if joined else result[n : 2 * n]))

    split = [(call[:1], call[1:]) for call in calls[1:]]
    n = len(calls[0])
    nearby = split[0][0] if split else []
    out_shape = blocks(n) + [table] * 2
    if nearby:
        out_shape = out_shape + [jax.ShapeDtypeStruct(*entry) for entry in near(len(nearby))]
    count = (n + len(nearby)) * (1 + 2 * share // per_copy)
    result = pl.pallas_call(
        functools.partial(
            attend_kernel,
            [calls[0], nearby] if nearby else [calls[0]],
            share,
            per_copy,
            row_cuts,
            joined,
        ),
        in_specs=[SMEM, VMEM] + [HBM] * 3,
        out_specs=[VMEM] * len(out_shape),
        out_shape=out_shape,
        scratch_shapes=[pltpu.VMEM(*entry) for entry in near(n)]
        + [pltpu.SemaphoreType.DMA((count,))],
        cost_estimate=price(n),
        compiler_params=mib(FIRST_MIB),
        name="attend",
    )(cache_length, positions[None], queries, keys, values)
    skip = len(blocks(n))
    tables, kept = result[skip : skip + 2], result[skip + 2 :]
    blocks_of = [found(result, n)]
    for c, (groups, fresh) in enumerate(split):
        later = split[c + 1][0] if c + 1 < len(split) else []
        n = len(groups) + len(fresh)
        moving = bool(fresh or later)
        out_shape = blocks(n)
        scratch = []
        if later:
            out_shape = out_shape + [jax.ShapeDtypeStruct(*entry) for entry in near(len(later))]
        if fresh:
            scratch = [pltpu.VMEM(*entry) for entry in near(len(fresh))]
        if moving:
            count = (len(fresh) + len(later)) * (1 + 2 * share // per_copy)
            scratch = scratch + [pltpu.SemaphoreType.DMA((count,))]
        result = pl.pallas_call(
            functools.partial(
                attend_near_kernel, groups, fresh, later, share, per_copy, row_cuts, joined
            ),
            in_specs=[SMEM] + [VMEM] * 5 + [HBM] * 3 * moving,
            out_specs=[VMEM] * len(out_shape),
            out_shape=out_shape,
            scratch_shapes=scratch,
            cost_estimate=price(n),
            compiler_params=mib(NEXT_MIB if moving else 16),
            name="attend_near",
        )(cache_length, *tables, *kept, *([queries, keys, values] if moving else []))
        blocks_of.append(found(result, n))
        kept = result[len(blocks(n)) :]
    return blocks_of


def merge_kernel(count, share, *refs):
    out_ref = refs[-1]
    rows = out_ref.shape[0]
    outs, stats = refs[:count], refs[count:-1]
    if stats:
        tables = [s[...] for s in stats]
    else:
        tables = [
            sum_pieces([o[rows:, p * rows : (p + 1) * rows] for p in range(PIECES)]) for o in outs
        ]
    maxima = [s[:share] for s in tables]
    totals = [s[share : 2 * share] for s in tables]
    top = functools.reduce(jnp.maximum, maxima)
    factors = [jnp.exp(m - top) for m in maxima]
    total = sum(f * s for f, s in zip(factors, totals))
    scales = [f / total for f in factors]
    pad = -(count * share) % LANES
    table = jnp.concatenate(scales + [jnp.zeros((pad, rows), jnp.float32)], axis=0).T
    for head in range(share):
        at = slice(head * HD, (head + 1) * HD)
        value = sum(
            o[:rows, at].astype(jnp.float32) * table[:, i * share + head : i * share + head + 1]
            for i, o in enumerate(outs)
        )
        out_ref[:, at] = value.astype(jnp.bfloat16)


def merge(outs, stats, share, rows):
    width = outs[0].shape[1]
    stats = [s for s in stats if s is not None]
    return pl.pallas_call(
        functools.partial(merge_kernel, len(outs), share),
        in_specs=[VMEM] * (len(outs) + len(stats)),
        out_specs=VMEM,
        out_shape=jax.ShapeDtypeStruct((rows, width), jnp.bfloat16),
        cost_estimate=cost(4 * len(outs) * rows * width, 0, *outs, *stats),
        compiler_params=mib(4),
        name="merge",
    )(*outs, *stats)


def core_order(part, chips):
    core = lax.axis_index("heads") % 2
    rows = part.shape[0] // (2 * chips)
    firsts = [
        pl.multiple_of((2 * chip + c) * rows, rows) for c in (core, 1 - core) for chip in range(chips)
    ]
    return jnp.concatenate([part[pl.ds(first, rows), :] for first in firsts], axis=0)


def project_kernel(cuts, later, row_cuts, chips, *refs):
    parts, refs = refs[: len(cuts)], refs[len(cuts) :]
    w_hbm, total_ref, kept_ref, w_buf, sem = refs
    own = lax.axis_index("tm") // row_cuts
    depth = w_buf.shape[1]
    copies = []
    for i, a in enumerate((*cuts, *later)):
        first = pl.multiple_of((own ^ a) * depth, depth)
        to = w_buf.at[i] if i < len(cuts) else kept_ref.at[i - len(cuts)]
        copies.append(pltpu.make_async_copy(w_hbm.at[pl.ds(first, depth)], to, sem.at[i]))
        copies[i].start()
    for i, part in enumerate(parts):
        copies[i].wait()
        product = jnp.dot(
            core_order(part, chips), w_buf[i], preferred_element_type=jnp.float32
        )
        total_ref[...] = product + total_ref[...] if i else product
    for copy in copies[len(cuts) :]:
        copy.wait()


def project(parts, cuts, later, weight, row_cuts, chips):
    rows, depth = parts[0].shape
    columns = weight.shape[1]
    return pl.pallas_call(
        functools.partial(project_kernel, cuts, later, row_cuts, chips),
        in_specs=[VMEM] * len(parts) + [HBM],
        out_specs=[VMEM, VMEM],
        out_shape=[
            jax.ShapeDtypeStruct((rows, columns), jnp.float32),
            jax.ShapeDtypeStruct((len(later), depth, columns), weight.dtype),
        ],
        scratch_shapes=[
            pltpu.VMEM((len(cuts), depth, columns), weight.dtype),
            pltpu.SemaphoreType.DMA((len(cuts) + len(later),)),
        ],
        cost_estimate=cost(2 * len(parts) * rows * depth * columns, 0, weight),
        compiler_params=mib(16),
        name="project",
    )(*parts, weight)


def project_rest_kernel(count, total_ref, kept_ref, *refs):
    parts, (keep_ref, send_ref) = refs[:count], refs[count:]
    chips, rows = keep_ref.shape[:2]
    value = total_ref[...]
    for i, part in enumerate(parts):
        value = value + jnp.dot(
            core_order(part, chips), kept_ref[i], preferred_element_type=jnp.float32
        )
    for chip in range(chips):
        keep_ref[chip] = value[chip * rows : (chip + 1) * rows]
        other = (chips + chip) * rows
        send_ref[chip] = value[other : other + rows].astype(jnp.bfloat16)


def project_rest(total, kept, parts, chips):
    rows, columns = total.shape
    block = (chips, rows // (2 * chips), columns)
    return pl.pallas_call(
        functools.partial(project_rest_kernel, len(parts)),
        in_specs=[VMEM] * (2 + len(parts)),
        out_specs=[VMEM, VMEM],
        out_shape=[
            jax.ShapeDtypeStruct(block, jnp.float32),
            jax.ShapeDtypeStruct(block, jnp.bfloat16),
        ],
        cost_estimate=cost(2 * rows * columns * kept.shape[0] * kept.shape[1], 0, kept),
        compiler_params=mib(16),
        name="project_rest",
    )(total, kept, *parts)


def pair_kernel(keep_ref, got_ref, mine_ref, *send_refs):
    chip = lax.axis_index("heads") // 2
    mine_ref[...] = keep_ref[chip] + got_ref[chip].astype(jnp.float32)
    for s, send_ref in enumerate(send_refs, 1):
        send_ref[...] = (keep_ref[chip ^ s] + got_ref[chip ^ s].astype(jnp.float32)).astype(
            jnp.bfloat16
        )


def pair_sum(keep, got):
    chips, rows, columns = keep.shape
    result = pl.pallas_call(
        pair_kernel,
        in_specs=[VMEM] * 2,
        out_specs=[VMEM] * chips,
        out_shape=[jax.ShapeDtypeStruct((rows, columns), jnp.float32)]
        + [jax.ShapeDtypeStruct((rows, columns), jnp.bfloat16)] * (chips - 1),
        cost_estimate=cost(chips * rows * columns, 0, keep, got),
        compiler_params=mib(8),
        name="pair",
    )(keep, got)
    return result[0], result[1:]


def condition_kernel(chips, shards, own_rows, mine_ref, residual_ref, gain_ref, *refs):
    got, refs = refs[: chips - 1], refs[chips - 1 :]
    weights, refs = refs[:shards], refs[shards:]
    rows = mine_ref.shape[0]
    h = lax.axis_index("heads")
    hidden = residual_ref[h].astype(jnp.float32) + mine_ref[...]
    for ref in got:
        hidden = hidden + ref[...].astype(jnp.float32)
    squares = jnp.sum(hidden * hidden, axis=1, keepdims=True)
    scaled = (hidden * gain_ref[...]).astype(jnp.bfloat16)
    width = weights[0].shape[1]
    products = [jnp.dot(scaled, w[...], preferred_element_type=jnp.float32) for w in weights]
    tail = jnp.zeros((rows, LANES), jnp.float32)
    lane = lax.broadcasted_iota(jnp.int32, (rows, LANES), 1)
    for p, piece in enumerate(pieces_of(squares)):
        tail = jnp.where(lane == p, piece.astype(jnp.float32), tail)
    if own_rows % 8 == 0 and width % LANES == 0:
        outs, held = refs[:-1], refs[-1]
        t = lax.axis_index("tm")
        for s, product in enumerate(products):
            held[:, pl.ds(pl.multiple_of((h ^ s) * width, LANES), width)] = product
        held[:, shards * width :] = tail
        for s, out_ref in enumerate(outs):
            first = pl.multiple_of((t ^ s) * own_rows, own_rows)
            out_ref[...] = held[pl.ds(first, own_rows), :].astype(jnp.bfloat16)
    else:
        for s, product in enumerate(products):
            refs[0][:, s * width : (s + 1) * width] = product.astype(jnp.bfloat16)
        refs[0][:, shards * width :] = tail.astype(jnp.bfloat16)


def condition_parts(mine, got, residual, gain, weights, n_tm, h, t):
    rows, depth = mine.shape
    shards = len(weights)
    width = weights[0].shape[1]
    full = shards * width + LANES
    own_rows = rows // n_tm
    aligned = own_rows % 8 == 0 and width % LANES == 0
    block = jax.ShapeDtypeStruct((own_rows, full), jnp.bfloat16)
    out_shape = [block] * n_tm if aligned else [jax.ShapeDtypeStruct((rows, full), jnp.bfloat16)]
    result = pl.pallas_call(
        functools.partial(condition_kernel, len(got) + 1, shards, own_rows),
        in_specs=[VMEM] * (3 + len(got) + shards),
        out_specs=[VMEM] * len(out_shape),
        out_shape=out_shape,
        scratch_shapes=[pltpu.VMEM((rows, full), jnp.float32)] * aligned,
        cost_estimate=cost(2 * rows * depth * full, 0, *weights),
        compiler_params=mib(12),
        name="condition",
    )(mine, residual.reshape(-1, rows, depth), gain[None, :], *got, *weights)
    if aligned:
        return result
    columns = result[0][:, :-LANES].reshape(rows, shards, width)
    columns = jnp.take(columns, jnp.arange(shards) ^ h, axis=1).reshape(rows, shards * width)
    result = jnp.concatenate([columns, result[0][:, -LANES:]], axis=1)
    result = result.reshape(n_tm, own_rows, full)
    return [pick(result, t ^ s) for s in range(n_tm)]


def opening_kernel(start_ref, in_ref, out_ref):
    start = start_ref[lax.axis_index("tm")].astype(jnp.bfloat16)
    out_ref[...] = jnp.dot(start, in_ref[...], preferred_element_type=jnp.float32)


def opening_product(start, in_weight):
    rows, width = start.shape[1], in_weight.shape[1]
    return pl.pallas_call(
        opening_kernel,
        in_specs=[VMEM] * 2,
        out_specs=VMEM,
        out_shape=jax.ShapeDtypeStruct((rows, width), jnp.float32),
        cost_estimate=cost(2 * rows * in_weight.size, 0, in_weight),
        compiler_params=mib(8),
        name="opening",
    )(start, in_weight)


def sweep_kernel(sizes, steps, start_ref, embed_ref, in_ref, head_ref, opening_ref, *refs):
    n_tm, time_each, rows, model = sizes
    noise_refs, refs = refs[:n_tm], refs[n_tm:]
    parts, refs = refs[:n_tm], refs[n_tm:]
    outs, held = refs[:n_tm], refs[n_tm]
    t = lax.axis_index("tm")
    times = n_tm * time_each
    start = start_ref[t]
    chan = start.shape[1]
    for s, ref in enumerate(noise_refs):
        held[t ^ s] = ref[...].astype(jnp.float32)

    def block(i):
        at = (i % time_each) * rows
        return i // time_each, slice(at, at + rows)

    noise = [steps[times + i] * held[block(i)] for i in range(times - 1)]
    width = in_ref.shape[1]
    opening = opening_ref[...]
    total = sum(p[...].astype(jnp.float32) for p in parts)
    squares = total[:, width : width + 1]
    for p in range(1, PIECES):
        squares = squares + total[:, width + p : width + p + 1]
    condition = total[:, :width] * lax.rsqrt(squares / model + 1e-06)

    def increments_at(first, products):
        last = first + len(products)
        inside = jnp.concatenate(
            [p + (condition + embed_ref[i : i + 1]) for i, p in enumerate(products, first)], axis=0
        )
        action = (inside * jax.nn.sigmoid(inside)).astype(jnp.bfloat16)
        drift = jnp.dot(action, head_ref[...], preferred_element_type=jnp.float32)
        return [
            steps[i] * drift[(i - first) * rows : (i - first + 1) * rows] + noise[i]
            for i in range(first, last)
        ]

    increments = increments_at(0, [opening] * (times - 1))
    for sweep in range(1, SWEEPS + 1):
        change = [jnp.zeros((rows, chan), jnp.float32)]
        for i in range(times - 1):
            change.append(change[-1] + increments[i])
        if sweep == SWEEPS or sweep >= times - 1:
            break
        states = jnp.concatenate([start + change[i] for i in range(sweep, times - 1)], axis=0)
        product = jnp.dot(
            states.astype(jnp.bfloat16), in_ref[...], preferred_element_type=jnp.float32
        )
        increments = increments[:sweep] + increments_at(
            sweep, [product[i * rows : (i + 1) * rows] for i in range(times - 1 - sweep)]
        )
    for i in range(times):
        held[block(i)] = change[i]
    for s, out_ref in enumerate(outs):
        out_ref[...] = held[t ^ s].astype(jnp.bfloat16)


def sweep_all(parts, noise, embedding, steps, start, in_weight, head_out, time_each, model):
    n_tm, rows, chan = start.shape
    block = (time_each * rows, chan)
    opening = opening_product(start, in_weight)
    return pl.pallas_call(
        functools.partial(sweep_kernel, (n_tm, time_each, rows, model)),
        in_specs=[SMEM] + [VMEM] * (5 + 2 * n_tm),
        out_specs=[VMEM] * n_tm,
        out_shape=[jax.ShapeDtypeStruct(block, jnp.bfloat16)] * n_tm,
        scratch_shapes=[pltpu.VMEM((n_tm, *block), jnp.float32)],
        cost_estimate=cost(
            10 * n_tm * time_each * rows * chan * in_weight.shape[1], 0, in_weight, head_out
        ),
        compiler_params=mib(16),
        name="sweeps",
    )(steps, start, embedding, in_weight, head_out, opening, *noise, *parts)


def noise_kernel(time_each, noise_ref, *outs):
    t = lax.axis_index("tm")
    rows = noise_ref.shape[1]
    for s, out_ref in enumerate(outs):
        block = noise_ref[t ^ s].astype(jnp.float32)
        for i in range(time_each):
            out_ref[i * rows : (i + 1) * rows] = block[:, i, :].astype(jnp.bfloat16)


def noise_blocks(noise_draws, n_tm):
    rows, time_each, chan = noise_draws.shape
    own_rows = rows // n_tm
    block = jax.ShapeDtypeStruct((time_each * own_rows, chan), noise_draws.dtype)
    return pl.pallas_call(
        functools.partial(noise_kernel, time_each),
        in_specs=[VMEM],
        out_specs=[VMEM] * n_tm,
        out_shape=[block] * n_tm,
        cost_estimate=cost(0, 0, noise_draws, noise_draws),
        compiler_params=mib(4),
        name="noise",
    )(noise_draws.reshape(n_tm, own_rows, time_each, chan))


def finish_kernel(sizes, start_ref, *refs):
    time_each, rows = sizes
    parts, out_ref = refs[:-1], refs[-1]
    t = lax.axis_index("tm")
    for s, part in enumerate(parts):
        start = start_ref[t ^ s]
        for i in range(time_each):
            out_ref[pl.ds((t ^ s) * rows, rows), i, :] = start + part[
                i * rows : (i + 1) * rows
            ].astype(jnp.float32)


def finish(start, parts, time_each):
    n_tm, rows, chan = start.shape
    return pl.pallas_call(
        functools.partial(finish_kernel, (time_each, rows)),
        in_specs=[VMEM] * (1 + len(parts)),
        out_specs=VMEM,
        out_shape=jax.ShapeDtypeStruct((n_tm * rows, time_each, chan), jnp.float32),
        cost_estimate=cost(n_tm * rows * time_each * chan, 0, start, *parts),
        compiler_params=mib(4),
        name="finish",
    )(start, *parts)


def shards(
    queries,
    cache_keys,
    cache_values,
    residual,
    out_weight,
    norm_gain,
    cond_weight,
    in_weight,
    head_out,
    start_state,
    noise_draws,
    positions,
    cache_length,
    plan,
):
    rows, width = queries.shape
    n_heads = lax.axis_size("heads")
    n_tm = lax.axis_size("tm")
    h = lax.axis_index("heads")
    t = lax.axis_index("tm")
    local_heads = width // HD
    model = out_weight.shape[1] * n_tm
    row_each, time_each, chan = noise_draws.shape
    own_rows = row_each // n_tm
    hidden_width = in_weight.shape[1]

    head_cuts = math.gcd(local_heads, n_tm)
    row_cuts = n_tm // head_cuts
    share = local_heads // head_cuts
    own_row_cut = t % row_cuts

    def cut(values, index, axis):
        if row_cuts == 1:
            return values
        size = values.shape[axis] // row_cuts
        return lax.dynamic_slice_in_dim(values, index * size, size, axis)

    chips = n_heads // 2
    far = []
    for s in range(1, chips):
        far.append(swap(cond_weight, "heads", 2 * s))
    near = swap(cond_weight, "heads", 1)

    order = list(range(head_cuts))[::-1]
    outs, stats = [None] * n_tm, [None] * n_tm
    calls = calls_of(order)
    found = attend(
        queries, cache_keys, cache_values, positions, cache_length, calls, share, row_cuts
    )
    for groups, blocks in zip(calls, found):
        for a, (out, stat) in zip(groups, blocks):
            for b in range(row_cuts):
                s = a * row_cuts + b
                outs[s] = cut(out, own_row_cut ^ b, 0)
                stats[s] = None if stat is None else cut(stat, own_row_cut ^ b, 1)
                if s:
                    outs[s] = swap(outs[s], "tm", s)
                    stats[s] = None if stat is None else swap(stats[s], "tm", s)
    attended = merge(outs, stats, share, rows // row_cuts)
    parts = exchange([attended] * n_tm)
    by_cut = []
    for a in range(head_cuts):
        part = parts[a * row_cuts : (a + 1) * row_cuts]
        if row_cuts > 1:
            part = jnp.take(jnp.stack(part), jnp.arange(row_cuts) ^ own_row_cut, axis=0)
            part = part.reshape(rows, share * HD)
        else:
            part = part[0]
        by_cut.append(part)
    half = max(1, head_cuts // 2)
    cuts = list(range(head_cuts))
    total, kept = project(by_cut[:half], cuts[:half], cuts[half:], out_weight, row_cuts, chips)
    keep, send = project_rest(total, kept, by_cut[half:], chips)

    far, send = lax.optimization_barrier((far, send))
    other = swap(send, "heads", 1)
    mine, far_rows = pair_sum(keep, other)
    got = []
    for s, r in enumerate(far_rows, 1):
        got.append(swap(r, "heads", 2 * s))

    cond_shards = [cond_weight, near]
    for s, w in enumerate(far, 1):
        cond_shards += [w, swap(w, "heads", 1)]

    cond = condition_parts(mine, got, residual, norm_gain, cond_shards, n_tm, h, t)
    cond = exchange(cond)

    noise = noise_blocks(noise_draws, n_tm)
    noise = exchange(noise)
    levels = plan.astype(jnp.float32)
    half_width = hidden_width // 2
    frequencies = jnp.exp(
        -math.log(10000.0) * jnp.arange(half_width, dtype=jnp.float32) / half_width
    )
    angles = levels[:-1, None] * frequencies[None, :]
    embedding = jnp.concatenate([jnp.sin(angles), jnp.cos(angles)], axis=1)
    step_size = (levels[:-1] - levels[1:]) / 1000.0
    steps = jnp.concatenate([step_size, jnp.sqrt(step_size)])
    start = start_state.reshape(n_tm, own_rows, chan)
    change = sweep_all(
        cond, noise, embedding, steps, start, in_weight, head_out, time_each, model
    )
    back = exchange(change)
    return finish(start, back, time_each)


def solution(mesh):
    placed = (
        P("groups", "heads"),
        P(("groups", "tm"), "heads"),
        P(("groups", "tm"), "heads"),
        P("groups", "tm"),
        P("heads", "tm"),
        P("tm"),
        P("tm", "heads"),
        P(),
        P(),
        P(("groups", "heads"), None),
        P(("groups", "heads"), "tm", None),
        P("groups"),
        P("groups"),
        P(),
    )

    return jax.shard_map(
        shards,
        mesh=mesh,
        in_specs=placed,
        out_specs=P(("groups", "heads"), "tm", None),
        check_vma=False,
    )
```
